128 devices in a mesh: dp: 128 (over z, y, x, core).
Axes of the slice: x: 4, y: 4, z: 4, core: 2. Of those that a mesh axis runs over, the one named last changes fastest.
Arguments:
- query_feat: bfloat16 [32768, 512], P('dp')
- item_feat: bfloat16 [32768, 512], P('dp')
- log_q: float32 [32768], P('dp')
- w_query_in: bfloat16 [512, 256], replicated
- w_query_out: bfloat16 [256, 128], replicated
- w_item_in: bfloat16 [512, 256], replicated
- w_item_out: bfloat16 [256, 128], replicated
Outputs:
- output 1: float32 [1], replicated
- output 2: float32 [512, 256], replicated
- output 3: float32 [256, 128], replicated
- output 4: float32 [512, 256], replicated
- output 5: float32 [256, 128], replicated
All inputs are finite; a program needn't handle non-finite values.
Results may differ from the reference program's by a relative error of at most 0.00699549.
Values are sent between devices in bfloat16 or wider.
A program may use at most 1 GiB of HBM per device.

```python
import jax
import jax.numpy as jnp
from jax import lax

GROUP_DEVICES = 128
ROWS_DEV = 256
FEAT_DIM = 512
HIDDEN_DIM = 256
EMBED_DIM = 128
GLOBAL_ROWS = GROUP_DEVICES * ROWS_DEV
POOL_SIZE = GLOBAL_ROWS // 4
BLOCK_ROWS = min(GLOBAL_ROWS, 256)
TEMPERATURE = 0.05
NORM_EPS = 1e-6


def setup_inputs(seed: int = 0) -> dict:
    base_key = jax.random.key(seed)
    keys_all = jax.random.split(base_key, 9)
    query_feat = jax.random.normal(keys_all[0], (GLOBAL_ROWS, FEAT_DIM), jnp.float32).astype(jnp.bfloat16)
    item_pool = jax.random.normal(keys_all[1], (POOL_SIZE, FEAT_DIM), jnp.float32)
    pick_a = jax.random.randint(keys_all[2], (GLOBAL_ROWS,), 0, POOL_SIZE)
    pick_b = jax.random.randint(keys_all[3], (GLOBAL_ROWS,), 0, POOL_SIZE)
    item_ids = (pick_a * pick_b) // POOL_SIZE
    item_feat = jnp.take(item_pool, item_ids, axis=0).astype(jnp.bfloat16)
    counts = jax.ops.segment_sum(jnp.ones((GLOBAL_ROWS,), jnp.float32), item_ids, num_segments=POOL_SIZE)
    log_q = jnp.log(jnp.take(counts, item_ids) / GLOBAL_ROWS) + 0.3 * jax.random.normal(keys_all[4], (GLOBAL_ROWS,), jnp.float32)
    w_query_in = (jax.random.normal(keys_all[5], (FEAT_DIM, HIDDEN_DIM), jnp.float32) * FEAT_DIM ** -0.5).astype(jnp.bfloat16)
    w_query_out = (jax.random.normal(keys_all[6], (HIDDEN_DIM, EMBED_DIM), jnp.float32) * HIDDEN_DIM ** -0.5).astype(jnp.bfloat16)
    w_item_in = (jax.random.normal(keys_all[7], (FEAT_DIM, HIDDEN_DIM), jnp.float32) * FEAT_DIM ** -0.5).astype(jnp.bfloat16)
    w_item_out = (jax.random.normal(keys_all[8], (HIDDEN_DIM, EMBED_DIM), jnp.float32) * HIDDEN_DIM ** -0.5).astype(jnp.bfloat16)
    return {'query_feat': query_feat, 'item_feat': item_feat, 'log_q': log_q, 'w_query_in': w_query_in, 'w_query_out': w_query_out, 'w_item_in': w_item_in, 'w_item_out': w_item_out}


def tower_forward(feat_rows, w_in, w_out):
    pre_act = jnp.dot(feat_rows, w_in, preferred_element_type=jnp.float32)
    hidden = jnp.maximum(pre_act, 0.0).astype(jnp.bfloat16)
    embed = jnp.dot(hidden, w_out, preferred_element_type=jnp.float32)
    inv_norm = lax.rsqrt(jnp.sum(embed * embed, axis=-1, keepdims=True) + NORM_EPS)
    return pre_act, hidden, inv_norm, embed * inv_norm


def tower_backward(feat_rows, w_out, pre_act, hidden, inv_norm, unit_vec, d_unit):
    d_embed = inv_norm * (d_unit - unit_vec * jnp.sum(unit_vec * d_unit, axis=-1, keepdims=True))
    d_embed_bf = d_embed.astype(jnp.bfloat16)
    grad_out = jnp.dot(hidden.T, d_embed_bf, preferred_element_type=jnp.float32)
    d_hidden = jnp.dot(d_embed_bf, w_out.T, preferred_element_type=jnp.float32)
    d_pre = jnp.where(pre_act > 0, d_hidden, 0.0).astype(jnp.bfloat16)
    grad_in = jnp.dot(feat_rows.T, d_pre, preferred_element_type=jnp.float32)
    return grad_in, grad_out


def softmax_grads(query_bf, items_bf, log_q):
    num_blocks = GLOBAL_ROWS // BLOCK_ROWS
    grad_scale = 1.0 / (TEMPERATURE * GLOBAL_ROWS)
    col_ids = jnp.arange(GLOBAL_ROWS)[None, :]
    query_blocks = query_bf.reshape(num_blocks, BLOCK_ROWS, EMBED_DIM)

    def block_step(d_item_acc, inputs):
        block_index, query_blk = inputs
        logits = jnp.dot(query_blk, items_bf.T, preferred_element_type=jnp.float32) / TEMPERATURE - log_q[None, :]
        row_ids = block_index * BLOCK_ROWS + jnp.arange(BLOCK_ROWS)[:, None]
        is_pos = row_ids == col_ids
        row_max = jnp.max(logits, axis=1, keepdims=True)
        log_norm = row_max + jnp.log(jnp.sum(jnp.exp(logits - row_max), axis=1, keepdims=True))
        pos_logit = jnp.sum(jnp.where(is_pos, logits, 0.0), axis=1, keepdims=True)
        prob_rows = jnp.exp(logits - log_norm)
        grad_logits = jnp.where(is_pos, prob_rows - 1.0, prob_rows).astype(jnp.bfloat16)
        d_query_blk = jnp.dot(grad_logits, items_bf, preferred_element_type=jnp.float32) * grad_scale
        d_item_acc = d_item_acc + jnp.dot(grad_logits.T, query_blk, preferred_element_type=jnp.float32)
        return d_item_acc, (jnp.sum(log_norm - pos_logit), d_query_blk)

    acc_init = jnp.zeros((GLOBAL_ROWS, EMBED_DIM), jnp.float32)
    d_item_acc, (loss_parts, d_query_blocks) = lax.scan(block_step, acc_init, (jnp.arange(num_blocks), query_blocks))
    return jnp.sum(loss_parts), d_query_blocks.reshape(GLOBAL_ROWS, EMBED_DIM), d_item_acc * grad_scale


def reference(query_feat, item_feat, log_q, w_query_in, w_query_out, w_item_in, w_item_out):
    q_pre, q_hidden, q_inv, q_unit = tower_forward(query_feat, w_query_in, w_query_out)
    v_pre, v_hidden, v_inv, v_unit = tower_forward(item_feat, w_item_in, w_item_out)
    loss_sum, d_query, d_item = softmax_grads(q_unit.astype(jnp.bfloat16), v_unit.astype(jnp.bfloat16), log_q)
    grad_query_in, grad_query_out = tower_backward(query_feat, w_query_out, q_pre, q_hidden, q_inv, q_unit, d_query)
    grad_item_in, grad_item_out = tower_backward(item_feat, w_item_out, v_pre, v_hidden, v_inv, v_unit, d_item)
    loss = jnp.reshape(loss_sum / GLOBAL_ROWS, (1,))
    return (loss, grad_query_in, grad_query_out, grad_item_in, grad_item_out)
```

```python
import functools

import jax
import jax.numpy as jnp
from jax import lax
from jax.experimental import pallas as pl
from jax.experimental.pallas import tpu as pltpu
from jax.sharding import PartitionSpec as P

TEMP = 0.05
NORM_EPS = 1e-6
LOG2E = 1.4426950408889634
BOUND = 20.25
F32 = jnp.float32
BF16 = jnp.bfloat16
NA, NB, NC = 8, 16, 8
STEP = (0, 1, 3, 2)
BACK = (0, 2, 1, 3)
INV_A = [2 * BACK[s // 2] + s % 2 for s in range(NA)]
INV_B = [4 * BACK[t // 4] + t % 4 for t in range(NB)]


def rel_a(r, s):
    dy = (STEP[r // 2] - STEP[s // 2]) % 4
    return 2 * STEP.index(dy) + (r % 2 + s % 2) % 2


def nt(a, b):
    return lax.dot_general(a, b, (((1,), (1,)), ((), ())), preferred_element_type=F32)


def tn(a, b):
    return lax.dot_general(a, b, (((0,), (0,)), ((), ())), preferred_element_type=F32)


def nn(a, b):
    return jnp.dot(a, b, preferred_element_type=F32)


def forward(x, w_in, w_out, pre_s, hid_s, inv_s, unit_s, out):
    pre = nn(x[...], w_in[...])
    hid = jnp.maximum(pre, 0.0).astype(BF16)
    emb = nn(hid, w_out[...])
    inv = lax.rsqrt(jnp.sum(emb * emb, axis=-1, keepdims=True) + NORM_EPS)
    unit = emb * inv
    out[0] = unit.astype(BF16)
    pre_s[...] = pre
    hid_s[...] = hid
    inv_s[...] = jnp.broadcast_to(inv, unit.shape)
    unit_s[...] = unit


def backward(x, w_out, pre_s, hid_s, inv_s, unit_s, d_unit):
    unit = unit_s[...]
    d_emb = inv_s[...] * (d_unit - unit * jnp.sum(unit * d_unit, axis=-1, keepdims=True))
    d_emb = d_emb.astype(BF16)
    g_out = tn(hid_s[...], d_emb)
    d_hid = nt(d_emb, w_out[...])
    d_pre = jnp.where(pre_s[...] > 0, d_hid, 0.0).astype(BF16)
    g_in = tn(x[...], d_pre)
    return g_in, g_out


def kernel(total_rows, qx, vx, lq, wqi, wqo, wvi, wvo,
           loss_o, gqi_o, gqo_o, gvi_o, gvo_o,
           u_all, v_all, lq_all, kcol, e_all, zacc, zs, rz, dut, dur, dvs, dvr,
           q_pre, q_hid, q_inv, q_unit, v_pre, v_hid, v_inv, v_unit,
           gq, gv, pq, pv, hq, hv, rq, rv, oq, ov, xq, xv, fq, fv,
           us, ur, vs, vr, ls, lr, zss, zsr, dus, durs, dvss, dvsr,
           ps, pr, r1s, r1r, r2s, r2r, r3s, r3r, r4s, r4r):
    me = lax.axis_index("dp")
    core = me % 2
    x = (me // 2) % 4
    y = (me // 8) % 4
    z = me // 32
    lo = ((z + 1) // 2) % 2
    hi = z // 2
    scale = 1.0 / (TEMP * total_rows)

    def a_dev(s):
        zz = z + (s % 2) * (1 - 2 * (z % 2))
        return zz * 32 + ((y + STEP[s // 2]) % 4) * 8 + x * 2 + core

    def b_dev(t):
        i = t // 4
        step = STEP[i] if isinstance(t, int) else i + (i // 2) * (1 - 2 * (i % 2))
        zz = z + ((t // 2) % 2) * (3 - 2 * z)
        return zz * 32 + y * 8 + ((x + step) % 4) * 2 + (core + t % 2) % 2

    def copy(src, dst, ssem, rsem, dev):
        return pltpu.make_async_remote_copy(src_ref=src, dst_ref=dst, send_sem=ssem, recv_sem=rsem,
                                            device_id=(dev,), device_id_type=pl.DeviceIdType.MESH)

    sent = []

    def send(src, dst, ssem, rsem, dev):
        c = copy(src, dst, ssem, rsem, dev)
        c.start()
        sent.append(c)

    def arrived(dst, ssem, rsem):
        copy(dst, dst, ssem, rsem, me).wait_recv()

    barrier = pltpu.get_barrier_semaphore()
    for s in range(1, NA):
        pl.semaphore_signal(barrier, inc=1, device_id=(a_dev(s),), device_id_type=pl.DeviceIdType.MESH)
    for t in range(1, NB):
        pl.semaphore_signal(barrier, inc=1, device_id=(b_dev(t),), device_id_type=pl.DeviceIdType.MESH)

    forward(vx, wvi, wvo, v_pre, v_hid, v_inv, v_unit, v_all)
    pl.semaphore_wait(barrier, NA + NB - 2)
    for t in range(1, NB):
        send(lq, lq_all.at[INV_B[t]], ls.at[t], lr.at[INV_B[t]], b_dev(t))
    forward(qx, wqi, wqo, q_pre, q_hid, q_inv, q_unit, u_all)
    for t in range(1, NB):
        send(v_all.at[0], v_all.at[INV_B[t]], vs.at[t], vr.at[INV_B[t]], b_dev(t))
        if t % 2 == 1:
            s = t // 2
            if s >= 1:
                send(u_all.at[0], u_all.at[INV_A[s]], us.at[s], ur.at[INV_A[s]], a_dev(s))
    lq_all[0] = lq[...]
    zacc[...] = jnp.zeros_like(zacc)

    low = lq[...]
    for t in range(1, NB):
        arrived(lq_all.at[t], ls.at[t], lr.at[t])
        low = jnp.minimum(low, lq_all[t])
    low = jnp.min(low, axis=1, keepdims=True)

    def column(t, c):
        row = LOG2E * ((lq_all[t] - low) + BOUND)
        kcol[t] = jnp.transpose(jnp.broadcast_to(row, (128, 256)))
        return c

    lax.fori_loop(0, NB, column, 0)
    for s in range(1, NA):
        arrived(u_all.at[s], us.at[s], ur.at[s])

    c2 = LOG2E / TEMP

    def logits(t, c):
        @pl.when(t > 0)
        def _():
            arrived(v_all.at[t], vs.at[t], vr.at[t])

        vt = v_all[t]
        kc = kcol[t]
        kc = jnp.concatenate([kc, kc], axis=1)
        for s in range(NA):
            e = jnp.exp2(nt(vt, u_all[s]) * c2 - kc)
            e_all[t, s] = e
            zacc[s] += jnp.sum(e.reshape(32, 8, 256), axis=0)
        return c

    lax.fori_loop(0, NB, logits, 0)

    rows = [jnp.sum(zacc[s], axis=0, keepdims=True) for s in range(NA)]
    zs[0] = jnp.concatenate(rows + [jnp.broadcast_to(low, (8, 256))], axis=0)
    eye = lax.broadcasted_iota(jnp.int32, (256, 256), 0) == lax.broadcasted_iota(jnp.int32, (256, 256), 1)
    dots = jnp.sum(jnp.where(eye, nt(v_all[0], u_all[0]), 0.0), axis=0, keepdims=True)
    for s in range(1, NA):
        send(zs.at[0], zs.at[INV_A[s]], zss.at[s], zsr.at[INV_A[s]], a_dev(s))
    for s in range(1, NA):
        arrived(zs.at[s], zss.at[s], zsr.at[s])

    lows = [zs[s, 8:9, :] for s in range(NA)]
    least = functools.reduce(jnp.minimum, lows)
    fac = [jnp.exp(least - w) for w in lows]
    tot = []
    for r in range(NA):
        acc = None
        for s in range(NA):
            k = rel_a(r, s)
            term = fac[s] * zs[s, k:k + 1, :]
            acc = term if acc is None else acc + term
        tot.append(acc)
    for r in range(NA):
        rz[r:r + 1, :] = fac[0] / tot[r]
    loss_rows = ((BOUND - least) + jnp.log(tot[0])) - (dots / TEMP - lq[...])
    loss_loc = jnp.sum(loss_rows, axis=1, keepdims=True)

    def grads(t, diag):
        vt = v_all[t]
        dv = None
        for s in range(NA):
            p = e_all[t, s] * rz[s:s + 1, :]
            if diag and s == 0:
                p = jnp.where(eye, p - 1.0, p)
            g = p.astype(BF16)
            d = nn(g, u_all[s])
            dv = d if dv is None else dv + d
            du = tn(vt, g)
            if diag:
                dut[s] = du
            else:
                dut[s] += du
        dvs[t] = dv

    def dv_copy(t):
        i = t // 4
        back = i + ((i + 1) // 2) * (3 - 2 * i) * (1 - i // 3)
        slot = 4 * back + t % 4
        return copy(dvs.at[t], dvr.at[slot], dvss.at[t], dvsr.at[slot], b_dev(t))

    grads(0, True)

    def step(t, c):
        grads(t, False)

        @pl.when(t > 1)
        def _():
            dv_copy(t - 1).start()
        return c

    lax.fori_loop(1, NB, step, 0)
    for s in range(1, NA):
        send(dut.at[s], dur.at[INV_A[s]], dus.at[s], durs.at[INV_A[s]], a_dev(s))
    dv_copy(jnp.int32(NB - 1)).start()

    du = dut[0]
    for s in range(1, NA):
        arrived(dur.at[s], dus.at[s], durs.at[s])
        du = du + dur[s]
    d_unit = jnp.transpose(du) * scale
    g_in, g_out = backward(qx, wqo, q_pre, q_hid, q_inv, q_unit, d_unit)

    def pack(buf, g_in, g_out):
        buf[0, 0:512, :] = g_in[:, 0:128]
        buf[0, 512:640, :] = g_in[0:128, 128:256]
        buf[1, 0:384, :] = g_in[128:512, 128:256]
        buf[1, 384:640, :] = g_out

    pack(gq, g_in, g_out)
    lt = jnp.broadcast_to(loss_loc, (8, 128))
    gq[0, 640:648, :] = lt
    gq[1, 640:648, :] = lt
    send(gq.at[(core + 1) % 2], pq, ps.at[0], pr.at[0], b_dev(1))

    def add_dv(t, acc):
        arrived(dvr.at[t], dvss.at[t], dvsr.at[t])
        return acc + dvr[t]

    dv = lax.fori_loop(1, NB, add_dv, dvs[0])
    g_in, g_out = backward(vx, wvo, v_pre, v_hid, v_inv, v_unit, dv * scale)
    pack(gv, g_in, g_out)
    send(gv.at[(core + 1) % 2], pv, ps.at[1], pr.at[1], b_dev(1))

    a_me, b_me = y * 2 + lo, x * 2 + hi

    def a_idx(s):
        return ((y + STEP[s // 2]) % 4) * 2 + (lo + s % 2) % 2

    def c_idx(t):
        return ((x + STEP[t // 2]) % 4) * 2 + (hi + t % 2) % 2

    def c_dev(t):
        return b_dev(2 * t)

    paths = (
        (gq, pq, hq, rq, oq, xq, fq, c_dev, c_idx, b_me, a_dev, 88, 0),
        (gv, pv, hv, rv, ov, xv, fv, a_dev, a_idx, a_me, c_dev, 80, 1),
    )
    for g, p, h, r, o, xx, f, dev1, idx1, mine, dev2, n, w in paths:
        arrived(p, ps.at[w], pr.at[w])
        h[:, 0:80, :] = (g[core, 0:640, :] + p[0:640, :]).reshape(8, 80, 128)
        if n > 80:
            extra = g[core, 640:648, :] + p[640:648, :]
            for k in range(8):
                h[k, 80:88, :] = extra
        for s in range(1, 8):
            k = INV_A[s]
            send(h.at[idx1(s)], r.at[k], r1s.at[w, s], r1r.at[w, k], dev1(s))
    for g, p, h, r, o, xx, f, dev1, idx1, mine, dev2, n, w in paths:
        acc = h[mine]
        for s in range(1, 8):
            arrived(r.at[s], r1s.at[w, s], r1r.at[w, s])
            acc = acc + r[s]
        o[...] = acc
        for s in range(1, 8):
            k = INV_A[s]
            send(o, xx.at[k], r2s.at[w, s], r2r.at[w, k], dev2(s))
    for g, p, h, r, o, xx, f, dev1, idx1, mine, dev2, n, w in paths:
        acc = o[...]
        for s in range(1, 8):
            arrived(xx.at[s], r2s.at[w, s], r2r.at[w, s])
            acc = acc + xx[s]
        f[core, mine] = acc
        for s in range(1, 8):
            k = INV_A[s]
            send(f.at[core, mine], f.at[core, mine], r3s.at[w, s], r3r.at[w, k], dev1(s))
        send(f.at[core, mine], f.at[core, mine], r4s.at[w, 0], r4r.at[w, 0], b_dev(1))
        if n > 80:
            loss_o[0] = acc[80, 0] * (1.0 / total_rows)
    other = (core + 1) % 2
    for g, p, h, r, o, xx, f, dev1, idx1, mine, dev2, n, w in paths:
        for s in range(1, 8):
            k = idx1(s)
            arrived(f.at[core, k], r3s.at[w, s], r3r.at[w, s])
            send(f.at[core, k], f.at[core, k], r4s.at[w, s], r4r.at[w, s], b_dev(1))
    for g, p, h, r, o, xx, f, dev1, idx1, mine, dev2, n, w in paths:
        arrived(f.at[other, mine], r4s.at[w, 0], r4r.at[w, 0])
        for s in range(1, 8):
            arrived(f.at[other, idx1(s)], r4s.at[w, s], r4r.at[w, s])
        go_in, go_out = (gqi_o, gqo_o) if w == 0 else (gvi_o, gvo_o)
        first = f[0, :, 0:80, :].reshape(640, 128)
        second = f[1, :, 0:80, :].reshape(640, 128)
        go_in[:, 0:128] = first[0:512]
        go_in[0:128, 128:256] = first[512:640]
        go_in[128:512, 128:256] = second[0:384]
        go_out[...] = second[384:640]

    for c in sent:
        c.wait_send()

    def drain(t, c):
        dv_copy(t).wait_send()
        return c

    lax.fori_loop(1, NB, drain, 0)


def solution(mesh):
    group = mesh.shape["dp"]

    def local_step(query_feat, item_feat, log_q, w_query_in, w_query_out, w_item_in, w_item_out):
        local_rows = query_feat.shape[0]
        vm = lambda *s: pltpu.VMEM(s, F32)
        vb = lambda *s: pltpu.VMEM(s, BF16)
        sem = lambda *s: pltpu.SemaphoreType.DMA(s)
        scratch = [
            vb(NA, 256, 128), vb(NB, 256, 128), vm(NB, 1, 256), vm(NB, 256, 128), vm(NB, NA, 256, 256),
            vm(NA, 8, 256), vm(NA, 16, 256), vm(NA, 256), vm(NA, 128, 256), vm(NA, 128, 256),
            vm(NB, 256, 128), vm(NB, 256, 128),
            vm(256, 256), vb(256, 256), vm(256, 128), vm(256, 128),
            vm(256, 256), vb(256, 256), vm(256, 128), vm(256, 128),
            vm(2, 648, 128), vm(2, 640, 128), vm(648, 128), vm(640, 128),
            vm(8, 88, 128), vm(8, 80, 128), vm(8, 88, 128), vm(8, 80, 128),
            vm(88, 128), vm(80, 128), vm(8, 88, 128), vm(8, 80, 128),
            vm(2, 8, 88, 128), vm(2, 8, 80, 128),
            sem(NA), sem(NA), sem(NB), sem(NB), sem(NB), sem(NB), sem(NA), sem(NA),
            sem(NA), sem(NA), sem(NB), sem(NB),
            sem(2), sem(2), sem(2, 8), sem(2, 8), sem(2, 8), sem(2, 8), sem(2, 8), sem(2, 8), sem(2, 8), sem(2, 8),
        ]
        vspec = pl.BlockSpec(memory_space=pltpu.VMEM)
        return pl.pallas_call(
            functools.partial(kernel, local_rows * group),
            out_shape=(jax.ShapeDtypeStruct((1,), F32),
                       jax.ShapeDtypeStruct((512, 256), F32), jax.ShapeDtypeStruct((256, 128), F32),
                       jax.ShapeDtypeStruct((512, 256), F32), jax.ShapeDtypeStruct((256, 128), F32)),
            in_specs=[vspec] * 7,
            out_specs=(pl.BlockSpec(memory_space=pltpu.SMEM), vspec, vspec, vspec, vspec),
            scratch_shapes=scratch,
            compiler_params=pltpu.CompilerParams(collective_id=0, has_side_effects=True,
                                                 vmem_limit_bytes=62 * 1024 * 1024),
        )(query_feat, item_feat, log_q.reshape(1, local_rows), w_query_in, w_query_out, w_item_in, w_item_out)

    return jax.shard_map(local_step, mesh=mesh,
                         in_specs=(P("dp", None), P("dp", None), P("dp"), P(), P(), P(), P()),
                         out_specs=(P(), P(), P(), P(), P()), check_vma=False)
```

```python
import functools

import jax
import jax.numpy as jnp
from jax import lax
from jax.experimental import pallas as pl
from jax.experimental.pallas import tpu as pltpu
from jax.sharding import PartitionSpec as P

TEMP = 0.05
NORM_EPS = 1e-6
LOG2E = 1.4426950408889634
BOUND = 20.25
F32 = jnp.float32
BF16 = jnp.bfloat16
NA, NB, NC = 8, 16, 8
STEP = (0, 1, 3, 2)
BACK = (0, 2, 1, 3)
INV_A = [2 * BACK[s // 2] + s % 2 for s in range(NA)]
INV_B = [4 * BACK[t // 4] + t % 4 for t in range(NB)]


def rel_a(r, s):
    dy = (STEP[r // 2] - STEP[s // 2]) % 4
    return 2 * STEP.index(dy) + (r % 2 + s % 2) % 2


def nt(a, b):
    return lax.dot_general(a, b, (((1,), (1,)), ((), ())), preferred_element_type=F32)


def tn(a, b):
    return lax.dot_general(a, b, (((0,), (0,)), ((), ())), preferred_element_type=F32)


def nn(a, b):
    return jnp.dot(a, b, preferred_element_type=F32)


def forward(x, w_in, w_out, pre_s, hid_s, inv_s, unit_s):
    pre = nn(x[...], w_in[...])
    hid = jnp.maximum(pre, 0.0).astype(BF16)
    emb = nn(hid, w_out[...])
    inv = lax.rsqrt(jnp.sum(emb * emb, axis=-1, keepdims=True) + NORM_EPS)
    unit = emb * inv
    pre_s[...] = pre
    hid_s[...] = hid
    inv_s[...] = jnp.broadcast_to(inv, unit.shape)
    unit_s[...] = unit


def backward(x, w_out, pre_s, hid_s, inv_s, unit_s, d_unit):
    unit = unit_s[...]
    d_emb = inv_s[...] * (d_unit - unit * jnp.sum(unit * d_unit, axis=-1, keepdims=True))
    d_emb = d_emb.astype(BF16)
    g_out = tn(hid_s[...], d_emb)
    d_hid = nt(d_emb, w_out[...])
    d_pre = jnp.where(pre_s[...] > 0, d_hid, 0.0).astype(BF16)
    g_in = tn(x[...], d_pre)
    return g_in, g_out


def kernel(total_rows, qx, vx, lq, wqi, wqo, wvi, wvo,
           loss_o, gqi_o, gqo_o, gvi_o, gvo_o,
           u_all, v_all, lq_all, lows, kcol, e_all, zacc, zs, rz, dut, dur, dvs, dvp, dvc, dvr,
           q_pre, q_hid, q_inv, q_unit, v_pre, v_hid, v_inv, v_unit,
           gq, gv, pq, pv, hq, hv, rq, rv, oq, ov, xq, xv, fq, fv,
           us, ur, vs, vr, ls, lr, lows_s, lows_r, zss, zsr, dus, durs, dvps, dvpr, dvss, dvsr,
           ps, pr, r1s, r1r, r2s, r2r, r3s, r3r, r4s, r4r):
    me = lax.axis_index("dp")
    core = me % 2
    x = (me // 2) % 4
    y = (me // 8) % 4
    z = me // 32
    lo = ((z + 1) // 2) % 2
    hi = z // 2
    scale = 1.0 / (TEMP * total_rows)
    other = (core + 1) % 2
    mate = z * 32 + y * 8 + x * 2 + other

    def a_dev(s):
        zz = z + (s % 2) * (1 - 2 * (z % 2))
        return zz * 32 + ((y + STEP[s // 2]) % 4) * 8 + x * 2 + core

    def c_dev(t, flip=0):
        i = t // 2
        step = STEP[i] if isinstance(t, int) else i + (i // 2) * (1 - 2 * (i % 2))
        zz = z + (t % 2) * (3 - 2 * z)
        return zz * 32 + y * 8 + ((x + step) % 4) * 2 + (core + flip) % 2

    def back_c(t):
        i = t // 2
        return 2 * (i + ((i + 1) // 2) * (3 - 2 * i) * (1 - i // 3)) + t % 2

    def copy(src, dst, ssem, rsem, dev):
        return pltpu.make_async_remote_copy(src_ref=src, dst_ref=dst, send_sem=ssem, recv_sem=rsem,
                                            device_id=(dev,), device_id_type=pl.DeviceIdType.MESH)

    sent = []

    def send(src, dst, ssem, rsem, dev):
        c = copy(src, dst, ssem, rsem, dev)
        c.start()
        sent.append(c)

    def arrived(dst, ssem, rsem):
        copy(dst, dst, ssem, rsem, me).wait_recv()

    barrier = pltpu.get_barrier_semaphore()
    partners = [a_dev(s) for s in range(1, NA)] + [c_dev(t // 2, t % 2) for t in range(1, NB)]
    for dev in partners:
        pl.semaphore_signal(barrier, inc=1, device_id=(dev,), device_id_type=pl.DeviceIdType.MESH)

    forward(vx, wvi, wvo, v_pre, v_hid, v_inv, v_unit)
    v_all[0] = v_unit[...].astype(BF16)
    pl.semaphore_wait(barrier, len(partners))
    for t in range(1, NB):
        send(lq, lq_all.at[INV_B[t]], ls.at[t], lr.at[INV_B[t]], c_dev(t // 2, t % 2))
    forward(qx, wqi, wqo, q_pre, q_hid, q_inv, q_unit)
    ub = q_unit[...].astype(BF16)
    u_all[0, 0] = ub[0:128]
    u_all[1, 0] = ub[128:256]
    send(v_all.at[0], v_all.at[1], vs.at[1], vr.at[1], mate)
    for t in range(1, NC):
        k = INV_A[t]
        send(v_all.at[0], v_all.at[2 * k], vs.at[2 * t], vr.at[2 * k], c_dev(t))
        send(u_all.at[0, 0], u_all.at[0, k], us.at[0, t], ur.at[0, k], a_dev(t))
    for t in range(1, NA):
        k = INV_A[t]
        send(u_all.at[1, 0], u_all.at[1, k], us.at[1, t], ur.at[1, k], a_dev(t))
    lq_all[0] = lq[...]
    zacc[...] = jnp.zeros_like(zacc)

    low = lq[...]
    for t in range(1, NB):
        arrived(lq_all.at[t], ls.at[t], lr.at[t])
        low = jnp.minimum(low, lq_all[t])
    low = jnp.min(low, axis=1, keepdims=True)
    lows[0] = jnp.broadcast_to(low, (1, 128))

    def column(t, c):
        row = LOG2E * ((lq_all[t] - low) + BOUND)
        kcol[t] = jnp.transpose(jnp.broadcast_to(row, (128, 256)))
        return c

    lax.fori_loop(0, NB, column, 0)
    for s in range(1, NA):
        send(lows.at[0], lows.at[INV_A[s]], lows_s.at[s], lows_r.at[INV_A[s]], a_dev(s))
    for s in range(1, NA):
        arrived(u_all.at[0, s], us.at[0, s], ur.at[0, s])

    c2 = LOG2E / TEMP

    def logits(t, h):
        vt = v_all[t]
        kc = kcol[t]
        kc = jnp.concatenate([kc, kc], axis=1)
        for m in range(4):
            um = u_all[h, 2 * m:2 * m + 2].reshape(256, 128)
            e = jnp.exp2(nt(vt, um) * c2 - kc)
            e_all[t, h, m] = e
            zacc[h, m] += jnp.sum(e.reshape(32, 8, 256), axis=0)

    def first(n, c):
        arrived(v_all.at[2 * n], vs.at[2 * n], vr.at[2 * n])
        copy(v_all.at[2 * n], v_all.at[2 * n + 1], vs.at[2 * n + 1], vr.at[2 * n + 1], mate).start()
        logits(2 * n, 0)
        arrived(v_all.at[2 * n - 1], vs.at[2 * n - 1], vr.at[2 * n - 1])
        logits(2 * n - 1, 0)
        return c

    def share(h):
        rows = []
        for m in range(4):
            row = jnp.sum(zacc[h, m], axis=0, keepdims=True)
            rows += [row[:, 0:128], row[:, 128:256]]
        zs[h, 0] = jnp.concatenate(rows, axis=0)

    def share_send(h):
        for s in range(1, NA):
            send(zs.at[h, 0], zs.at[h, INV_A[s]], zss.at[h, s], zsr.at[h, INV_A[s]], a_dev(s))

    logits(0, 0)
    lax.fori_loop(1, NC, first, 0)
    arrived(v_all.at[NB - 1], vs.at[NB - 1], vr.at[NB - 1])
    logits(NB - 1, 0)
    share(0)
    for s in range(1, NA):
        arrived(u_all.at[1, s], us.at[1, s], ur.at[1, s])
    share_send(0)

    def second(n, c):
        logits(2 * n, 1)
        logits(2 * n + 1, 1)
        return c

    lax.fori_loop(0, NC, second, 0)
    share(1)

    ji = lax.broadcasted_iota(jnp.int32, (256, 256), 0)
    qi = lax.broadcasted_iota(jnp.int32, (256, 256), 1)
    own = q_unit[...].astype(BF16).astype(F32) * v_unit[...].astype(BF16).astype(F32)
    pos = jnp.sum(own) / TEMP
    share_send(1)

    def combine(h):
        for s in range(1, NA):
            arrived(zs.at[h, s], zss.at[h, s], zsr.at[h, s])
        tot = []
        for r in range(NA):
            acc = None
            for s in range(NA):
                k = rel_a(r, s)
                term = fac[s] * zs[h, s, k:k + 1, :]
                acc = term if acc is None else acc + term
            tot.append(acc)
        inv = [fac[0] / w for w in tot]
        for m in range(4):
            rz[h, m] = jnp.concatenate([inv[2 * m], inv[2 * m + 1]], axis=1)
        return jnp.log(tot[0])

    def grads(t, h, diag):
        vt = v_all[t]
        dv = None
        for m in range(4):
            p = e_all[t, h, m] * rz[h, m]
            if diag and m == 0:
                p = jnp.where((ji == qi + h * 128) & (qi < 128), p - 1.0, p)
            g = p.astype(BF16)
            d = nn(g, u_all[h, 2 * m:2 * m + 2].reshape(256, 128))
            dv = d if dv is None else dv + d
            du = tn(vt, g)
            if diag:
                dut[h, 2 * m] = du[:, 0:128]
                dut[h, 2 * m + 1] = du[:, 128:256]
            else:
                dut[h, 2 * m] += du[:, 0:128]
                dut[h, 2 * m + 1] += du[:, 128:256]
        if h == 0:
            dvs[t] = dv
        else:
            dvs[t] += dv

    for s in range(1, NA):
        arrived(lows.at[s], lows_s.at[s], lows_r.at[s])
    lowv = [lows[s] for s in range(NA)]
    least = functools.reduce(jnp.minimum, lowv)
    fac = [jnp.exp(least - w) for w in lowv]
    log0 = combine(0)
    grads(0, 0, True)
    grads(1, 0, False)

    def third(n, c):
        grads(2 * n, 0, False)
        grads(2 * n + 1, 0, False)
        return c

    lax.fori_loop(1, NC, third, 0)
    log1 = combine(1)
    for s in range(1, NA):
        send(dut.at[0, s], dur.at[0, INV_A[s]], dus.at[0, s], durs.at[0, INV_A[s]], a_dev(s))

    def mate_copy(t):
        return copy(dvs.at[2 * t + 1], dvp.at[t], dvps.at[t], dvpr.at[t], mate)

    def dv_copy(t):
        return copy(dvc.at[t], dvr.at[back_c(t)], dvss.at[t], dvsr.at[back_c(t)], c_dev(t))

    def dv_sum(t):
        arrived(dvp.at[t], dvps.at[t], dvpr.at[t])
        dvc[t] = dvs[2 * t] + dvp[t]

    grads(0, 1, True)

    def fourth(n, c):
        grads(2 * n + 1, 1, False)

        @pl.when(n > 2)
        def _():
            dv_sum(n - 2)

        grads(2 * n, 1, False)
        mate_copy(n).start()

        @pl.when(n > 2)
        def _():
            dv_copy(n - 2).start()
        return c

    lax.fori_loop(1, NC, fourth, 0)
    grads(1, 1, False)
    for s in range(1, NA):
        send(dut.at[1, s], dur.at[1, INV_A[s]], dus.at[1, s], durs.at[1, INV_A[s]], a_dev(s))
    mate_copy(0).start()
    dv_sum(NC - 2)
    dv_sum(NC - 1)
    dv_copy(jnp.int32(NC - 2)).start()
    loss_rows = ((BOUND - least) * 2.0 + log0 + log1) + (lq[:, 0:128] + lq[:, 128:256])
    loss_loc = jnp.sum(loss_rows, axis=1, keepdims=True) - pos
    dv_copy(jnp.int32(NC - 1)).start()
    dv_sum(0)

    parts = []
    for h in range(2):
        du = dut[h, 0]
        for s in range(1, NA):
            arrived(dur.at[h, s], dus.at[h, s], durs.at[h, s])
            du = du + dur[h, s]
        parts.append(jnp.transpose(du))
    d_unit = jnp.concatenate(parts, axis=0) * scale
    g_in, g_out = backward(qx, wqo, q_pre, q_hid, q_inv, q_unit, d_unit)

    def pack(buf, g_in, g_out):
        buf[0, 0:512, :] = g_in[:, 0:128]
        buf[0, 512:640, :] = g_in[0:128, 128:256]
        buf[1, 0:384, :] = g_in[128:512, 128:256]
        buf[1, 384:640, :] = g_out

    pack(gq, g_in, g_out)
    lt = jnp.broadcast_to(loss_loc, (8, 128))
    gq[0, 640:648, :] = lt
    gq[1, 640:648, :] = lt
    send(gq.at[other], pq, ps.at[0], pr.at[0], mate)

    def add_dv(t, acc):
        arrived(dvr.at[t], dvss.at[t], dvsr.at[t])
        return acc + dvr[t]

    dv = lax.fori_loop(1, NC, add_dv, dvc[0])
    g_in, g_out = backward(vx, wvo, v_pre, v_hid, v_inv, v_unit, dv * scale)
    pack(gv, g_in, g_out)
    send(gv.at[other], pv, ps.at[1], pr.at[1], mate)

    a_me, b_me = y * 2 + lo, x * 2 + hi

    def a_idx(s):
        return ((y + STEP[s // 2]) % 4) * 2 + (lo + s % 2) % 2

    def c_idx(t):
        return ((x + STEP[t // 2]) % 4) * 2 + (hi + t % 2) % 2

    paths = (
        (gq, pq, hq, rq, oq, xq, fq, c_dev, c_idx, b_me, a_dev, 88, 0),
        (gv, pv, hv, rv, ov, xv, fv, a_dev, a_idx, a_me, c_dev, 80, 1),
    )
    for g, p, h, r, o, xx, f, dev1, idx1, mine, dev2, n, w in paths:
        arrived(p, ps.at[w], pr.at[w])
        h[:, 0:80, :] = (g[core, 0:640, :] + p[0:640, :]).reshape(8, 80, 128)
        if n > 80:
            extra = g[core, 640:648, :] + p[640:648, :]
            for k in range(8):
                h[k, 80:88, :] = extra
        for s in range(1, 8):
            k = INV_A[s]
            send(h.at[idx1(s)], r.at[k], r1s.at[w, s], r1r.at[w, k], dev1(s))
    for g, p, h, r, o, xx, f, dev1, idx1, mine, dev2, n, w in paths:
        acc = h[mine]
        for s in range(1, 8):
            arrived(r.at[s], r1s.at[w, s], r1r.at[w, s])
            acc = acc + r[s]
        o[...] = acc
        for s in range(1, 8):
            k = INV_A[s]
            send(o, xx.at[k], r2s.at[w, s], r2r.at[w, k], dev2(s))
    for g, p, h, r, o, xx, f, dev1, idx1, mine, dev2, n, w in paths:
        acc = o[...]
        for s in range(1, 8):
            arrived(xx.at[s], r2s.at[w, s], r2r.at[w, s])
            acc = acc + xx[s]
        f[core, mine] = acc
        for s in range(1, 8):
            k = INV_A[s]
            send(f.at[core, mine], f.at[core, mine], r3s.at[w, s], r3r.at[w, k], dev1(s))
        send(f.at[core, mine], f.at[core, mine], r4s.at[w, 0], r4r.at[w, 0], mate)
        if n > 80:
            loss_o[0] = acc[80, 0] * (1.0 / total_rows)
    for g, p, h, r, o, xx, f, dev1, idx1, mine, dev2, n, w in paths:
        for s in range(1, 8):
            k = idx1(s)
            arrived(f.at[core, k], r3s.at[w, s], r3r.at[w, s])
            send(f.at[core, k], f.at[core, k], r4s.at[w, s], r4r.at[w, s], mate)
    for g, p, h, r, o, xx, f, dev1, idx1, mine, dev2, n, w in paths:
        arrived(f.at[other, mine], r4s.at[w, 0], r4r.at[w, 0])
        for s in range(1, 8):
            arrived(f.at[other, idx1(s)], r4s.at[w, s], r4r.at[w, s])
        go_in, go_out = (gqi_o, gqo_o) if w == 0 else (gvi_o, gvo_o)
        head = f[0, :, 0:80, :].reshape(640, 128)
        tail = f[1, :, 0:80, :].reshape(640, 128)
        go_in[:, 0:128] = head[0:512]
        go_in[0:128, 128:256] = head[512:640]
        go_in[128:512, 128:256] = tail[0:384]
        go_out[...] = tail[384:640]

    for c in sent:
        c.wait_send()

    def drain(t, c):
        copy(v_all.at[2 * t], v_all.at[2 * t + 1], vs.at[2 * t + 1], vr.at[2 * t + 1], mate).wait_send()
        mate_copy(t).wait_send()
        dv_copy(t).wait_send()
        return c

    lax.fori_loop(1, NC, drain, 0)
    mate_copy(0).wait_send()


def emit(*refs):
    sem = refs[-1]
    copies = [pltpu.make_async_copy(refs[i], refs[4 + i], sem.at[i]) for i in range(4)]
    for c in copies:
        c.start()
    for c in copies:
        c.wait()


def solution(mesh):
    group = mesh.shape["dp"]

    def local_step(query_feat, item_feat, log_q, w_query_in, w_query_out, w_item_in, w_item_out):
        local_rows = query_feat.shape[0]
        vm = lambda *s: pltpu.VMEM(s, F32)
        vb = lambda *s: pltpu.VMEM(s, BF16)
        sem = lambda *s: pltpu.SemaphoreType.DMA(s)
        scratch = [
            vb(2, NA, 128, 128), vb(NB, 256, 128), vm(NB, 1, 256), vm(NA, 1, 128), vm(NB, 256, 128),
            vm(NB, 2, 4, 256, 256), vm(2, 4, 8, 256), vm(2, NA, 8, 128), vm(2, 4, 1, 256),
            vm(2, NA, 128, 128), vm(2, NA, 128, 128),
            vm(NB, 256, 128), vm(NC, 256, 128), vm(NC, 256, 128), vm(NC, 256, 128),
            vm(256, 256), vb(256, 256), vm(256, 128), vm(256, 128),
            vm(256, 256), vb(256, 256), vm(256, 128), vm(256, 128),
            vm(2, 648, 128), vm(2, 640, 128), vm(648, 128), vm(640, 128),
            vm(8, 88, 128), vm(8, 80, 128), vm(8, 88, 128), vm(8, 80, 128),
            vm(88, 128), vm(80, 128), vm(8, 88, 128), vm(8, 80, 128),
            vm(2, 8, 88, 128), vm(2, 8, 80, 128),
            sem(2, NA), sem(2, NA), sem(NB), sem(NB), sem(NB), sem(NB), sem(NA), sem(NA), sem(2, NA), sem(2, NA),
            sem(2, NA), sem(2, NA), sem(NC), sem(NC), sem(NC), sem(NC),
            sem(2), sem(2), sem(2, 8), sem(2, 8), sem(2, 8), sem(2, 8), sem(2, 8), sem(2, 8), sem(2, 8), sem(2, 8),
        ]
        vspec = pl.BlockSpec(memory_space=pltpu.VMEM)
        shapes = ((512, 256), (256, 128), (512, 256), (256, 128))
        loss, *grads = pl.pallas_call(
            functools.partial(kernel, local_rows * group),
            out_shape=(jax.ShapeDtypeStruct((1,), F32), *[pltpu.VMEM(s, F32) for s in shapes]),
            in_specs=[vspec] * 7,
            out_specs=(pl.BlockSpec(memory_space=pltpu.SMEM), vspec, vspec, vspec, vspec),
            scratch_shapes=scratch,
            compiler_params=pltpu.CompilerParams(collective_id=0, has_side_effects=True,
                                                 vmem_limit_bytes=56 * 1024 * 1024),
        )(query_feat, item_feat, log_q.reshape(1, local_rows), w_query_in, w_query_out, w_item_in, w_item_out)
        anys = pl.BlockSpec(memory_space=pl.ANY)
        grads = pl.pallas_call(
            emit,
            out_shape=tuple(jax.ShapeDtypeStruct(s, F32) for s in shapes),
            in_specs=[vspec] * 4,
            out_specs=(anys,) * 4,
            scratch_shapes=[sem(4)],
            compiler_params=pltpu.CompilerParams(vmem_limit_bytes=1024 * 1024),
        )(*grads)
        return (loss, *grads)

    return jax.shard_map(local_step, mesh=mesh,
                         in_specs=(P("dp", None), P("dp", None), P("dp"), P(), P(), P(), P()),
                         out_specs=(P(), P(), P(), P(), P()), check_vma=False)
```

```python
import functools

import jax
import jax.numpy as jnp
from jax import lax
from jax.experimental import pallas as pl
from jax.experimental.pallas import tpu as pltpu
from jax.sharding import PartitionSpec as P

TEMP = 0.05
NORM_EPS = 1e-6
LOG2E = 1.4426950408889634
BOUND = 20.25
F32 = jnp.float32
BF16 = jnp.bfloat16
NA, NB, NC = 8, 16, 8
STEP = (0, 1, 3, 2)
BACK = (0, 2, 1, 3)
FAR = (7, 6, 3, 5, 2, 4, 1)
INV_A = [2 * BACK[s // 2] + s % 2 for s in range(NA)]
INV_B = [4 * BACK[t // 4] + t % 4 for t in range(NB)]


def rel_a(r, s):
    dy = (STEP[r // 2] - STEP[s // 2]) % 4
    return 2 * STEP.index(dy) + (r % 2 + s % 2) % 2


def nt(a, b):
    return lax.dot_general(a, b, (((1,), (1,)), ((), ())), preferred_element_type=F32)


def tn(a, b):
    return lax.dot_general(a, b, (((0,), (0,)), ((), ())), preferred_element_type=F32)


def nn(a, b):
    return jnp.dot(a, b, preferred_element_type=F32)


def forward(x, w_in, w_out, pre_s, hid_s, inv_s, unit_s):
    pre = nn(x[...], w_in[...])
    hid = jnp.maximum(pre, 0.0).astype(BF16)
    emb = nn(hid, w_out[...])
    inv = lax.rsqrt(jnp.sum(emb * emb, axis=-1, keepdims=True) + NORM_EPS)
    unit = emb * inv
    pre_s[...] = pre
    hid_s[...] = hid
    inv_s[...] = jnp.broadcast_to(inv, unit.shape)
    unit_s[...] = unit


def backward(x, w_out, pre_s, hid_s, inv_s, unit_s, d_unit):
    unit = unit_s[...]
    d_emb = inv_s[...] * (d_unit - unit * jnp.sum(unit * d_unit, axis=-1, keepdims=True))
    d_emb = d_emb.astype(BF16)
    g_out = tn(hid_s[...], d_emb)
    d_hid = nt(d_emb, w_out[...])
    d_pre = jnp.where(pre_s[...] > 0, d_hid, 0.0).astype(BF16)
    g_in = tn(x[...], d_pre)
    return g_in, g_out


def kernel(total_rows, qx_h, vx_h, lq_h, wqi_h, wqo_h, wvi_h, wvo_h,
           loss_o, gqi_o, gqo_o, gvi_o, gvo_o,
           qx, vx, lq, wqi, wqo, wvi, wvo,
           u_all, v_all, lq_all, lows, kcol, e_all, zacc, zs, rz, dut, dur, dvs, dvp, dvc, dvr,
           q_pre, q_hid, q_inv, q_unit, v_pre, v_hid, v_inv, v_unit,
           gq, gv, pq, pv,
           h0, h1, h2, h3, r0, r1, r2, r3, o0, o1, o2, o3, x0, x1, x2, x3, f0, f1, f2, f3,
           ins, us, ur, vs, vr, ls, lr, lows_s, lows_r, zss, zsr, dus, durs, dvps, dvpr, dvss, dvsr,
           ps, pr, rss, rsr):
    me = lax.axis_index("dp")
    core = me % 2
    x = (me // 2) % 4
    y = (me // 8) % 4
    z = me // 32
    lo = ((z + 1) // 2) % 2
    hi = z // 2
    scale = 1.0 / (TEMP * total_rows)
    other = (core + 1) % 2
    mate = z * 32 + y * 8 + x * 2 + other

    def a_dev(s):
        zz = z + (s % 2) * (1 - 2 * (z % 2))
        return zz * 32 + ((y + STEP[s // 2]) % 4) * 8 + x * 2 + core

    def c_dev(t, flip=0):
        i = t // 2
        step = STEP[i] if isinstance(t, int) else i + (i // 2) * (1 - 2 * (i % 2))
        zz = z + (t % 2) * (3 - 2 * z)
        return zz * 32 + y * 8 + ((x + step) % 4) * 2 + (core + flip) % 2

    def back_c(t):
        i = t // 2
        return 2 * (i + ((i + 1) // 2) * (3 - 2 * i) * (1 - i // 3)) + t % 2

    def copy(src, dst, ssem, rsem, dev):
        return pltpu.make_async_remote_copy(src_ref=src, dst_ref=dst, send_sem=ssem, recv_sem=rsem,
                                            device_id=(dev,), device_id_type=pl.DeviceIdType.MESH)

    def send(src, dst, ssem, rsem, dev):
        copy(src, dst, ssem, rsem, dev).start()

    def arrived(dst, rsem):
        copy(dst, dst, rsem, rsem, me).wait_recv()

    def gone(src, ssem):
        copy(src, src, ssem, ssem, me).wait_send()

    barrier = pltpu.get_barrier_semaphore()
    partners = [a_dev(s) for s in range(1, NA)] + [c_dev(t // 2, t % 2) for t in range(1, NB)]
    for dev in partners:
        pl.semaphore_signal(barrier, inc=1, device_id=(dev,), device_id_type=pl.DeviceIdType.MESH)

    loads = [pltpu.make_async_copy(a, b, ins.at[i]) for i, (a, b) in enumerate((
        (vx_h, vx), (wvi_h, wvi), (wvo_h, wvo), (qx_h, qx), (wqi_h, wqi), (wqo_h, wqo), (lq_h, lq)))]
    for c in loads:
        c.start()
    for c in loads[:3]:
        c.wait()
    forward(vx, wvi, wvo, v_pre, v_hid, v_inv, v_unit)
    v_all[0] = v_unit[...].astype(BF16)
    for c in loads[3:]:
        c.wait()
    forward(qx, wqi, wqo, q_pre, q_hid, q_inv, q_unit)
    ub = q_unit[...].astype(BF16)
    u_all[0, 0] = ub[0:128]
    u_all[1, 0] = ub[128:256]
    pl.semaphore_wait(barrier, len(partners))
    for t in (14, 15, 12, 13, 6, 7, 10, 11, 4, 5, 8, 9, 2, 3, 1):
        send(lq, lq_all.at[INV_B[t]], ls, lr, c_dev(t // 2, t % 2))
    send(v_all.at[0], v_all.at[1], vs, vr.at[1], mate)
    for t in FAR:
        k = INV_A[t]
        send(u_all.at[0, 0], u_all.at[0, k], us.at[0], ur.at[0], a_dev(t))
        send(v_all.at[0], v_all.at[2 * k], vs, vr.at[2 * k], c_dev(t))
    for t in FAR:
        k = INV_A[t]
        send(u_all.at[1, 0], u_all.at[1, k], us.at[1], ur.at[1], a_dev(t))
    lq_all[0] = lq[...]
    zacc[...] = jnp.zeros_like(zacc)

    low = lq[...]
    arrived(lq_all.at[1:NB], lr)
    for t in range(1, NB):
        low = jnp.minimum(low, lq_all[t])
    low = jnp.min(low, axis=1, keepdims=True)
    lows[0] = jnp.broadcast_to(low, (1, 128))

    def column(t, c):
        row = LOG2E * ((lq_all[t] - low) + BOUND)
        kcol[t] = jnp.transpose(jnp.broadcast_to(row, (128, 256)))
        return c

    lax.fori_loop(0, NB, column, 0)
    for s in FAR:
        send(lows.at[0], lows.at[INV_A[s]], lows_s, lows_r, a_dev(s))
    arrived(u_all.at[0, 1:NA], ur.at[0])

    c2 = LOG2E / TEMP

    def logits(t, h):
        vt = v_all[t]
        kc = kcol[t]
        kc = jnp.concatenate([kc, kc], axis=1)
        for m in range(4):
            um = u_all[h, 2 * m:2 * m + 2].reshape(256, 128)
            e = jnp.exp2(nt(vt, um) * c2 - kc)
            e_all[t, h, m] = e
            zacc[h, m] += jnp.sum(e.reshape(32, 8, 256), axis=0)

    def first(n, c):
        arrived(v_all.at[2 * n], vr.at[2 * n])
        copy(v_all.at[2 * n], v_all.at[2 * n + 1], vs, vr.at[2 * n + 1], mate).start()
        logits(2 * n, 0)
        arrived(v_all.at[2 * n - 1], vr.at[2 * n - 1])
        logits(2 * n - 1, 0)
        return c

    def share(h):
        rows = []
        for m in range(4):
            row = jnp.sum(zacc[h, m], axis=0, keepdims=True)
            rows += [row[:, 0:128], row[:, 128:256]]
        zs[h, 0] = jnp.concatenate(rows, axis=0)

    def share_send(h):
        for s in FAR:
            send(zs.at[h, 0], zs.at[h, INV_A[s]], zss.at[h], zsr.at[h], a_dev(s))

    logits(0, 0)
    lax.fori_loop(1, NC, first, 0)
    arrived(v_all.at[NB - 1], vr.at[NB - 1])
    logits(NB - 1, 0)
    share(0)
    arrived(u_all.at[1, 1:NA], ur.at[1])
    share_send(0)

    def second(n, c):
        logits(2 * n, 1)
        logits(2 * n + 1, 1)
        return c

    lax.fori_loop(0, NC, second, 0)
    share(1)

    ji = lax.broadcasted_iota(jnp.int32, (256, 256), 0)
    qi = lax.broadcasted_iota(jnp.int32, (256, 256), 1)
    own = q_unit[...].astype(BF16).astype(F32) * v_unit[...].astype(BF16).astype(F32)
    pos = jnp.sum(own) / TEMP
    share_send(1)

    def combine(h):
        arrived(zs.at[h, 1:NA], zsr.at[h])
        tot = []
        for r in range(NA):
            acc = None
            for s in range(NA):
                k = rel_a(r, s)
                term = fac[s] * zs[h, s, k:k + 1, :]
                acc = term if acc is None else acc + term
            tot.append(acc)
        inv = [fac[0] / w for w in tot]
        for m in range(4):
            rz[h, m] = jnp.concatenate([inv[2 * m], inv[2 * m + 1]], axis=1)
        return jnp.log(tot[0])

    def grads(t, h, diag):
        vt = v_all[t]
        dv = None
        for m in range(4):
            p = e_all[t, h, m] * rz[h, m]
            if diag and m == 0:
                p = jnp.where((ji == qi + h * 128) & (qi < 128), p - 1.0, p)
            g = p.astype(BF16)
            d = nn(g, u_all[h, 2 * m:2 * m + 2].reshape(256, 128))
            dv = d if dv is None else dv + d
            du = tn(vt, g)
            if diag:
                dut[h, 2 * m] = du[:, 0:128]
                dut[h, 2 * m + 1] = du[:, 128:256]
            else:
                dut[h, 2 * m] += du[:, 0:128]
                dut[h, 2 * m + 1] += du[:, 128:256]
        if h == 0:
            dvs[t] = dv
        else:
            dvs[t] += dv

    arrived(lows.at[1:NA], lows_r)
    lowv = [lows[s] for s in range(NA)]
    least = functools.reduce(jnp.minimum, lowv)
    fac = [jnp.exp(least - w) for w in lowv]
    log0 = combine(0)
    grads(0, 0, True)
    grads(1, 0, False)

    def third(n, c):
        grads(2 * n, 0, False)
        grads(2 * n + 1, 0, False)
        return c

    lax.fori_loop(1, NC, third, 0)
    log1 = combine(1)
    for s in FAR:
        send(dut.at[0, s], dur.at[0, INV_A[s]], dus.at[0], durs.at[0], a_dev(s))

    def mate_copy(t):
        return copy(dvs.at[2 * t + 1], dvp.at[t], dvps, dvpr.at[t], mate)

    def dv_copy(t):
        return copy(dvc.at[t], dvr.at[back_c(t)], dvss, dvsr, c_dev(t))

    def dv_sum(t):
        arrived(dvp.at[t], dvpr.at[t])
        dvc[t] = dvs[2 * t] + dvp[t]

    grads(0, 1, True)

    def fourth(n, c):
        t = NC - n
        grads(2 * t + 1, 1, False)

        @pl.when(n > 2)
        def _():
            dv_sum(t + 2)

        grads(2 * t, 1, False)
        mate_copy(t).start()

        @pl.when(n > 2)
        def _():
            dv_copy(t + 2).start()
        return c

    lax.fori_loop(1, NC, fourth, 0)
    grads(1, 1, False)
    for s in FAR:
        send(dut.at[1, s], dur.at[1, INV_A[s]], dus.at[1], durs.at[1], a_dev(s))
    mate_copy(0).start()
    dv_sum(2)
    dv_sum(1)
    dv_copy(jnp.int32(2)).start()
    loss_rows = ((BOUND - least) * 2.0 + log0 + log1) + (lq[:, 0:128] + lq[:, 128:256])
    loss_loc = jnp.sum(loss_rows, axis=1, keepdims=True) - pos
    dv_copy(jnp.int32(1)).start()
    dv_sum(0)

    parts = []
    for h in range(2):
        arrived(dur.at[h, 1:NA], durs.at[h])
        du = dut[h, 0]
        for s in range(1, NA):
            du = du + dur[h, s]
        parts.append(jnp.transpose(du))
    d_unit = jnp.concatenate(parts, axis=0) * scale
    g_in, g_out = backward(qx, wqo, q_pre, q_hid, q_inv, q_unit, d_unit)

    def pack(buf, g_in, g_out):
        buf[0, 0:512, :] = g_in[:, 0:128]
        buf[0, 512:640, :] = g_in[0:128, 128:256]
        buf[1, 0:384, :] = g_in[128:512, 128:256]
        buf[1, 384:640, :] = g_out

    pack(gq, g_in, g_out)
    lt = jnp.broadcast_to(loss_loc, (8, 128))
    gq[0, 640:648, :] = lt
    gq[1, 640:648, :] = lt
    send(gq.at[other], pq, ps.at[0], pr.at[0], mate)

    a_me, b_me = y * 2 + lo, x * 2 + hi

    def a_idx(s):
        return ((y + STEP[s // 2]) % 4) * 2 + (lo + s % 2) % 2

    def c_idx(t):
        return ((x + STEP[t // 2]) % 4) * 2 + (hi + t % 2) % 2

    side_a, side_c = (a_dev, a_idx, a_me), (c_dev, c_idx, b_me)
    paths = (
        (0, h0, r0, o0, x0, f0, side_c, side_a),
        (1, h1, r1, o1, x1, f1, side_a, side_c),
        (2, h2, r2, o2, x2, f2, side_a, side_c),
        (3, h3, r3, o3, x3, f3, side_c, side_a),
    )

    def pair(w, g, p):
        arrived(p, pr.at[w])
        for i, h, r, o, xx, f, (dev, idx, mine), _ in paths[2 * w:2 * w + 2]:
            base = 320 * (i % 2)
            h[:, 0:40, :] = (g[core, base:base + 320, :] + p[base:base + 320, :]).reshape(8, 40, 128)
            if i == 0:
                extra = g[core, 640:648, :] + p[640:648, :]
                for n in range(8):
                    h[n, 40:48, :] = extra
        for i, h, r, o, xx, f, (dev, idx, mine), _ in paths[2 * w:2 * w + 2]:
            for s in FAR:
                send(h.at[idx(s)], r.at[INV_A[s]], rss.at[0, i], rsr.at[0, i], dev(s))

    def scatter(w):
        for i, h, r, o, xx, f, (_, _, mine), (dev, _, _) in paths[2 * w:2 * w + 2]:
            arrived(r.at[1:8], rsr.at[0, i])
            acc = h[mine]
            for s in range(1, 8):
                acc = acc + r[s]
            o[...] = acc
            for s in FAR:
                send(o, xx.at[INV_A[s]], rss.at[1, i], rsr.at[1, i], dev(s))

    def exchange(w):
        for i, h, r, o, xx, f, (dev, idx, mine), _ in paths[2 * w:2 * w + 2]:
            arrived(xx.at[1:8], rsr.at[1, i])
            acc = o[...]
            for s in range(1, 8):
                acc = acc + xx[s]
            f[core, mine] = acc
            for s in FAR:
                send(f.at[core, mine], f.at[core, mine], rss.at[2, i], rsr.at[2, i], dev(s))
            if i == 0:
                loss_o[...] = acc[40:48] * (1.0 / total_rows)

    def gather(w):
        for i, h, r, o, xx, f, _, _ in paths[2 * w:2 * w + 2]:
            arrived(r.at[1:8], rsr.at[2, i])
            send(f.at[core], f.at[core], rss.at[3, i], rsr.at[3, i], mate)

    def finish(w, go_in, go_out):
        halves = [[], []]
        for i, h, r, o, xx, f, _, _ in paths[2 * w:2 * w + 2]:
            arrived(h, rsr.at[3, i])
            for c in range(2):
                halves[c].append(f[c, :, 0:40, :].reshape(320, 128))
        head, tail = [jnp.concatenate(c, axis=0) for c in halves]
        go_in[:, 0:128] = head[0:512]
        go_in[0:128, 128:256] = head[512:640]
        go_in[128:512, 128:256] = tail[0:384]
        go_out[...] = tail[384:640]

    pair(0, gq, pq)
    arrived(dvr.at[1:NC], dvsr)
    dv = lax.fori_loop(1, NC, lambda t, acc: acc + dvr[t], dvc[0])
    g_in, g_out = backward(vx, wvo, v_pre, v_hid, v_inv, v_unit, dv * scale)
    pack(gv, g_in, g_out)
    send(gv.at[other], pv, ps.at[1], pr.at[1], mate)
    pair(1, gv, pv)
    scatter(0)
    scatter(1)
    exchange(0)
    exchange(1)
    gather(0)
    finish(0, gqi_o, gqo_o)
    gather(1)
    finish(1, gvi_o, gvo_o)
    gone(lq_all.at[1:NB], ls)
    gone(lows.at[1:NA], lows_s)
    gone(v_all.at[1:NB], vs)
    for h in range(2):
        gone(u_all.at[h, 1:NA], us.at[h])
        gone(zs.at[h, 1:NA], zss.at[h])
        gone(dur.at[h, 1:NA], dus.at[h])
    gone(dvp, dvps)
    gone(dvr.at[1:NC], dvss)
    gone(pq, ps.at[0])
    gone(pv, ps.at[1])
    for i, h, r, o, xx, f, _, _ in paths:
        gone(r.at[1:8], rss.at[0, i])
        gone(xx.at[1:8], rss.at[1, i])
        gone(r.at[1:8], rss.at[2, i])
        gone(h, rss.at[3, i])


def emit(*refs):
    sem = refs[-1]
    copies = [pltpu.make_async_copy(refs[1 + i], refs[6 + i], sem.at[i]) for i in range(4)]
    for c in copies:
        c.start()
    refs[5][0] = refs[0][0, 0]
    for c in copies:
        c.wait()


def solution(mesh):
    group = mesh.shape["dp"]

    def local_step(query_feat, item_feat, log_q, w_query_in, w_query_out, w_item_in, w_item_out):
        local_rows = query_feat.shape[0]
        vm = lambda *s: pltpu.VMEM(s, F32)
        vb = lambda *s: pltpu.VMEM(s, BF16)
        sem = lambda *s: pltpu.SemaphoreType.DMA(s)
        one = pltpu.SemaphoreType.DMA
        scratch = [
            vb(256, 512), vb(256, 512), vm(1, 256), vb(512, 256), vb(256, 128), vb(512, 256), vb(256, 128),
            vb(2, NA, 128, 128), vb(NB, 256, 128), vm(NB, 1, 256), vm(NA, 1, 128), vm(NB, 256, 128),
            vm(NB, 2, 4, 256, 256), vm(2, 4, 8, 256), vm(2, NA, 8, 128), vm(2, 4, 1, 256),
            vm(2, NA, 128, 128), vm(2, NA, 128, 128),
            vm(NB, 256, 128), vm(NC, 256, 128), vm(NC, 256, 128), vm(NC, 256, 128),
            vm(256, 256), vb(256, 256), vm(256, 128), vm(256, 128),
            vm(256, 256), vb(256, 256), vm(256, 128), vm(256, 128),
            vm(2, 648, 128), vm(2, 640, 128), vm(648, 128), vm(640, 128),
            vm(8, 48, 128), vm(8, 40, 128), vm(8, 40, 128), vm(8, 40, 128),
            vm(8, 48, 128), vm(8, 40, 128), vm(8, 40, 128), vm(8, 40, 128),
            vm(48, 128), vm(40, 128), vm(40, 128), vm(40, 128),
            vm(8, 48, 128), vm(8, 40, 128), vm(8, 40, 128), vm(8, 40, 128),
            vm(2, 8, 48, 128), vm(2, 8, 40, 128), vm(2, 8, 40, 128), vm(2, 8, 40, 128),
            sem(7), sem(2), sem(2), one, sem(NB), one, one, one, one, sem(2), sem(2),
            sem(2), sem(2), one, sem(NC), one, one,
            sem(2), sem(2), sem(4, 4), sem(4, 4),
        ]
        vspec = pl.BlockSpec(memory_space=pltpu.VMEM)
        shapes = ((512, 256), (256, 128), (512, 256), (256, 128))
        hbm = pl.BlockSpec(memory_space=pltpu.HBM)
        staged = pl.pallas_call(
            functools.partial(kernel, local_rows * group),
            out_shape=tuple(pltpu.VMEM(s, F32) for s in ((8, 128), *shapes)),
            in_specs=[hbm] * 7,
            out_specs=(vspec,) * 5,
            scratch_shapes=scratch,
            compiler_params=pltpu.CompilerParams(collective_id=0, has_side_effects=True,
                                                 vmem_limit_bytes=56 * 1024 * 1024),
        )(query_feat, item_feat, log_q.reshape(1, local_rows), w_query_in, w_query_out, w_item_in, w_item_out)
        return pl.pallas_call(
            emit,
            out_shape=tuple(jax.ShapeDtypeStruct(s, F32) for s in ((1,), *shapes)),
            in_specs=[vspec] * 5,
            out_specs=(pl.BlockSpec(memory_space=pltpu.SMEM), hbm, hbm, hbm, hbm),
            scratch_shapes=[sem(4)],
            compiler_params=pltpu.CompilerParams(vmem_limit_bytes=1024 * 1024),
        )(*staged)

    return jax.shard_map(local_step, mesh=mesh,
                         in_specs=(P("dp", None), P("dp", None), P("dp"), P(), P(), P(), P()),
                         out_specs=(P(), P(), P(), P(), P()), check_vma=False)
```

```python
import functools

import jax
import jax.numpy as jnp
from jax import lax
from jax.experimental import pallas as pl
from jax.experimental.pallas import tpu as pltpu
from jax.sharding import PartitionSpec as P

TEMP = 0.05
NORM_EPS = 1e-6
LOG2E = 1.4426950408889634
BOUND = 20.25
F32 = jnp.float32
BF16 = jnp.bfloat16
NA, NB, NC = 8, 16, 8
STEP = (0, 1, 3, 2)
BACK = (0, 2, 1, 3)
FAR = (7, 6, 3, 5, 2, 4, 1)
INV_A = [2 * BACK[s // 2] + s % 2 for s in range(NA)]
INV_B = [4 * BACK[t // 4] + t % 4 for t in range(NB)]


def rel_a(r, s):
    dy = (STEP[r // 2] - STEP[s // 2]) % 4
    return 2 * STEP.index(dy) + (r % 2 + s % 2) % 2


def nt(a, b):
    return lax.dot_general(a, b, (((1,), (1,)), ((), ())), preferred_element_type=F32)


def tn(a, b):
    return lax.dot_general(a, b, (((0,), (0,)), ((), ())), preferred_element_type=F32)


def nn(a, b):
    return jnp.dot(a, b, preferred_element_type=F32)


def forward(x, w_in, w_out, pre_s, hid_s, inv_s, unit_s):
    pre = nn(x[...], w_in[...])
    hid = jnp.maximum(pre, 0.0).astype(BF16)
    emb = nn(hid, w_out[...])
    inv = lax.rsqrt(jnp.sum(emb * emb, axis=-1, keepdims=True) + NORM_EPS)
    unit = emb * inv
    pre_s[...] = pre
    hid_s[...] = hid
    inv_s[...] = jnp.broadcast_to(inv, unit.shape)
    unit_s[...] = unit


def backward(x, w_out, pre_s, hid_s, inv_s, unit_s, d_unit):
    unit = unit_s[...]
    d_emb = inv_s[...] * (d_unit - unit * jnp.sum(unit * d_unit, axis=-1, keepdims=True))
    d_emb = d_emb.astype(BF16)
    g_out = tn(hid_s[...], d_emb)
    d_hid = nt(d_emb, w_out[...])
    d_pre = jnp.where(pre_s[...] > 0, d_hid, 0.0).astype(BF16)
    g_in = tn(x[...], d_pre)
    return g_in, g_out


def kernel(total_rows, qx_h, vx_h, lq_h, wqi_h, wqo_h, wvi_h, wvo_h,
           loss_o, gqi_o, gqo_o, gvi_o, gvo_o,
           qx, vx, lq, wqi, wqo, wvi, wvo,
           u_all, v_all, lq_all, lows, kcol, e_all, zacc, zs, rz, dut, dur, dvs, dvp, dvc, dvr,
           q_pre, q_hid, q_inv, q_unit, v_pre, v_hid, v_inv, v_unit,
           gq, gv, pq, pv,
           h0, h1, h2, h3, r0, r1, r2, r3, o0, o1, o2, o3, x0, x1, x2, x3, f0, f1, f2, f3,
           ins, us, ur, vs, vr, ls, lr, lows_s, lows_r, zss, zsr, dus, durs, dvps, dvpr, dvss, dvsr,
           ps, pr, rss, rsr):
    me = lax.axis_index("dp")
    core = me % 2
    x = (me // 2) % 4
    y = (me // 8) % 4
    z = me // 32
    lo = ((z + 1) // 2) % 2
    hi = z // 2
    scale = 1.0 / (TEMP * total_rows)
    other = (core + 1) % 2
    mate = z * 32 + y * 8 + x * 2 + other

    def a_dev(s):
        zz = z + (s % 2) * (1 - 2 * (z % 2))
        return zz * 32 + ((y + STEP[s // 2]) % 4) * 8 + x * 2 + core

    def c_dev(t, flip=0):
        i = t // 2
        step = STEP[i] if isinstance(t, int) else i + (i // 2) * (1 - 2 * (i % 2))
        zz = z + (t % 2) * (3 - 2 * z)
        return zz * 32 + y * 8 + ((x + step) % 4) * 2 + (core + flip) % 2

    def back_c(t):
        i = t // 2
        return 2 * (i + ((i + 1) // 2) * (3 - 2 * i) * (1 - i // 3)) + t % 2

    def copy(src, dst, ssem, rsem, dev):
        return pltpu.make_async_remote_copy(src_ref=src, dst_ref=dst, send_sem=ssem, recv_sem=rsem,
                                            device_id=(dev,), device_id_type=pl.DeviceIdType.MESH)

    def send(src, dst, ssem, rsem, dev):
        copy(src, dst, ssem, rsem, dev).start()

    def arrived(dst, rsem):
        copy(dst, dst, rsem, rsem, me).wait_recv()

    def gone(src, ssem):
        copy(src, src, ssem, ssem, me).wait_send()

    barrier = pltpu.get_barrier_semaphore()
    partners = [a_dev(s) for s in range(1, NA)] + [c_dev(t // 2, t % 2) for t in range(1, NB)]
    for dev in partners:
        pl.semaphore_signal(barrier, inc=1, device_id=(dev,), device_id_type=pl.DeviceIdType.MESH)

    loads = [pltpu.make_async_copy(a, b, ins.at[i]) for i, (a, b) in enumerate((
        (vx_h, vx), (wvi_h, wvi), (wvo_h, wvo), (qx_h, qx), (wqi_h, wqi), (wqo_h, wqo), (lq_h, lq)))]
    for c in loads:
        c.start()
    for c in loads[:3]:
        c.wait()
    forward(vx, wvi, wvo, v_pre, v_hid, v_inv, v_unit)
    v_all[0] = v_unit[...].astype(BF16)
    for c in loads[3:]:
        c.wait()
    forward(qx, wqi, wqo, q_pre, q_hid, q_inv, q_unit)
    ub = q_unit[...].astype(BF16)
    u_all[0, 0] = ub[0:128]
    u_all[1, 0] = ub[128:256]
    pl.semaphore_wait(barrier, len(partners))
    for t in (14, 15, 12, 13, 6, 7, 10, 11, 4, 5, 8, 9, 2, 3, 1):
        send(lq, lq_all.at[INV_B[t]], ls, lr, c_dev(t // 2, t % 2))
    send(v_all.at[0], v_all.at[1], vs, vr.at[1], mate)
    for t in FAR:
        k = INV_A[t]
        send(u_all.at[0, 0], u_all.at[0, k], us.at[0], ur.at[0], a_dev(t))
        send(v_all.at[0], v_all.at[2 * k], vs, vr.at[2 * k], c_dev(t))
    for t in FAR:
        k = INV_A[t]
        send(u_all.at[1, 0], u_all.at[1, k], us.at[1], ur.at[1], a_dev(t))
    lq_all[0] = lq[...]
    zacc[...] = jnp.zeros_like(zacc)

    low = lq[...]
    arrived(lq_all.at[1:NB], lr)
    for t in range(1, NB):
        low = jnp.minimum(low, lq_all[t])
    low = jnp.min(low, axis=1, keepdims=True)
    lows[0] = jnp.broadcast_to(low, (1, 128))

    def column(t, c):
        row = LOG2E * ((lq_all[t] - low) + BOUND)
        kcol[t] = jnp.transpose(jnp.broadcast_to(row, (128, 256)))
        return c

    lax.fori_loop(0, NB, column, 0)
    for s in FAR:
        send(lows.at[0], lows.at[INV_A[s]], lows_s, lows_r, a_dev(s))
    arrived(u_all.at[0, 1:NA], ur.at[0])

    c2 = LOG2E / TEMP

    def logits(t, h):
        vt = v_all[t]
        kc = kcol[t]
        kc = jnp.concatenate([kc, kc], axis=1)
        for m in range(4):
            um = u_all[h, 2 * m:2 * m + 2].reshape(256, 128)
            e = jnp.exp2(nt(vt, um) * c2 - kc)
            e_all[t, h, m] = e
            zacc[h, m] += jnp.sum(e.reshape(32, 8, 256), axis=0)

    def share(h):
        rows = []
        for m in range(4):
            row = jnp.sum(zacc[h, m], axis=0, keepdims=True)
            rows += [row[:, 0:128], row[:, 128:256]]
        zs[h, 0] = jnp.concatenate(rows, axis=0)

    def share_send(h):
        for s in FAR:
            send(zs.at[h, 0], zs.at[h, INV_A[s]], zss.at[h], zsr.at[h], a_dev(s))

    arrived(v_all.at[1], vr.at[1])
    logits(0, 0)
    logits(1, 0)
    for t in range(NC - 1, 0, -1):
        arrived(v_all.at[2 * t], vr.at[2 * t])
        copy(v_all.at[2 * t], v_all.at[2 * t + 1], vs, vr.at[2 * t + 1], mate).start()

    def first(n, c):
        logits(14 - 4 * n, 0)
        logits(12 - 4 * n, 0)
        return c

    lax.fori_loop(0, 3, first, 0)
    logits(2, 0)

    def mates(n, c):
        for i in range(3):
            t = 15 - 2 * i - 6 * n
            arrived(v_all.at[t], vr.at[t])
        for i in range(3):
            logits(15 - 2 * i - 6 * n, 0)
        return c

    lax.fori_loop(0, 2, mates, 0)
    arrived(v_all.at[3], vr.at[3])
    logits(3, 0)
    share(0)
    arrived(u_all.at[1, 1:NA], ur.at[1])
    share_send(0)

    def second(n, c):
        for i in range(4):
            logits(4 * n + i, 1)
        return c

    lax.fori_loop(0, NB // 4, second, 0)
    share(1)

    ji = lax.broadcasted_iota(jnp.int32, (256, 256), 0)
    qi = lax.broadcasted_iota(jnp.int32, (256, 256), 1)
    own = q_unit[...].astype(BF16).astype(F32) * v_unit[...].astype(BF16).astype(F32)
    pos = jnp.sum(own) / TEMP
    share_send(1)

    def combine(h):
        arrived(zs.at[h, 1:NA], zsr.at[h])
        tot = []
        for r in range(NA):
            acc = None
            for s in range(NA):
                k = rel_a(r, s)
                term = fac[s] * zs[h, s, k:k + 1, :]
                acc = term if acc is None else acc + term
            tot.append(acc)
        inv = [fac[0] / w for w in tot]
        for m in range(4):
            rz[h, m] = jnp.concatenate([inv[2 * m], inv[2 * m + 1]], axis=1)
        return jnp.log(tot[0])

    def grads(t, h, diag, even=False):
        vt = v_all[t]
        dv = None
        for m in range(4):
            p = e_all[t, h, m] * rz[h, m]
            if diag and m == 0:
                p = jnp.where((ji == qi + h * 128) & (qi < 128), p - 1.0, p)
            g = p.astype(BF16)
            d = nn(g, u_all[h, 2 * m:2 * m + 2].reshape(256, 128))
            dv = d if dv is None else dv + d
            du = tn(vt, g)
            if diag:
                dut[h, 2 * m] = du[:, 0:128]
                dut[h, 2 * m + 1] = du[:, 128:256]
            else:
                dut[h, 2 * m] += du[:, 0:128]
                dut[h, 2 * m + 1] += du[:, 128:256]
        if h == 0:
            dvs[t] = dv
        elif even:
            dvc[t // 2] = dvs[t] + dv + dvp[t // 2]
        else:
            dvs[t] += dv

    arrived(lows.at[1:NA], lows_r)
    lowv = [lows[s] for s in range(NA)]
    least = functools.reduce(jnp.minimum, lowv)
    fac = [jnp.exp(least - w) for w in lowv]
    log0 = combine(0)
    grads(0, 0, True)

    def third(n, c):
        for i in range(1, 4):
            grads(3 * n + i, 0, False)
        return c

    lax.fori_loop(0, 5, third, 0)
    log1 = combine(1)
    for s in FAR:
        send(dut.at[0, s], dur.at[0, INV_A[s]], dus.at[0], durs.at[0], a_dev(s))

    def mate_copy(t):
        return copy(dvs.at[2 * t + 1], dvp.at[t], dvps, dvpr.at[t], mate)

    def dv_copy(t):
        return copy(dvc.at[t], dvr.at[back_c(t)], dvss, dvsr, c_dev(t))

    grads(0, 1, True)

    def odd(n, c):
        t = 7 - 2 * n

        @pl.when(n > 0)
        def _():
            mate_copy(t + 1).start()

        grads(2 * t + 1, 1, False)
        grads(2 * t - 1, 1, False)
        mate_copy(t).start()
        return c

    lax.fori_loop(0, 4, odd, 0)

    def even(n, c):
        t = 7 - 2 * n

        @pl.when(n > 0)
        def _():
            dv_copy(t + 1).start()

        @pl.when(n == 0)
        def _():
            mate_copy(0).start()

        arrived(dvp.at[t], dvpr.at[t])
        arrived(dvp.at[t - 1], dvpr.at[t - 1])
        grads(2 * t, 1, False, True)
        grads(2 * t - 2, 1, False, True)
        dv_copy(t).start()
        return c

    lax.fori_loop(0, 3, even, 0)
    dv_copy(jnp.int32(2)).start()
    arrived(dvp.at[1], dvpr.at[1])
    grads(2, 1, False, True)
    for s in FAR:
        send(dut.at[1, s], dur.at[1, INV_A[s]], dus.at[1], durs.at[1], a_dev(s))
    loss_rows = ((BOUND - least) * 2.0 + log0 + log1) + (lq[:, 0:128] + lq[:, 128:256])
    loss_loc = jnp.sum(loss_rows, axis=1, keepdims=True) - pos
    dv_copy(jnp.int32(1)).start()
    arrived(dvp.at[0], dvpr.at[0])
    dvc[0] = dvs[0] + dvp[0]

    parts = []
    for h in range(2):
        arrived(dur.at[h, 1:NA], durs.at[h])
        du = dut[h, 0]
        for s in range(1, NA):
            du = du + dur[h, s]
        parts.append(jnp.transpose(du))
    d_unit = jnp.concatenate(parts, axis=0) * scale
    g_in, g_out = backward(qx, wqo, q_pre, q_hid, q_inv, q_unit, d_unit)

    def pack(buf, g_in, g_out):
        buf[0, 0:512, :] = g_in[:, 0:128]
        buf[0, 512:640, :] = g_in[0:128, 128:256]
        buf[1, 0:384, :] = g_in[128:512, 128:256]
        buf[1, 384:640, :] = g_out

    pack(gq, g_in, g_out)
    lt = jnp.broadcast_to(loss_loc, (8, 128))
    gq[0, 640:648, :] = lt
    gq[1, 640:648, :] = lt
    send(gq.at[other], pq, ps.at[0], pr.at[0], mate)

    a_me, b_me = y * 2 + lo, x * 2 + hi

    def a_idx(s):
        return ((y + STEP[s // 2]) % 4) * 2 + (lo + s % 2) % 2

    def c_idx(t):
        return ((x + STEP[t // 2]) % 4) * 2 + (hi + t % 2) % 2

    side_a, side_c = (a_dev, a_idx, a_me), (c_dev, c_idx, b_me)
    paths = (
        (0, h0, r0, o0, x0, f0, side_c, side_a),
        (1, h1, r1, o1, x1, f1, side_a, side_c),
        (2, h2, r2, o2, x2, f2, side_a, side_c),
        (3, h3, r3, o3, x3, f3, side_c, side_a),
    )

    def pair(w, g, p):
        arrived(p, pr.at[w])
        for i, h, r, o, xx, f, (dev, idx, mine), _ in paths[2 * w:2 * w + 2]:
            base = 320 * (i % 2)
            h[:, 0:40, :] = (g[core, base:base + 320, :] + p[base:base + 320, :]).reshape(8, 40, 128)
            if i == 0:
                extra = g[core, 640:648, :] + p[640:648, :]
                for n in range(8):
                    h[n, 40:48, :] = extra
        for i, h, r, o, xx, f, (dev, idx, mine), _ in paths[2 * w:2 * w + 2]:
            for s in FAR:
                send(h.at[idx(s)], r.at[INV_A[s]], rss.at[0, i], rsr.at[0, i], dev(s))

    def scatter(w):
        for i, h, r, o, xx, f, (_, _, mine), (dev, _, _) in paths[2 * w:2 * w + 2]:
            arrived(r.at[1:8], rsr.at[0, i])
            acc = h[mine]
            for s in range(1, 8):
                acc = acc + r[s]
            o[...] = acc
            for s in FAR:
                send(o, xx.at[INV_A[s]], rss.at[1, i], rsr.at[1, i], dev(s))

    def exchange(w):
        for i, h, r, o, xx, f, (dev, idx, mine), _ in paths[2 * w:2 * w + 2]:
            arrived(xx.at[1:8], rsr.at[1, i])
            acc = o[...]
            for s in range(1, 8):
                acc = acc + xx[s]
            f[core, mine] = acc
            for s in FAR:
                send(f.at[core, mine], f.at[core, mine], rss.at[2, i], rsr.at[2, i], dev(s))
            if i == 0:
                loss_o[...] = acc[40:48] * (1.0 / total_rows)

    def gather(w):
        for i, h, r, o, xx, f, _, _ in paths[2 * w:2 * w + 2]:
            arrived(r.at[1:8], rsr.at[2, i])
            send(f.at[core], f.at[core], rss.at[3, i], rsr.at[3, i], mate)

    def finish(w, go_in, go_out):
        halves = [[], []]
        for i, h, r, o, xx, f, _, _ in paths[2 * w:2 * w + 2]:
            arrived(h, rsr.at[3, i])
            for c in range(2):
                halves[c].append(f[c, :, 0:40, :].reshape(320, 128))
        head, tail = [jnp.concatenate(c, axis=0) for c in halves]
        go_in[:, 0:128] = head[0:512]
        go_in[0:128, 128:256] = head[512:640]
        go_in[128:512, 128:256] = tail[0:384]
        go_out[...] = tail[384:640]

    pair(0, gq, pq)
    arrived(dvr.at[1:NC], dvsr)
    dv = lax.fori_loop(1, NC, lambda t, acc: acc + dvr[t], dvc[0])
    g_in, g_out = backward(vx, wvo, v_pre, v_hid, v_inv, v_unit, dv * scale)
    pack(gv, g_in, g_out)
    send(gv.at[other], pv, ps.at[1], pr.at[1], mate)
    pair(1, gv, pv)
    scatter(0)
    scatter(1)
    exchange(0)
    exchange(1)
    gather(0)
    finish(0, gqi_o, gqo_o)
    gather(1)
    finish(1, gvi_o, gvo_o)
    gone(lq_all.at[1:NB], ls)
    gone(lows.at[1:NA], lows_s)
    gone(v_all.at[1:NB], vs)
    for h in range(2):
        gone(u_all.at[h, 1:NA], us.at[h])
        gone(zs.at[h, 1:NA], zss.at[h])
        gone(dur.at[h, 1:NA], dus.at[h])
    gone(dvp, dvps)
    gone(dvr.at[1:NC], dvss)
    gone(pq, ps.at[0])
    gone(pv, ps.at[1])
    for i, h, r, o, xx, f, _, _ in paths:
        gone(r.at[1:8], rss.at[0, i])
        gone(xx.at[1:8], rss.at[1, i])
        gone(r.at[1:8], rss.at[2, i])
        gone(h, rss.at[3, i])


def emit(loss, gqi, gqo, gvi, gvo, loss_o, gqi_o, gqo_o, gvi_o, gvo_o, value, sem):
    pairs = ((value, loss_o), (gqi, gqi_o), (gvi, gvi_o), (gqo, gqo_o), (gvo, gvo_o))
    copies = [pltpu.make_async_copy(a, b, sem.at[i]) for i, (a, b) in enumerate(pairs)]
    for c in copies[1:]:
        c.start()
    value[0] = loss[0, 0]
    copies[0].start()
    for c in copies:
        c.wait()


def solution(mesh):
    group = mesh.shape["dp"]

    def local_step(query_feat, item_feat, log_q, w_query_in, w_query_out, w_item_in, w_item_out):
        local_rows = query_feat.shape[0]
        vm = lambda *s: pltpu.VMEM(s, F32)
        vb = lambda *s: pltpu.VMEM(s, BF16)
        sem = lambda *s: pltpu.SemaphoreType.DMA(s)
        one = pltpu.SemaphoreType.DMA
        scratch = [
            vb(256, 512), vb(256, 512), vm(1, 256), vb(512, 256), vb(256, 128), vb(512, 256), vb(256, 128),
            vb(2, NA, 128, 128), vb(NB, 256, 128), vm(NB, 1, 256), vm(NA, 1, 128), vm(NB, 256, 128),
            vm(NB, 2, 4, 256, 256), vm(2, 4, 8, 256), vm(2, NA, 8, 128), vm(2, 4, 1, 256),
            vm(2, NA, 128, 128), vm(2, NA, 128, 128),
            vm(NB, 256, 128), vm(NC, 256, 128), vm(NC, 256, 128), vm(NC, 256, 128),
            vm(256, 256), vb(256, 256), vm(256, 128), vm(256, 128),
            vm(256, 256), vb(256, 256), vm(256, 128), vm(256, 128),
            vm(2, 648, 128), vm(2, 640, 128), vm(648, 128), vm(640, 128),
            vm(8, 48, 128), vm(8, 40, 128), vm(8, 40, 128), vm(8, 40, 128),
            vm(8, 48, 128), vm(8, 40, 128), vm(8, 40, 128), vm(8, 40, 128),
            vm(48, 128), vm(40, 128), vm(40, 128), vm(40, 128),
            vm(8, 48, 128), vm(8, 40, 128), vm(8, 40, 128), vm(8, 40, 128),
            vm(2, 8, 48, 128), vm(2, 8, 40, 128), vm(2, 8, 40, 128), vm(2, 8, 40, 128),
            sem(7), sem(2), sem(2), one, sem(NB), one, one, one, one, sem(2), sem(2),
            sem(2), sem(2), one, sem(NC), one, one,
            sem(2), sem(2), sem(4, 4), sem(4, 4),
        ]
        vspec = pl.BlockSpec(memory_space=pltpu.VMEM)
        shapes = ((512, 256), (256, 128), (512, 256), (256, 128))
        hbm = pl.BlockSpec(memory_space=pltpu.HBM)
        staged = pl.pallas_call(
            functools.partial(kernel, local_rows * group),
            out_shape=tuple(pltpu.VMEM(s, F32) for s in ((8, 128), *shapes)),
            in_specs=[hbm] * 7,
            out_specs=(vspec,) * 5,
            scratch_shapes=scratch,
            compiler_params=pltpu.CompilerParams(collective_id=0, has_side_effects=True,
                                                 vmem_limit_bytes=56 * 1024 * 1024),
        )(query_feat, item_feat, log_q.reshape(1, local_rows), w_query_in, w_query_out, w_item_in, w_item_out)
        return pl.pallas_call(
            emit,
            out_shape=tuple(jax.ShapeDtypeStruct(s, F32) for s in ((1,), *shapes)),
            in_specs=[vspec] * 5,
            out_specs=(hbm,) * 5,
            scratch_shapes=[pltpu.SMEM((1,), F32), sem(5)],
            compiler_params=pltpu.CompilerParams(vmem_limit_bytes=1024 * 1024),
        )(*staged)

    return jax.shard_map(local_step, mesh=mesh,
                         in_specs=(P("dp", None), P("dp", None), P("dp"), P(), P(), P(), P()),
                         out_specs=(P(), P(), P(), P(), P()), check_vma=False)
```

```python
import functools

import jax
import jax.numpy as jnp
from jax import lax
from jax.experimental import pallas as pl
from jax.experimental.pallas import tpu as pltpu
from jax.sharding import PartitionSpec as P

TEMP = 0.05
NORM_EPS = 1e-6
LOG2E = 1.4426950408889634
BOUND = 20.25
F32 = jnp.float32
BF16 = jnp.bfloat16
NA, NB, NC = 8, 16, 8
STEP = (0, 1, 3, 2)
BACK = (0, 2, 1, 3)
FAR = (7, 6, 3, 5, 2, 4, 1)
PEER_C = ((0, 0), (0, 1), (2, 0), (1, 0), (3, 0), (3, 1), (1, 1), (2, 1))
FAR_C = (7, 6, 5, 2, 4, 3, 1)
INV_C = (0, 1, 2, 4, 3, 6, 5, 7)
INV_A = [2 * BACK[s // 2] + s % 2 for s in range(NA)]
INV_B = [2 * INV_C[t // 2] + t % 2 for t in range(NB)]


def rel_a(r, s):
    dy = (STEP[r // 2] - STEP[s // 2]) % 4
    return 2 * STEP.index(dy) + (r % 2 + s % 2) % 2


def nt(a, b):
    return lax.dot_general(a, b, (((1,), (1,)), ((), ())), preferred_element_type=F32)


def tn(a, b):
    return lax.dot_general(a, b, (((0,), (0,)), ((), ())), preferred_element_type=F32)


def nn(a, b):
    return jnp.dot(a, b, preferred_element_type=F32)


def forward(x, w_in, w_out, pre_s, hid_s, inv_s, unit_s):
    pre = nn(x[...], w_in[...])
    hid = jnp.maximum(pre, 0.0).astype(BF16)
    emb = nn(hid, w_out[...])
    inv = lax.rsqrt(jnp.sum(emb * emb, axis=-1, keepdims=True) + NORM_EPS)
    unit = emb * inv
    pre_s[...] = pre
    hid_s[...] = hid
    inv_s[...] = jnp.broadcast_to(inv, unit.shape)
    unit_s[...] = unit


def backward(x, w_out, pre_s, hid_s, inv_s, unit_s, d_unit):
    unit = unit_s[...]
    d_emb = inv_s[...] * (d_unit - unit * jnp.sum(unit * d_unit, axis=-1, keepdims=True))
    d_emb = d_emb.astype(BF16)
    g_out = tn(hid_s[...], d_emb)
    d_hid = nt(d_emb, w_out[...])
    d_pre = jnp.where(pre_s[...] > 0, d_hid, 0.0).astype(BF16)
    g_in = tn(x[...], d_pre)
    return g_in, g_out


def kernel(total_rows, qx_h, vx_h, lq_h, wqi_h, wqo_h, wvi_h, wvo_h,
           loss_o, gqi_o, gqo_o, gvi_o, gvo_o,
           qx, vx, lq, wqi, wqo, wvi, wvo,
           u_all, v_all, lq_all, lows, kcol, e_all, zacc, zs, rz, dut, dur, dvs, dvp, dvc, dvr, relay,
           q_pre, q_hid, q_inv, q_unit, v_pre, v_hid, v_inv, v_unit,
           gq, gv, pq, pv,
           h0, h1, h2, h3, r0, r1, r2, r3, o0, o1, o2, o3, x0, x1, x2, x3, f0, f1, f2, f3,
           ins, us, ur, vs, vr, ls, lr, lows_s, lows_r, zss, zsr, dus, durs, dvps, dvpr, dvss, dvsr, relay_r,
           ps, pr, rss, rsr):
    me = lax.axis_index("dp")
    core = me % 2
    x = (me // 2) % 4
    y = (me // 8) % 4
    z = me // 32
    lo = ((z + 1) // 2) % 2
    hi = z // 2
    scale = 1.0 / (TEMP * total_rows)
    other = (core + 1) % 2
    mate = z * 32 + y * 8 + x * 2 + other

    def a_dev(s):
        zz = z + (s % 2) * (1 - 2 * (z % 2))
        return zz * 32 + ((y + STEP[s // 2]) % 4) * 8 + x * 2 + core

    def c_dev(t, flip=0):
        dx, dh = PEER_C[t]
        return (z + dh * (3 - 2 * z)) * 32 + y * 8 + ((x + dx) % 4) * 2 + (core + flip) % 2

    def copy(src, dst, ssem, rsem, dev):
        return pltpu.make_async_remote_copy(src_ref=src, dst_ref=dst, send_sem=ssem, recv_sem=rsem,
                                            device_id=(dev,), device_id_type=pl.DeviceIdType.MESH)

    def send(src, dst, ssem, rsem, dev):
        copy(src, dst, ssem, rsem, dev).start()

    def arrived(dst, rsem):
        copy(dst, dst, rsem, rsem, me).wait_recv()

    def gone(src, ssem):
        copy(src, src, ssem, ssem, me).wait_send()

    barrier = pltpu.get_barrier_semaphore()
    partners = [a_dev(s) for s in range(1, NA)] + [c_dev(t // 2, t % 2) for t in range(1, NB)]
    for dev in partners:
        pl.semaphore_signal(barrier, inc=1, device_id=(dev,), device_id_type=pl.DeviceIdType.MESH)

    loads = [pltpu.make_async_copy(a, b, ins.at[i]) for i, (a, b) in enumerate((
        (vx_h, vx), (wvi_h, wvi), (wvo_h, wvo), (qx_h, qx), (wqi_h, wqi), (wqo_h, wqo), (lq_h, lq)))]
    for c in loads:
        c.start()
    for c in loads[:3]:
        c.wait()
    forward(vx, wvi, wvo, v_pre, v_hid, v_inv, v_unit)
    v_all[0] = v_unit[...].astype(BF16)
    for c in loads[3:]:
        c.wait()
    forward(qx, wqi, wqo, q_pre, q_hid, q_inv, q_unit)
    ub = q_unit[...].astype(BF16)
    u_all[0, 0] = ub[0:128]
    u_all[1, 0] = ub[128:256]
    pl.semaphore_wait(barrier, len(partners))
    for t in (15, 14, 13, 12, 11, 10, 5, 4, 9, 8, 7, 6, 3, 2, 1):
        send(lq, lq_all.at[INV_B[t]], ls, lr, c_dev(t // 2, t % 2))
    send(v_all.at[0], v_all.at[1], vs, vr.at[1], mate)
    for s, t in zip(FAR, FAR_C):
        k = 2 * INV_C[t]
        send(u_all.at[0, 0], u_all.at[0, INV_A[s]], us.at[0], ur.at[0], a_dev(s))
        send(v_all.at[0], v_all.at[k], vs, vr.at[k], c_dev(t))
    for t in FAR:
        k = INV_A[t]
        send(u_all.at[1, 0], u_all.at[1, k], us.at[1], ur.at[1], a_dev(t))
    lq_all[0] = lq[...]
    zacc[...] = jnp.zeros_like(zacc)

    low = lq[...]
    arrived(lq_all.at[1:NB], lr)
    for t in range(1, NB):
        low = jnp.minimum(low, lq_all[t])
    low = jnp.min(low, axis=1, keepdims=True)
    lows[0] = jnp.broadcast_to(low, (1, 128))

    def column(t, c):
        row = LOG2E * ((lq_all[t] - low) + BOUND)
        kcol[t] = jnp.transpose(jnp.broadcast_to(row, (128, 256)))
        return c

    lax.fori_loop(0, NB, column, 0)
    for s in FAR:
        send(lows.at[0], lows.at[INV_A[s]], lows_s, lows_r, a_dev(s))
    arrived(u_all.at[0, 1:NA], ur.at[0])

    c2 = LOG2E / TEMP

    def logits(t, h):
        vt = v_all[t]
        kc = kcol[t]
        kc = jnp.concatenate([kc, kc], axis=1)
        for m in range(4):
            um = u_all[h, 2 * m:2 * m + 2].reshape(256, 128)
            e = jnp.exp2(nt(vt, um) * c2 - kc)
            e_all[t, h, m] = e
            zacc[h, m] += jnp.sum(e.reshape(32, 8, 256), axis=0)

    def share(h):
        rows = []
        for m in range(4):
            row = jnp.sum(zacc[h, m], axis=0, keepdims=True)
            rows += [row[:, 0:128], row[:, 128:256]]
        zs[h, 0] = jnp.concatenate(rows, axis=0)

    def share_send(h):
        for s in FAR:
            send(zs.at[h, 0], zs.at[h, INV_A[s]], zss.at[h], zsr.at[h], a_dev(s))

    arrived(v_all.at[1], vr.at[1])
    logits(0, 0)
    logits(1, 0)
    for t in range(NC - 1, 0, -1):
        arrived(v_all.at[2 * t], vr.at[2 * t])
        copy(v_all.at[2 * t], v_all.at[2 * t + 1], vs, vr.at[2 * t + 1], mate).start()

    def first(n, c):
        logits(14 - 4 * n, 0)
        logits(12 - 4 * n, 0)
        return c

    lax.fori_loop(0, 3, first, 0)
    logits(2, 0)

    def mates(n, c):
        for i in range(3):
            t = 15 - 2 * i - 6 * n
            arrived(v_all.at[t], vr.at[t])
        for i in range(3):
            logits(15 - 2 * i - 6 * n, 0)
        return c

    lax.fori_loop(0, 2, mates, 0)
    arrived(v_all.at[3], vr.at[3])
    logits(3, 0)
    share(0)
    arrived(u_all.at[1, 1:NA], ur.at[1])
    share_send(0)

    def second(n, c):
        for i in range(4):
            logits(4 * n + i, 1)
        return c

    lax.fori_loop(0, NB // 4, second, 0)
    share(1)

    ji = lax.broadcasted_iota(jnp.int32, (256, 256), 0)
    qi = lax.broadcasted_iota(jnp.int32, (256, 256), 1)
    own = q_unit[...].astype(BF16).astype(F32) * v_unit[...].astype(BF16).astype(F32)
    pos = jnp.sum(own) / TEMP
    share_send(1)

    def combine(h):
        arrived(zs.at[h, 1:NA], zsr.at[h])
        tot = []
        for r in range(NA):
            acc = None
            for s in range(NA):
                k = rel_a(r, s)
                term = fac[s] * zs[h, s, k:k + 1, :]
                acc = term if acc is None else acc + term
            tot.append(acc)
        inv = [fac[0] / w for w in tot]
        for m in range(4):
            rz[h, m] = jnp.concatenate([inv[2 * m], inv[2 * m + 1]], axis=1)
        return jnp.log(tot[0])

    def grads(t, h, diag, even=False):
        vt = v_all[t]
        dv = None
        for m in range(4):
            p = e_all[t, h, m] * rz[h, m]
            if diag and m == 0:
                p = jnp.where((ji == qi + h * 128) & (qi < 128), p - 1.0, p)
            g = p.astype(BF16)
            d = nn(g, u_all[h, 2 * m:2 * m + 2].reshape(256, 128))
            dv = d if dv is None else dv + d
            du = tn(vt, g)
            if diag:
                dut[h, 2 * m] = du[:, 0:128]
                dut[h, 2 * m + 1] = du[:, 128:256]
            else:
                dut[h, 2 * m] += du[:, 0:128]
                dut[h, 2 * m + 1] += du[:, 128:256]
        if h == 0:
            dvs[t] = dv
        elif even:
            dvc[t // 2] = dvs[t] + dv + dvp[t // 2]
        else:
            dvs[t] += dv

    arrived(lows.at[1:NA], lows_r)
    lowv = [lows[s] for s in range(NA)]
    least = functools.reduce(jnp.minimum, lowv)
    fac = [jnp.exp(least - w) for w in lowv]
    log0 = combine(0)
    grads(0, 0, True)

    def third(n, c):
        for i in range(1, 4):
            grads(3 * n + i, 0, False)
        return c

    lax.fori_loop(0, 5, third, 0)
    log1 = combine(1)
    for s in FAR:
        send(dut.at[0, s], dur.at[0, INV_A[s]], dus.at[0], durs.at[0], a_dev(s))

    def mate_copy(t):
        return copy(dvs.at[2 * t + 1], dvp.at[t], dvps, dvpr.at[t], mate)

    def dv_send(t):
        if t > 5:
            send(dvc.at[t], relay.at[7 - t], dvss, relay_r.at[7 - t], c_dev(1 if t == 7 else 3))
        else:
            send(dvc.at[t], dvr.at[t], dvss, dvsr, c_dev(t))

    grads(0, 1, True)

    def odd(n, c):
        t = 7 - 2 * n

        @pl.when(n > 0)
        def _():
            mate_copy(t + 1).start()

        grads(2 * t + 1, 1, False)
        grads(2 * t - 1, 1, False)
        mate_copy(t).start()
        return c

    lax.fori_loop(0, 4, odd, 0)

    mate_copy(0).start()
    for t in (7, 5, 3):
        arrived(dvp.at[t], dvpr.at[t])
        arrived(dvp.at[t - 1], dvpr.at[t - 1])
        if t < 7:
            dv_send(t + 1)
        grads(2 * t, 1, False, True)
        grads(2 * t - 2, 1, False, True)
        dv_send(t)
    arrived(dvp.at[1], dvpr.at[1])
    grads(2, 1, False, True)
    for s in FAR:
        send(dut.at[1, s], dur.at[1, INV_A[s]], dus.at[1], durs.at[1], a_dev(s))
    loss_rows = ((BOUND - least) * 2.0 + log0 + log1) + (lq[:, 0:128] + lq[:, 128:256])
    loss_loc = jnp.sum(loss_rows, axis=1, keepdims=True) - pos
    arrived(dvp.at[0], dvpr.at[0])
    dvc[0] = dvs[0] + dvp[0]
    arrived(relay.at[0], relay_r.at[0])
    dvc[2] += relay[0]
    arrived(relay.at[1], relay_r.at[1])
    dv_send(2)
    dvc[1] += relay[1]
    du = dut[0, 0]
    for s in range(1, NA):
        if s == 1:
            arrived(dur.at[0, 1:NA], durs.at[0])
        du = du + dur[0, s]
    parts = [jnp.transpose(du)]
    dv_send(1)
    for h in range(1, 2):
        arrived(dur.at[h, 1:NA], durs.at[h])
        du = dut[h, 0]
        for s in range(1, NA):
            du = du + dur[h, s]
        parts.append(jnp.transpose(du))
    d_unit = jnp.concatenate(parts, axis=0) * scale
    g_in, g_out = backward(qx, wqo, q_pre, q_hid, q_inv, q_unit, d_unit)

    def pack(buf, g_in, g_out):
        buf[0, 0:512, :] = g_in[:, 0:128]
        buf[0, 512:640, :] = g_in[0:128, 128:256]
        buf[1, 0:384, :] = g_in[128:512, 128:256]
        buf[1, 384:640, :] = g_out

    pack(gq, g_in, g_out)
    lt = jnp.broadcast_to(loss_loc, (8, 128))
    gq[0, 640:648, :] = lt
    gq[1, 640:648, :] = lt
    send(gq.at[other], pq, ps.at[0], pr.at[0], mate)

    a_me, b_me = y * 2 + lo, x * 2 + hi

    def a_idx(s):
        return ((y + STEP[s // 2]) % 4) * 2 + (lo + s % 2) % 2

    def c_idx(t):
        return ((x + PEER_C[t][0]) % 4) * 2 + (hi + PEER_C[t][1]) % 2

    side_a, side_c = (a_dev, a_idx, a_me, FAR, INV_A), (c_dev, c_idx, b_me, FAR_C, INV_C)
    paths = (
        (0, h0, r0, o0, x0, f0, side_c, side_a),
        (1, h1, r1, o1, x1, f1, side_a, side_c),
        (2, h2, r2, o2, x2, f2, side_a, side_c),
        (3, h3, r3, o3, x3, f3, side_c, side_a),
    )

    def pair(w, g, p):
        arrived(p, pr.at[w])
        for i, h, r, o, xx, f, (dev, idx, mine, far, inv), _ in paths[2 * w:2 * w + 2]:
            base = 320 * (i % 2)
            h[:, 0:40, :] = (g[core, base:base + 320, :] + p[base:base + 320, :]).reshape(8, 40, 128)
            if i == 0:
                extra = g[core, 640:648, :] + p[640:648, :]
                for n in range(8):
                    h[n, 40:48, :] = extra
        for i, h, r, o, xx, f, (dev, idx, mine, far, inv), _ in paths[2 * w:2 * w + 2]:
            for s in far:
                send(h.at[idx(s)], r.at[inv[s]], rss.at[0, i], rsr.at[0, i], dev(s))

    def scatter(w):
        for i, h, r, o, xx, f, (_, _, mine, _, _), (dev, _, _, far, inv) in paths[2 * w:2 * w + 2]:
            arrived(r.at[1:8], rsr.at[0, i])
            acc = h[mine]
            for s in range(1, 8):
                acc = acc + r[s]
            o[...] = acc
            for s in far:
                send(o, xx.at[inv[s]], rss.at[1, i], rsr.at[1, i], dev(s))

    def exchange(w):
        for i, h, r, o, xx, f, (dev, idx, mine, far, inv), _ in paths[2 * w:2 * w + 2]:
            arrived(xx.at[1:8], rsr.at[1, i])
            acc = o[...]
            for s in range(1, 8):
                acc = acc + xx[s]
            f[core, mine] = acc
            for s in far:
                send(f.at[core, mine], f.at[core, mine], rss.at[2, i], rsr.at[2, i], dev(s))
            if i == 0:
                loss_o[...] = acc[40:48] * (1.0 / total_rows)

    def gather(w):
        for i, h, r, o, xx, f, _, _ in paths[2 * w:2 * w + 2]:
            arrived(r.at[1:8], rsr.at[2, i])
            send(f.at[core], f.at[core], rss.at[3, i], rsr.at[3, i], mate)

    def finish(w, go_in, go_out):
        halves = [[], []]
        for i, h, r, o, xx, f, _, _ in paths[2 * w:2 * w + 2]:
            arrived(h, rsr.at[3, i])
            for c in range(2):
                halves[c].append(f[c, :, 0:40, :].reshape(320, 128))
        head, tail = [jnp.concatenate(c, axis=0) for c in halves]
        go_in[:, 0:128] = head[0:512]
        go_in[0:128, 128:256] = head[512:640]
        go_in[128:512, 128:256] = tail[0:384]
        go_out[...] = tail[384:640]

    pair(0, gq, pq)
    arrived(dvr.at[1:6], dvsr)
    dv = lax.fori_loop(1, 6, lambda t, acc: acc + dvr[t], dvc[0])
    g_in, g_out = backward(vx, wvo, v_pre, v_hid, v_inv, v_unit, dv * scale)
    pack(gv, g_in, g_out)
    send(gv.at[other], pv, ps.at[1], pr.at[1], mate)
    pair(1, gv, pv)
    scatter(0)
    scatter(1)
    exchange(0)
    exchange(1)
    gather(0)
    finish(0, gqi_o, gqo_o)
    gather(1)
    finish(1, gvi_o, gvo_o)
    gone(lq_all.at[1:NB], ls)
    gone(lows.at[1:NA], lows_s)
    gone(v_all.at[1:NB], vs)
    for h in range(2):
        gone(u_all.at[h, 1:NA], us.at[h])
        gone(zs.at[h, 1:NA], zss.at[h])
        gone(dur.at[h, 1:NA], dus.at[h])
    gone(dvp, dvps)
    gone(dvr.at[1:NC], dvss)
    gone(pq, ps.at[0])
    gone(pv, ps.at[1])
    for i, h, r, o, xx, f, _, _ in paths:
        gone(r.at[1:8], rss.at[0, i])
        gone(xx.at[1:8], rss.at[1, i])
        gone(r.at[1:8], rss.at[2, i])
        gone(h, rss.at[3, i])


def emit(loss, gqi, gqo, gvi, gvo, loss_o, gqi_o, gqo_o, gvi_o, gvo_o, value, sem):
    pairs = ((value, loss_o), (gqi, gqi_o), (gvi, gvi_o), (gqo, gqo_o), (gvo, gvo_o))
    copies = [pltpu.make_async_copy(a, b, sem.at[i]) for i, (a, b) in enumerate(pairs)]
    for c in copies[1:]:
        c.start()
    value[0] = loss[0, 0]
    copies[0].start()
    for c in copies:
        c.wait()


def solution(mesh):
    group = mesh.shape["dp"]

    def local_step(query_feat, item_feat, log_q, w_query_in, w_query_out, w_item_in, w_item_out):
        local_rows = query_feat.shape[0]
        vm = lambda *s: pltpu.VMEM(s, F32)
        vb = lambda *s: pltpu.VMEM(s, BF16)
        sem = lambda *s: pltpu.SemaphoreType.DMA(s)
        one = pltpu.SemaphoreType.DMA
        scratch = [
            vb(256, 512), vb(256, 512), vm(1, 256), vb(512, 256), vb(256, 128), vb(512, 256), vb(256, 128),
            vb(2, NA, 128, 128), vb(NB, 256, 128), vm(NB, 1, 256), vm(NA, 1, 128), vm(NB, 256, 128),
            vm(NB, 2, 4, 256, 256), vm(2, 4, 8, 256), vm(2, NA, 8, 128), vm(2, 4, 1, 256),
            vm(2, NA, 128, 128), vm(2, NA, 128, 128),
            vm(NB, 256, 128), vm(NC, 256, 128), vm(NC, 256, 128), vm(NC, 256, 128), vm(2, 256, 128),
            vm(256, 256), vb(256, 256), vm(256, 128), vm(256, 128),
            vm(256, 256), vb(256, 256), vm(256, 128), vm(256, 128),
            vm(2, 648, 128), vm(2, 640, 128), vm(648, 128), vm(640, 128),
            vm(8, 48, 128), vm(8, 40, 128), vm(8, 40, 128), vm(8, 40, 128),
            vm(8, 48, 128), vm(8, 40, 128), vm(8, 40, 128), vm(8, 40, 128),
            vm(48, 128), vm(40, 128), vm(40, 128), vm(40, 128),
            vm(8, 48, 128), vm(8, 40, 128), vm(8, 40, 128), vm(8, 40, 128),
            vm(2, 8, 48, 128), vm(2, 8, 40, 128), vm(2, 8, 40, 128), vm(2, 8, 40, 128),
            sem(7), sem(2), sem(2), one, sem(NB), one, one, one, one, sem(2), sem(2),
            sem(2), sem(2), one, sem(NC), one, one, sem(2),
            sem(2), sem(2), sem(4, 4), sem(4, 4),
        ]
        vspec = pl.BlockSpec(memory_space=pltpu.VMEM)
        shapes = ((512, 256), (256, 128), (512, 256), (256, 128))
        hbm = pl.BlockSpec(memory_space=pltpu.HBM)
        staged = pl.pallas_call(
            functools.partial(kernel, local_rows * group),
            out_shape=tuple(pltpu.VMEM(s, F32) for s in ((8, 128), *shapes)),
            in_specs=[hbm] * 7,
            out_specs=(vspec,) * 5,
            scratch_shapes=scratch,
            compiler_params=pltpu.CompilerParams(collective_id=0, has_side_effects=True,
                                                 vmem_limit_bytes=56 * 1024 * 1024),
        )(query_feat, item_feat, log_q.reshape(1, local_rows), w_query_in, w_query_out, w_item_in, w_item_out)
        return pl.pallas_call(
            emit,
            out_shape=tuple(jax.ShapeDtypeStruct(s, F32) for s in ((1,), *shapes)),
            in_specs=[vspec] * 5,
            out_specs=(hbm,) * 5,
            scratch_shapes=[pltpu.SMEM((1,), F32), sem(5)],
            compiler_params=pltpu.CompilerParams(vmem_limit_bytes=1024 * 1024),
        )(*staged)

    return jax.shard_map(local_step, mesh=mesh,
                         in_specs=(P("dp", None), P("dp", None), P("dp"), P(), P(), P(), P()),
                         out_specs=(P(), P(), P(), P(), P()), check_vma=False)
```

```python
import functools

import jax
import jax.numpy as jnp
from jax import lax
from jax.experimental import pallas as pl
from jax.experimental.pallas import tpu as pltpu
from jax.sharding import PartitionSpec as P

TEMP = 0.05
NORM_EPS = 1e-6
LOG2E = 1.4426950408889634
BOUND = 20.25
F32 = jnp.float32
BF16 = jnp.bfloat16
NA, NB, NC = 8, 16, 8
STEP = (0, 1, 3, 2)
BACK = (0, 2, 1, 3)
FAR = (7, 6, 3, 5, 2, 4, 1)
PEER_C = ((0, 0), (0, 1), (2, 0), (3, 1), (1, 0), (3, 0), (1, 1), (2, 1))
FAR_C = (7, 6, 3, 2, 5, 4, 1)
INV_C = (0, 1, 2, 6, 5, 4, 3, 7)
INV_A = [2 * BACK[s // 2] + s % 2 for s in range(NA)]
INV_B = [2 * INV_C[t // 2] + t % 2 for t in range(NB)]


def rel_a(r, s):
    dy = (STEP[r // 2] - STEP[s // 2]) % 4
    return 2 * STEP.index(dy) + (r % 2 + s % 2) % 2


def nt(a, b):
    return lax.dot_general(a, b, (((1,), (1,)), ((), ())), preferred_element_type=F32)


def tn(a, b):
    return lax.dot_general(a, b, (((0,), (0,)), ((), ())), preferred_element_type=F32)


def nn(a, b):
    return jnp.dot(a, b, preferred_element_type=F32)


def forward(x, w_in, w_out, pre_s, hid_s, inv_s, unit_s):
    pre = nn(x[...], w_in[...])
    hid = jnp.maximum(pre, 0.0).astype(BF16)
    emb = nn(hid, w_out[...])
    inv = lax.rsqrt(jnp.sum(emb * emb, axis=-1, keepdims=True) + NORM_EPS)
    unit = emb * inv
    pre_s[...] = pre
    hid_s[...] = hid
    inv_s[...] = jnp.broadcast_to(inv, unit.shape)
    unit_s[...] = unit


def backward(x, w_out, pre_s, hid_s, inv_s, unit_s, d_unit):
    unit = unit_s[...]
    d_emb = inv_s[...] * (d_unit - unit * jnp.sum(unit * d_unit, axis=-1, keepdims=True))
    d_emb = d_emb.astype(BF16)
    g_out = tn(hid_s[...], d_emb)
    d_hid = nt(d_emb, w_out[...])
    d_pre = jnp.where(pre_s[...] > 0, d_hid, 0.0).astype(BF16)
    g_in = tn(x[...], d_pre)
    return g_in, g_out


def kernel(total_rows, qx_h, vx_h, lq_h, wqi_h, wqo_h, wvi_h, wvo_h,
           loss_o, gqi_o, gqo_o, gvi_o, gvo_o,
           qx, vx, lq, wqi, wqo, wvi, wvo,
           u_all, v_all, lq_all, lows, kcol, e_all, zacc, zs, rz, dut, dur, dvs, dvp, dvc, dvr, relay,
           q_pre, q_hid, q_inv, q_unit, v_pre, v_hid, v_inv, v_unit,
           gq, gv, pq, pv,
           h0, h1, h2, h3, r0, r1, r2, r3, o0, o1, o2, o3, x0, x1, x2, x3, f0, f1, f2, f3,
           ins, us, ur, vs, vr, ls, lr, lows_s, lows_r, zss, zsr, dus, durs, dvps, dvpr, dvss, dvsr, relay_r,
           ps, pr, rss, rsr):
    me = lax.axis_index("dp")
    core = me % 2
    x = (me // 2) % 4
    y = (me // 8) % 4
    z = me // 32
    lo = ((z + 1) // 2) % 2
    hi = z // 2
    scale = 1.0 / (TEMP * total_rows)
    other = (core + 1) % 2
    mate = z * 32 + y * 8 + x * 2 + other

    def a_dev(s):
        zz = z + (s % 2) * (1 - 2 * (z % 2))
        return zz * 32 + ((y + STEP[s // 2]) % 4) * 8 + x * 2 + core

    def c_dev(t, flip=0):
        dx, dh = PEER_C[t]
        return (z + dh * (3 - 2 * z)) * 32 + y * 8 + ((x + dx) % 4) * 2 + (core + flip) % 2

    def copy(src, dst, ssem, rsem, dev):
        return pltpu.make_async_remote_copy(src_ref=src, dst_ref=dst, send_sem=ssem, recv_sem=rsem,
                                            device_id=(dev,), device_id_type=pl.DeviceIdType.MESH)

    def send(src, dst, ssem, rsem, dev):
        copy(src, dst, ssem, rsem, dev).start()

    def arrived(dst, rsem):
        copy(dst, dst, rsem, rsem, me).wait_recv()

    def gone(src, ssem):
        copy(src, src, ssem, ssem, me).wait_send()

    barrier = pltpu.get_barrier_semaphore()
    partners = [a_dev(s) for s in range(1, NA)] + [c_dev(t // 2, t % 2) for t in range(1, NB)]
    for dev in partners:
        pl.semaphore_signal(barrier, inc=1, device_id=(dev,), device_id_type=pl.DeviceIdType.MESH)

    loads = [pltpu.make_async_copy(a, b, ins.at[i]) for i, (a, b) in enumerate((
        (vx_h, vx), (wvi_h, wvi), (wvo_h, wvo), (qx_h, qx), (wqi_h, wqi), (wqo_h, wqo), (lq_h, lq)))]
    for c in loads:
        c.start()
    for c in loads[:3]:
        c.wait()
    forward(vx, wvi, wvo, v_pre, v_hid, v_inv, v_unit)
    v_all[0] = v_unit[...].astype(BF16)
    for c in loads[3:]:
        c.wait()
    forward(qx, wqi, wqo, q_pre, q_hid, q_inv, q_unit)
    ub = q_unit[...].astype(BF16)
    u_all[0, 0] = ub[0:128]
    u_all[1, 0] = ub[128:256]
    pl.semaphore_wait(barrier, len(partners))
    for t in (15, 14, 13, 12, 11, 10, 5, 4, 9, 8, 7, 6, 3, 2, 1):
        send(lq, lq_all.at[INV_B[t]], ls, lr, c_dev(t // 2, t % 2))
    send(v_all.at[0], v_all.at[1], vs, vr.at[1], mate)
    for s, t in zip(FAR, FAR_C):
        k = 2 * INV_C[t]
        send(u_all.at[0, 0], u_all.at[0, INV_A[s]], us.at[0], ur.at[0], a_dev(s))
        send(v_all.at[0], v_all.at[k], vs, vr.at[k], c_dev(t))
    for t in FAR:
        k = INV_A[t]
        send(u_all.at[1, 0], u_all.at[1, k], us.at[1], ur.at[1], a_dev(t))
    lq_all[0] = lq[...]
    zacc[...] = jnp.zeros_like(zacc)

    low = lq[...]
    arrived(lq_all.at[1:NB], lr)
    for t in range(1, NB):
        low = jnp.minimum(low, lq_all[t])
    low = jnp.min(low, axis=1, keepdims=True)
    lows[0] = jnp.broadcast_to(low, (1, 128))

    def column(t, c):
        row = LOG2E * ((lq_all[t] - low) + BOUND)
        kcol[t] = jnp.transpose(jnp.broadcast_to(row, (128, 256)))
        return c

    lax.fori_loop(0, NB, column, 0)
    for s in FAR:
        send(lows.at[0], lows.at[INV_A[s]], lows_s, lows_r, a_dev(s))
    arrived(u_all.at[0, 1:NA], ur.at[0])

    c2 = LOG2E / TEMP

    def logits(t, h):
        vt = v_all[t]
        kc = kcol[t]
        kc = jnp.concatenate([kc, kc], axis=1)
        for m in range(4):
            um = u_all[h, 2 * m:2 * m + 2].reshape(256, 128)
            e = jnp.exp2(nt(vt, um) * c2 - kc)
            e_all[t, h, m] = e
            zacc[h, m] += jnp.sum(e.reshape(32, 8, 256), axis=0)

    def share(h):
        rows = []
        for m in range(4):
            row = jnp.sum(zacc[h, m], axis=0, keepdims=True)
            rows += [row[:, 0:128], row[:, 128:256]]
        zs[h, 0] = jnp.concatenate(rows, axis=0)

    def share_send(h):
        for s in FAR:
            send(zs.at[h, 0], zs.at[h, INV_A[s]], zss.at[h], zsr.at[h], a_dev(s))

    arrived(v_all.at[1], vr.at[1])
    logits(0, 0)
    logits(1, 0)
    for t in range(NC - 1, 0, -1):
        arrived(v_all.at[2 * t], vr.at[2 * t])
        copy(v_all.at[2 * t], v_all.at[2 * t + 1], vs, vr.at[2 * t + 1], mate).start()

    def first(n, c):
        logits(14 - 4 * n, 0)
        logits(12 - 4 * n, 0)
        return c

    lax.fori_loop(0, 3, first, 0)
    logits(2, 0)

    def mates(n, c):
        for i in range(3):
            t = 15 - 2 * i - 6 * n
            arrived(v_all.at[t], vr.at[t])
        for i in range(3):
            logits(15 - 2 * i - 6 * n, 0)
        return c

    lax.fori_loop(0, 2, mates, 0)
    arrived(v_all.at[3], vr.at[3])
    logits(3, 0)
    share(0)
    arrived(u_all.at[1, 1:NA], ur.at[1])
    share_send(0)

    def second(n, c):
        for i in range(4):
            logits(4 * n + i, 1)
        return c

    lax.fori_loop(0, NB // 4, second, 0)
    share(1)

    ji = lax.broadcasted_iota(jnp.int32, (256, 256), 0)
    qi = lax.broadcasted_iota(jnp.int32, (256, 256), 1)
    own = q_unit[...].astype(BF16).astype(F32) * v_unit[...].astype(BF16).astype(F32)
    pos = jnp.sum(own) / TEMP
    share_send(1)

    def combine(h):
        arrived(zs.at[h, 1:NA], zsr.at[h])
        tot = []
        for r in range(NA):
            acc = None
            for s in range(NA):
                k = rel_a(r, s)
                term = fac[s] * zs[h, s, k:k + 1, :]
                acc = term if acc is None else acc + term
            tot.append(acc)
        inv = [fac[0] / w for w in tot]
        for m in range(4):
            rz[h, m] = jnp.concatenate([inv[2 * m], inv[2 * m + 1]], axis=1)
        return jnp.log(tot[0])

    def grads(t, h, diag, even=False):
        vt = v_all[t]
        dv = None
        for m in range(4):
            p = e_all[t, h, m] * rz[h, m]
            if diag and m == 0:
                p = jnp.where((ji == qi + h * 128) & (qi < 128), p - 1.0, p)
            g = p.astype(BF16)
            d = nn(g, u_all[h, 2 * m:2 * m + 2].reshape(256, 128))
            dv = d if dv is None else dv + d
            du = tn(vt, g)
            if diag:
                dut[h, 2 * m] = du[:, 0:128]
                dut[h, 2 * m + 1] = du[:, 128:256]
            else:
                dut[h, 2 * m] += du[:, 0:128]
                dut[h, 2 * m + 1] += du[:, 128:256]
        if h == 0:
            dvs[t] = dv
        elif even:
            dvc[t // 2] = dvs[t] + dv + dvp[t // 2]
        else:
            dvs[t] += dv

    arrived(lows.at[1:NA], lows_r)
    lowv = [lows[s] for s in range(NA)]
    least = functools.reduce(jnp.minimum, lowv)
    fac = [jnp.exp(least - w) for w in lowv]
    log0 = combine(0)
    grads(0, 0, True)

    def third(n, c):
        for i in range(1, 4):
            grads(3 * n + i, 0, False)
        return c

    lax.fori_loop(0, 5, third, 0)
    log1 = combine(1)
    for s in FAR:
        send(dut.at[0, s], dur.at[0, INV_A[s]], dus.at[0], durs.at[0], a_dev(s))

    def mate_copy(t):
        return copy(dvs.at[2 * t + 1], dvp.at[t], dvps, dvpr.at[t], mate)

    def dv_send(t):
        if t > 5:
            send(dvc.at[t], relay.at[7 - t], dvss, relay_r.at[7 - t], c_dev(1 if t == 7 else 4))
        else:
            send(dvc.at[t], dvr.at[t], dvss, dvsr, c_dev(t))

    grads(0, 1, True)

    def odd(n, c):
        t = 7 - 2 * n

        @pl.when(n > 0)
        def _():
            mate_copy(t + 1).start()

        grads(2 * t + 1, 1, False)
        grads(2 * t - 1, 1, False)
        mate_copy(t).start()
        return c

    lax.fori_loop(0, 4, odd, 0)

    mate_copy(0).start()
    for t in (7, 5, 3):
        arrived(dvp.at[t], dvpr.at[t])
        arrived(dvp.at[t - 1], dvpr.at[t - 1])
        if t < 7:
            dv_send(t + 1)
        grads(2 * t, 1, False, True)
        grads(2 * t - 2, 1, False, True)
        dv_send(t)
    arrived(dvp.at[1], dvpr.at[1])
    grads(2, 1, False, True)
    for s in FAR:
        send(dut.at[1, s], dur.at[1, INV_A[s]], dus.at[1], durs.at[1], a_dev(s))
    loss_rows = ((BOUND - least) * 2.0 + log0 + log1) + (lq[:, 0:128] + lq[:, 128:256])
    loss_loc = jnp.sum(loss_rows, axis=1, keepdims=True) - pos
    arrived(relay.at[0], relay_r.at[0])
    dvc[2] += relay[0]
    arrived(dvp.at[0], dvpr.at[0])
    dvc[0] = dvs[0] + dvp[0]
    dv_send(2)
    arrived(relay.at[1], relay_r.at[1])
    dvc[1] += relay[1]

    def sum_du(h):
        arrived(dur.at[h, 1:NA], durs.at[h])
        du = dut[h, 0]
        for s in range(1, NA):
            du = du + dur[h, s]
        return jnp.transpose(du)

    parts = [sum_du(0)]
    dv_send(1)
    parts.append(sum_du(1))
    d_unit = jnp.concatenate(parts, axis=0) * scale
    g_in, g_out = backward(qx, wqo, q_pre, q_hid, q_inv, q_unit, d_unit)

    def pack(buf, g_in, g_out):
        buf[0, 0:512, :] = g_in[:, 0:128]
        buf[0, 512:640, :] = g_in[0:128, 128:256]
        buf[1, 0:384, :] = g_in[128:512, 128:256]
        buf[1, 384:640, :] = g_out

    pack(gq, g_in, g_out)
    lt = jnp.broadcast_to(loss_loc, (8, 128))
    gq[0, 640:648, :] = lt
    gq[1, 640:648, :] = lt
    send(gq.at[other], pq, ps.at[0], pr.at[0], mate)

    a_me, b_me = y * 2 + lo, x * 2 + hi

    def a_idx(s):
        return ((y + STEP[s // 2]) % 4) * 2 + (lo + s % 2) % 2

    def c_idx(t):
        return ((x + PEER_C[t][0]) % 4) * 2 + (hi + PEER_C[t][1]) % 2

    side_a, side_c = (a_dev, a_idx, a_me, FAR, INV_A), (c_dev, c_idx, b_me, FAR_C, INV_C)
    paths = (
        (0, h0, r0, o0, x0, f0, side_c, side_a),
        (1, h1, r1, o1, x1, f1, side_a, side_c),
        (2, h2, r2, o2, x2, f2, side_a, side_c),
        (3, h3, r3, o3, x3, f3, side_c, side_a),
    )

    def pair(w, g, p):
        arrived(p, pr.at[w])
        for i, h, r, o, xx, f, (dev, idx, mine, far, inv), _ in paths[2 * w:2 * w + 2]:
            base = 320 * (i % 2)
            h[:, 0:40, :] = (g[core, base:base + 320, :] + p[base:base + 320, :]).reshape(8, 40, 128)
            if i == 0:
                extra = g[core, 640:648, :] + p[640:648, :]
                for n in range(8):
                    h[n, 40:48, :] = extra
        for i, h, r, o, xx, f, (dev, idx, mine, far, inv), _ in paths[2 * w:2 * w + 2]:
            for s in far:
                send(h.at[idx(s)], r.at[inv[s]], rss.at[0, i], rsr.at[0, i], dev(s))

    def scatter(w):
        for i, h, r, o, xx, f, (_, _, mine, _, _), (dev, _, _, far, inv) in paths[2 * w:2 * w + 2]:
            arrived(r.at[1:8], rsr.at[0, i])
            acc = h[mine]
            for s in range(1, 8):
                acc = acc + r[s]
            o[...] = acc
            for s in far:
                send(o, xx.at[inv[s]], rss.at[1, i], rsr.at[1, i], dev(s))

    def exchange(w):
        for i, h, r, o, xx, f, (dev, idx, mine, far, inv), _ in paths[2 * w:2 * w + 2]:
            arrived(xx.at[1:8], rsr.at[1, i])
            acc = o[...]
            for s in range(1, 8):
                acc = acc + xx[s]
            f[core, mine] = acc
            for s in far:
                send(f.at[core, mine], f.at[core, mine], rss.at[2, i], rsr.at[2, i], dev(s))
            if i == 0:
                loss_o[...] = acc[40:48] * (1.0 / total_rows)

    def gather(w):
        for i, h, r, o, xx, f, _, _ in paths[2 * w:2 * w + 2]:
            arrived(r.at[1:8], rsr.at[2, i])
            send(f.at[core], f.at[core], rss.at[3, i], rsr.at[3, i], mate)

    def finish(w, go_in, go_out):
        halves = [[], []]
        for i, h, r, o, xx, f, _, _ in paths[2 * w:2 * w + 2]:
            arrived(h, rsr.at[3, i])
            for c in range(2):
                halves[c].append(f[c, :, 0:40, :].reshape(320, 128))
        head, tail = [jnp.concatenate(c, axis=0) for c in halves]
        go_in[:, 0:128] = head[0:512]
        go_in[0:128, 128:256] = head[512:640]
        go_in[128:512, 128:256] = tail[0:384]
        go_out[...] = tail[384:640]

    pair(0, gq, pq)
    arrived(dvr.at[1:6], dvsr)
    dv = lax.fori_loop(1, 6, lambda t, acc: acc + dvr[t], dvc[0])
    g_in, g_out = backward(vx, wvo, v_pre, v_hid, v_inv, v_unit, dv * scale)
    pack(gv, g_in, g_out)
    send(gv.at[other], pv, ps.at[1], pr.at[1], mate)
    pair(1, gv, pv)
    scatter(0)
    scatter(1)
    exchange(0)
    exchange(1)
    gather(0)
    finish(0, gqi_o, gqo_o)
    gather(1)
    finish(1, gvi_o, gvo_o)
    gone(lq_all.at[1:NB], ls)
    gone(lows.at[1:NA], lows_s)
    gone(v_all.at[1:NB], vs)
    for h in range(2):
        gone(u_all.at[h, 1:NA], us.at[h])
        gone(zs.at[h, 1:NA], zss.at[h])
        gone(dur.at[h, 1:NA], dus.at[h])
    gone(dvp, dvps)
    gone(dvr.at[1:NC], dvss)
    gone(pq, ps.at[0])
    gone(pv, ps.at[1])
    for i, h, r, o, xx, f, _, _ in paths:
        gone(r.at[1:8], rss.at[0, i])
        gone(xx.at[1:8], rss.at[1, i])
        gone(r.at[1:8], rss.at[2, i])
        gone(h, rss.at[3, i])


def emit(loss, gqi, gqo, gvi, gvo, loss_o, gqi_o, gqo_o, gvi_o, gvo_o, value, sem):
    pairs = ((value, loss_o), (gqi, gqi_o), (gvi, gvi_o), (gqo, gqo_o), (gvo, gvo_o))
    copies = [pltpu.make_async_copy(a, b, sem.at[i]) for i, (a, b) in enumerate(pairs)]
    for c in copies[1:]:
        c.start()
    value[0] = loss[0, 0]
    copies[0].start()
    for c in copies:
        c.wait()


def solution(mesh):
    group = mesh.shape["dp"]

    def local_step(query_feat, item_feat, log_q, w_query_in, w_query_out, w_item_in, w_item_out):
        local_rows = query_feat.shape[0]
        vm = lambda *s: pltpu.VMEM(s, F32)
        vb = lambda *s: pltpu.VMEM(s, BF16)
        sem = lambda *s: pltpu.SemaphoreType.DMA(s)
        one = pltpu.SemaphoreType.DMA
        scratch = [
            vb(256, 512), vb(256, 512), vm(1, 256), vb(512, 256), vb(256, 128), vb(512, 256), vb(256, 128),
            vb(2, NA, 128, 128), vb(NB, 256, 128), vm(NB, 1, 256), vm(NA, 1, 128), vm(NB, 256, 128),
            vm(NB, 2, 4, 256, 256), vm(2, 4, 8, 256), vm(2, NA, 8, 128), vm(2, 4, 1, 256),
            vm(2, NA, 128, 128), vm(2, NA, 128, 128),
            vm(NB, 256, 128), vm(NC, 256, 128), vm(NC, 256, 128), vm(NC, 256, 128), vm(2, 256, 128),
            vm(256, 256), vb(256, 256), vm(256, 128), vm(256, 128),
            vm(256, 256), vb(256, 256), vm(256, 128), vm(256, 128),
            vm(2, 648, 128), vm(2, 640, 128), vm(648, 128), vm(640, 128),
            vm(8, 48, 128), vm(8, 40, 128), vm(8, 40, 128), vm(8, 40, 128),
            vm(8, 48, 128), vm(8, 40, 128), vm(8, 40, 128), vm(8, 40, 128),
            vm(48, 128), vm(40, 128), vm(40, 128), vm(40, 128),
            vm(8, 48, 128), vm(8, 40, 128), vm(8, 40, 128), vm(8, 40, 128),
            vm(2, 8, 48, 128), vm(2, 8, 40, 128), vm(2, 8, 40, 128), vm(2, 8, 40, 128),
            sem(7), sem(2), sem(2), one, sem(NB), one, one, one, one, sem(2), sem(2),
            sem(2), sem(2), one, sem(NC), one, one, sem(2),
            sem(2), sem(2), sem(4, 4), sem(4, 4),
        ]
        vspec = pl.BlockSpec(memory_space=pltpu.VMEM)
        shapes = ((512, 256), (256, 128), (512, 256), (256, 128))
        hbm = pl.BlockSpec(memory_space=pltpu.HBM)
        staged = pl.pallas_call(
            functools.partial(kernel, local_rows * group),
            out_shape=tuple(pltpu.VMEM(s, F32) for s in ((8, 128), *shapes)),
            in_specs=[hbm] * 7,
            out_specs=(vspec,) * 5,
            scratch_shapes=scratch,
            compiler_params=pltpu.CompilerParams(collective_id=0, has_side_effects=True,
                                                 vmem_limit_bytes=56 * 1024 * 1024),
        )(query_feat, item_feat, log_q.reshape(1, local_rows), w_query_in, w_query_out, w_item_in, w_item_out)
        return pl.pallas_call(
            emit,
            out_shape=tuple(jax.ShapeDtypeStruct(s, F32) for s in ((1,), *shapes)),
            in_specs=[vspec] * 5,
            out_specs=(hbm,) * 5,
            scratch_shapes=[pltpu.SMEM((1,), F32), sem(5)],
            compiler_params=pltpu.CompilerParams(vmem_limit_bytes=1024 * 1024),
        )(*staged)

    return jax.shard_map(local_step, mesh=mesh,
                         in_specs=(P("dp", None), P("dp", None), P("dp"), P(), P(), P(), P()),
                         out_specs=(P(), P(), P(), P(), P()), check_vma=False)
```

```python
import functools

import jax
import jax.numpy as jnp
from jax import lax
from jax.experimental import pallas as pl
from jax.experimental.pallas import tpu as pltpu
from jax.sharding import PartitionSpec as P

TEMP = 0.05
NORM_EPS = 1e-6
LOG2E = 1.4426950408889634
BOUND = 20.25
F32 = jnp.float32
BF16 = jnp.bfloat16
NA, NB, NC = 8, 16, 8
STEP = (0, 1, 3, 2)
BACK = (0, 2, 1, 3)
FAR = (7, 6, 3, 5, 2, 4, 1)
PEER_C = ((0, 0), (0, 1), (2, 0), (3, 1), (1, 0), (3, 0), (1, 1), (2, 1))
FAR_C = (7, 6, 3, 2, 5, 4, 1)
INV_C = (0, 1, 2, 6, 5, 4, 3, 7)
INV_A = [2 * BACK[s // 2] + s % 2 for s in range(NA)]
INV_B = [2 * INV_C[t // 2] + t % 2 for t in range(NB)]


def rel_a(r, s):
    dy = (STEP[r // 2] - STEP[s // 2]) % 4
    return 2 * STEP.index(dy) + (r % 2 + s % 2) % 2


def nt(a, b):
    return lax.dot_general(a, b, (((1,), (1,)), ((), ())), preferred_element_type=F32)


def tn(a, b):
    return lax.dot_general(a, b, (((0,), (0,)), ((), ())), preferred_element_type=F32)


def nn(a, b):
    return jnp.dot(a, b, preferred_element_type=F32)


def forward(x, w_in, w_out, pre_s, hid_s, inv_s, unit_s):
    pre = nn(x[...], w_in[...])
    hid = jnp.maximum(pre, 0.0).astype(BF16)
    emb = nn(hid, w_out[...])
    inv = lax.rsqrt(jnp.sum(emb * emb, axis=-1, keepdims=True) + NORM_EPS)
    unit = emb * inv
    pre_s[...] = pre
    hid_s[...] = hid
    inv_s[...] = jnp.broadcast_to(inv, unit.shape)
    unit_s[...] = unit


def backward(x, w_out, pre_s, hid_s, inv_s, unit_s, d_unit):
    unit = unit_s[...]
    d_emb = inv_s[...] * (d_unit - unit * jnp.sum(unit * d_unit, axis=-1, keepdims=True))
    d_emb = d_emb.astype(BF16)
    g_out = tn(hid_s[...], d_emb)
    d_hid = nt(d_emb, w_out[...])
    d_pre = jnp.where(pre_s[...] > 0, d_hid, 0.0).astype(BF16)
    g_in = tn(x[...], d_pre)
    return g_in, g_out


def kernel(total_rows, qx_h, vx_h, lq_h, wqi_h, wqo_h, wvi_h, wvo_h,
           loss_o, gqi_o, gqo_o, gvi_o, gvo_o,
           qx, vx, lq, wqi, wqo, wvi, wvo,
           u_all, v_all, lq_all, lows, kcol, e_all, zacc, zs, rz, dut, dur, dvs, dvp, dvc, dvr, relay,
           q_pre, q_hid, q_inv, q_unit, v_pre, v_hid, v_inv, v_unit,
           gq, gv, pq, pv,
           h0, h1, h2, h3, r0, r1, r2, r3, o0, o1, o2, o3, x0, x1, x2, x3, f0, f1, f2, f3,
           ins, us, ur, vs, vr, ls, lr, lows_s, lows_r, zss, zsr, dus, durs, dvps, dvpr, dvss, dvsr, relay_r,
           ps, pr, rss, rsr):
    me = lax.axis_index("dp")
    core = me % 2
    x = (me // 2) % 4
    y = (me // 8) % 4
    z = me // 32
    lo = ((z + 1) // 2) % 2
    hi = z // 2
    scale = 1.0 / (TEMP * total_rows)
    other = (core + 1) % 2
    mate = z * 32 + y * 8 + x * 2 + other

    def a_dev(s):
        zz = z + (s % 2) * (1 - 2 * (z % 2))
        return zz * 32 + ((y + STEP[s // 2]) % 4) * 8 + x * 2 + core

    def c_dev(t, flip=0):
        dx, dh = PEER_C[t]
        return (z + dh * (3 - 2 * z)) * 32 + y * 8 + ((x + dx) % 4) * 2 + (core + flip) % 2

    def copy(src, dst, ssem, rsem, dev):
        return pltpu.make_async_remote_copy(src_ref=src, dst_ref=dst, send_sem=ssem, recv_sem=rsem,
                                            device_id=(dev,), device_id_type=pl.DeviceIdType.MESH)

    def send(src, dst, ssem, rsem, dev):
        copy(src, dst, ssem, rsem, dev).start()

    def arrived(dst, rsem):
        copy(dst, dst, rsem, rsem, me).wait_recv()

    def gone(src, ssem):
        copy(src, src, ssem, ssem, me).wait_send()

    barrier = pltpu.get_barrier_semaphore()
    partners = [a_dev(s) for s in range(1, NA)] + [c_dev(t // 2, t % 2) for t in range(1, NB)]
    for dev in partners:
        pl.semaphore_signal(barrier, inc=1, device_id=(dev,), device_id_type=pl.DeviceIdType.MESH)

    loads = [pltpu.make_async_copy(a, b, ins.at[i]) for i, (a, b) in enumerate((
        (vx_h, vx), (wvi_h, wvi), (wvo_h, wvo), (qx_h, qx), (wqi_h, wqi), (wqo_h, wqo), (lq_h, lq)))]
    for c in loads:
        c.start()
    for c in loads[:3]:
        c.wait()
    forward(vx, wvi, wvo, v_pre, v_hid, v_inv, v_unit)
    v_all[0] = v_unit[...].astype(BF16)
    for c in loads[3:]:
        c.wait()
    forward(qx, wqi, wqo, q_pre, q_hid, q_inv, q_unit)
    ub = q_unit[...].astype(BF16)
    u_all[0, 0] = ub[0:128]
    u_all[1, 0] = ub[128:256]
    pl.semaphore_wait(barrier, len(partners))
    for t in (15, 14, 13, 12, 11, 10, 5, 4, 9, 8, 7, 6, 3, 2, 1):
        send(lq, lq_all.at[INV_B[t]], ls, lr, c_dev(t // 2, t % 2))
    send(v_all.at[0], v_all.at[1], vs, vr.at[1], mate)
    for s, t in zip(FAR, FAR_C):
        k = 2 * INV_C[t]
        send(u_all.at[0, 0], u_all.at[0, INV_A[s]], us.at[0], ur.at[0], a_dev(s))
        send(v_all.at[0], v_all.at[k], vs, vr.at[k], c_dev(t))
    for t in FAR:
        k = INV_A[t]
        send(u_all.at[1, 0], u_all.at[1, k], us.at[1], ur.at[1], a_dev(t))
    lq_all[0] = lq[...]
    zacc[...] = jnp.zeros_like(zacc)

    low = lq[...]
    arrived(lq_all.at[1:NB], lr)
    for t in range(1, NB):
        low = jnp.minimum(low, lq_all[t])
    low = jnp.min(low, axis=1, keepdims=True)
    lows[0] = jnp.broadcast_to(low, (1, 128))

    table = jnp.concatenate([lq_all[t] for t in range(NB)], axis=0)
    table = jnp.transpose(LOG2E * ((table - low) + BOUND))
    for t in range(NB):
        kcol[t] = jnp.broadcast_to(table[:, t:t + 1], (256, 128))
    for s in FAR:
        send(lows.at[0], lows.at[INV_A[s]], lows_s, lows_r, a_dev(s))
    arrived(u_all.at[0, 1:NA], ur.at[0])

    c2 = LOG2E / TEMP

    def logits(t, h):
        vt = v_all[t]
        kc = kcol[t]
        kc = jnp.concatenate([kc, kc], axis=1)
        for m in range(4):
            um = u_all[h, 2 * m:2 * m + 2].reshape(256, 128)
            e = jnp.exp2(nt(vt, um) * c2 - kc)
            e_all[t, h, m] = e
            zacc[h, m] += jnp.sum(e.reshape(32, 8, 256), axis=0)

    def share(h):
        rows = []
        for m in range(4):
            row = jnp.sum(zacc[h, m], axis=0, keepdims=True)
            rows += [row[:, 0:128], row[:, 128:256]]
        zs[h, 0] = jnp.concatenate(rows, axis=0)

    def share_send(h):
        for s in FAR:
            send(zs.at[h, 0], zs.at[h, INV_A[s]], zss.at[h], zsr.at[h], a_dev(s))

    arrived(v_all.at[1], vr.at[1])
    logits(0, 0)
    logits(1, 0)
    for group in ((6, 1), (4, 7), (3, 2, 5)):
        for t in group:
            arrived(v_all.at[2 * t], vr.at[2 * t])
            copy(v_all.at[2 * t], v_all.at[2 * t + 1], vs, vr.at[2 * t + 1], mate).start()
        for t in group:
            logits(2 * t, 0)
    for group in ((6, 1, 4), (7, 3, 2), (5,)):
        for t in group:
            arrived(v_all.at[2 * t + 1], vr.at[2 * t + 1])
        for t in group:
            logits(2 * t + 1, 0)
    share(0)
    arrived(u_all.at[1, 1:NA], ur.at[1])
    share_send(0)

    def second(n, c):
        for i in range(4):
            logits(4 * n + i, 1)
        return c

    lax.fori_loop(0, NB // 4, second, 0)
    share(1)

    ji = lax.broadcasted_iota(jnp.int32, (256, 256), 0)
    qi = lax.broadcasted_iota(jnp.int32, (256, 256), 1)
    own = q_unit[...].astype(BF16).astype(F32) * v_unit[...].astype(BF16).astype(F32)
    pos = jnp.sum(own) / TEMP
    share_send(1)

    def combine(h):
        arrived(zs.at[h, 1:NA], zsr.at[h])
        tot = []
        for r in range(NA):
            acc = None
            for s in range(NA):
                k = rel_a(r, s)
                term = fac[s] * zs[h, s, k:k + 1, :]
                acc = term if acc is None else acc + term
            tot.append(acc)
        inv = [fac[0] / w for w in tot]
        for m in range(4):
            rz[h, m] = jnp.concatenate([inv[2 * m], inv[2 * m + 1]], axis=1)
        return jnp.log(tot[0])

    def grads(t, h, diag, even=False):
        vt = v_all[t]
        dv = None
        for m in range(4):
            p = e_all[t, h, m] * rz[h, m]
            if diag and m == 0:
                p = jnp.where((ji == qi + h * 128) & (qi < 128), p - 1.0, p)
            g = p.astype(BF16)
            d = nn(g, u_all[h, 2 * m:2 * m + 2].reshape(256, 128))
            dv = d if dv is None else dv + d
            du = tn(vt, g)
            if diag:
                dut[h, 2 * m] = du[:, 0:128]
                dut[h, 2 * m + 1] = du[:, 128:256]
            else:
                dut[h, 2 * m] += du[:, 0:128]
                dut[h, 2 * m + 1] += du[:, 128:256]
        if h == 0:
            dvs[t] = dv
        elif even:
            dvc[t // 2] = dvs[t] + dv + dvp[t // 2]
        else:
            dvs[t] += dv

    arrived(lows.at[1:NA], lows_r)
    lowv = [lows[s] for s in range(NA)]
    least = functools.reduce(jnp.minimum, lowv)
    fac = [jnp.exp(least - w) for w in lowv]
    log0 = combine(0)
    grads(0, 0, True)

    def third(n, c):
        for i in range(1, 4):
            grads(3 * n + i, 0, False)
        return c

    lax.fori_loop(0, 5, third, 0)
    log1 = combine(1)
    for s in FAR:
        send(dut.at[0, s], dur.at[0, INV_A[s]], dus.at[0], durs.at[0], a_dev(s))

    def mate_copy(t):
        return copy(dvs.at[2 * t + 1], dvp.at[t], dvps, dvpr.at[t], mate)

    def dv_send(t):
        if t > 5:
            send(dvc.at[t], relay.at[7 - t], dvss, relay_r.at[7 - t], c_dev(1 if t == 7 else 4))
        else:
            send(dvc.at[t], dvr.at[t], dvss, dvsr, c_dev(t))

    grads(0, 1, True)

    def odd(n, c):
        t = 7 - 2 * n

        @pl.when(n > 0)
        def _():
            mate_copy(t + 1).start()

        grads(2 * t + 1, 1, False)
        grads(2 * t - 1, 1, False)
        mate_copy(t).start()
        return c

    lax.fori_loop(0, 4, odd, 0)

    mate_copy(0).start()
    for t in (7, 5, 3):
        arrived(dvp.at[t], dvpr.at[t])
        arrived(dvp.at[t - 1], dvpr.at[t - 1])
        if t < 7:
            dv_send(t + 1)
        grads(2 * t, 1, False, True)
        grads(2 * t - 2, 1, False, True)
        dv_send(t)
    arrived(dvp.at[1], dvpr.at[1])
    grads(2, 1, False, True)
    for s in FAR:
        send(dut.at[1, s], dur.at[1, INV_A[s]], dus.at[1], durs.at[1], a_dev(s))
    loss_rows = ((BOUND - least) * 2.0 + log0 + log1) + (lq[:, 0:128] + lq[:, 128:256])
    loss_loc = jnp.sum(loss_rows, axis=1, keepdims=True) - pos
    arrived(relay.at[0], relay_r.at[0])
    dvc[2] += relay[0]
    arrived(dvp.at[0], dvpr.at[0])
    dvc[0] = dvs[0] + dvp[0]
    dv_send(2)
    arrived(relay.at[1], relay_r.at[1])
    dvc[1] += relay[1]

    def sum_du(h):
        arrived(dur.at[h, 1:NA], durs.at[h])
        du = dut[h, 0]
        for s in range(1, NA):
            du = du + dur[h, s]
        return jnp.transpose(du)

    parts = [sum_du(0)]
    dv_send(1)
    parts.append(sum_du(1))
    d_unit = jnp.concatenate(parts, axis=0) * scale
    g_in, g_out = backward(qx, wqo, q_pre, q_hid, q_inv, q_unit, d_unit)

    def pack(buf, g_in, g_out):
        buf[0, 0:512, :] = g_in[:, 0:128]
        buf[0, 512:640, :] = g_in[0:128, 128:256]
        buf[1, 0:384, :] = g_in[128:512, 128:256]
        buf[1, 384:640, :] = g_out

    pack(gq, g_in, g_out)
    lt = jnp.broadcast_to(loss_loc, (8, 128))
    gq[0, 640:648, :] = lt
    gq[1, 640:648, :] = lt
    send(gq.at[other], pq, ps.at[0], pr.at[0], mate)

    a_me, b_me = y * 2 + lo, x * 2 + hi

    def a_idx(s):
        return ((y + STEP[s // 2]) % 4) * 2 + (lo + s % 2) % 2

    def c_idx(t):
        return ((x + PEER_C[t][0]) % 4) * 2 + (hi + PEER_C[t][1]) % 2

    side_a, side_c = (a_dev, a_idx, a_me, FAR, INV_A), (c_dev, c_idx, b_me, FAR_C, INV_C)
    paths = (
        (0, h0, r0, o0, x0, f0, side_c, side_a),
        (1, h1, r1, o1, x1, f1, side_a, side_c),
        (2, h2, r2, o2, x2, f2, side_a, side_c),
        (3, h3, r3, o3, x3, f3, side_c, side_a),
    )

    def pair(w, g, p):
        arrived(p, pr.at[w])
        for i, h, r, o, xx, f, (dev, idx, mine, far, inv), _ in paths[2 * w:2 * w + 2]:
            base = 320 * (i % 2)
            h[:, 0:40, :] = (g[core, base:base + 320, :] + p[base:base + 320, :]).reshape(8, 40, 128)
            if i == 0:
                extra = g[core, 640:648, :] + p[640:648, :]
                for n in range(8):
                    h[n, 40:48, :] = extra
        for i, h, r, o, xx, f, (dev, idx, mine, far, inv), _ in paths[2 * w:2 * w + 2]:
            for s in far:
                send(h.at[idx(s)], r.at[inv[s]], rss.at[0, i], rsr.at[0, i], dev(s))

    def scatter(w):
        for i, h, r, o, xx, f, (_, _, mine, _, _), (dev, _, _, far, inv) in paths[2 * w:2 * w + 2]:
            arrived(r.at[1:8], rsr.at[0, i])
            acc = h[mine]
            for s in range(1, 8):
                acc = acc + r[s]
            o[...] = acc
            for s in far:
                send(o, xx.at[inv[s]], rss.at[1, i], rsr.at[1, i], dev(s))

    def exchange(w):
        for i, h, r, o, xx, f, (dev, idx, mine, far, inv), _ in paths[2 * w:2 * w + 2]:
            arrived(xx.at[1:8], rsr.at[1, i])
            acc = o[...]
            for s in range(1, 8):
                acc = acc + xx[s]
            f[core, mine] = acc
            for s in far:
                send(f.at[core, mine], f.at[core, mine], rss.at[2, i], rsr.at[2, i], dev(s))
            if i == 0:
                loss_o[...] = acc[40:48] * (1.0 / total_rows)

    def gather(w):
        for i, h, r, o, xx, f, _, _ in paths[2 * w:2 * w + 2]:
            arrived(r.at[1:8], rsr.at[2, i])
            send(f.at[core], f.at[core], rss.at[3, i], rsr.at[3, i], mate)

    def finish(w, go_in, go_out):
        halves = [[], []]
        for i, h, r, o, xx, f, _, _ in paths[2 * w:2 * w + 2]:
            arrived(h, rsr.at[3, i])
            for c in range(2):
                halves[c].append(f[c, :, 0:40, :].reshape(320, 128))
        head, tail = [jnp.concatenate(c, axis=0) for c in halves]
        go_in[:, 0:128] = head[0:512]
        go_in[0:128, 128:256] = head[512:640]
        go_in[128:512, 128:256] = tail[0:384]
        go_out[...] = tail[384:640]

    pair(0, gq, pq)
    arrived(dvr.at[1:6], dvsr)
    dv = lax.fori_loop(1, 6, lambda t, acc: acc + dvr[t], dvc[0])
    g_in, g_out = backward(vx, wvo, v_pre, v_hid, v_inv, v_unit, dv * scale)
    pack(gv, g_in, g_out)
    send(gv.at[other], pv, ps.at[1], pr.at[1], mate)
    pair(1, gv, pv)
    scatter(0)
    scatter(1)
    exchange(0)
    exchange(1)
    gather(0)
    finish(0, gqi_o, gqo_o)
    gather(1)
    finish(1, gvi_o, gvo_o)
    gone(lq_all.at[1:NB], ls)
    gone(lows.at[1:NA], lows_s)
    gone(v_all.at[1:NB], vs)
    for h in range(2):
        gone(u_all.at[h, 1:NA], us.at[h])
        gone(zs.at[h, 1:NA], zss.at[h])
        gone(dur.at[h, 1:NA], dus.at[h])
    gone(dvp, dvps)
    gone(dvr.at[1:NC], dvss)
    gone(pq, ps.at[0])
    gone(pv, ps.at[1])
    for i, h, r, o, xx, f, _, _ in paths:
        gone(r.at[1:8], rss.at[0, i])
        gone(xx.at[1:8], rss.at[1, i])
        gone(r.at[1:8], rss.at[2, i])
        gone(h, rss.at[3, i])


def emit(loss, gqi, gqo, gvi, gvo, loss_o, gqi_o, gqo_o, gvi_o, gvo_o, value, sem):
    pairs = ((value, loss_o), (gqi, gqi_o), (gvi, gvi_o), (gqo, gqo_o), (gvo, gvo_o))
    copies = [pltpu.make_async_copy(a, b, sem.at[i]) for i, (a, b) in enumerate(pairs)]
    for c in copies[1:]:
        c.start()
    value[0] = loss[0, 0]
    copies[0].start()
    for c in copies:
        c.wait()


def solution(mesh):
    group = mesh.shape["dp"]

    def local_step(query_feat, item_feat, log_q, w_query_in, w_query_out, w_item_in, w_item_out):
        local_rows = query_feat.shape[0]
        vm = lambda *s: pltpu.VMEM(s, F32)
        vb = lambda *s: pltpu.VMEM(s, BF16)
        sem = lambda *s: pltpu.SemaphoreType.DMA(s)
        one = pltpu.SemaphoreType.DMA
        scratch = [
            vb(256, 512), vb(256, 512), vm(1, 256), vb(512, 256), vb(256, 128), vb(512, 256), vb(256, 128),
            vb(2, NA, 128, 128), vb(NB, 256, 128), vm(NB, 1, 256), vm(NA, 1, 128), vm(NB, 256, 128),
            vm(NB, 2, 4, 256, 256), vm(2, 4, 8, 256), vm(2, NA, 8, 128), vm(2, 4, 1, 256),
            vm(2, NA, 128, 128), vm(2, NA, 128, 128),
            vm(NB, 256, 128), vm(NC, 256, 128), vm(NC, 256, 128), vm(NC, 256, 128), vm(2, 256, 128),
            vm(256, 256), vb(256, 256), vm(256, 128), vm(256, 128),
            vm(256, 256), vb(256, 256), vm(256, 128), vm(256, 128),
            vm(2, 648, 128), vm(2, 640, 128), vm(648, 128), vm(640, 128),
            vm(8, 48, 128), vm(8, 40, 128), vm(8, 40, 128), vm(8, 40, 128),
            vm(8, 48, 128), vm(8, 40, 128), vm(8, 40, 128), vm(8, 40, 128),
            vm(48, 128), vm(40, 128), vm(40, 128), vm(40, 128),
            vm(8, 48, 128), vm(8, 40, 128), vm(8, 40, 128), vm(8, 40, 128),
            vm(2, 8, 48, 128), vm(2, 8, 40, 128), vm(2, 8, 40, 128), vm(2, 8, 40, 128),
            sem(7), sem(2), sem(2), one, sem(NB), one, one, one, one, sem(2), sem(2),
            sem(2), sem(2), one, sem(NC), one, one, sem(2),
            sem(2), sem(2), sem(4, 4), sem(4, 4),
        ]
        vspec = pl.BlockSpec(memory_space=pltpu.VMEM)
        shapes = ((512, 256), (256, 128), (512, 256), (256, 128))
        hbm = pl.BlockSpec(memory_space=pltpu.HBM)
        staged = pl.pallas_call(
            functools.partial(kernel, local_rows * group),
            out_shape=tuple(pltpu.VMEM(s, F32) for s in ((8, 128), *shapes)),
            in_specs=[hbm] * 7,
            out_specs=(vspec,) * 5,
            scratch_shapes=scratch,
            compiler_params=pltpu.CompilerParams(collective_id=0, has_side_effects=True,
                                                 vmem_limit_bytes=56 * 1024 * 1024),
        )(query_feat, item_feat, log_q.reshape(1, local_rows), w_query_in, w_query_out, w_item_in, w_item_out)
        return pl.pallas_call(
            emit,
            out_shape=tuple(jax.ShapeDtypeStruct(s, F32) for s in ((1,), *shapes)),
            in_specs=[vspec] * 5,
            out_specs=(hbm,) * 5,
            scratch_shapes=[pltpu.SMEM((1,), F32), sem(5)],
            compiler_params=pltpu.CompilerParams(vmem_limit_bytes=1024 * 1024),
        )(*staged)

    return jax.shard_map(local_step, mesh=mesh,
                         in_specs=(P("dp", None), P("dp", None), P("dp"), P(), P(), P(), P()),
                         out_specs=(P(), P(), P(), P(), P()), check_vma=False)
```

```python
import functools

import jax
import jax.numpy as jnp
from jax import lax
from jax.experimental import pallas as pl
from jax.experimental.pallas import tpu as pltpu
from jax.sharding import PartitionSpec as P

TEMP = 0.05
NORM_EPS = 1e-6
LOG2E = 1.4426950408889634
BOUND = 20.25
F32 = jnp.float32
BF16 = jnp.bfloat16
NA, NB, NC = 8, 16, 8
STEP = (0, 1, 3, 2)
BACK = (0, 2, 1, 3)
FAR = (7, 6, 3, 5, 2, 4, 1)
PEER_C = ((0, 0), (0, 1), (2, 0), (3, 1), (1, 0), (3, 0), (1, 1), (2, 1))
FAR_C = (7, 6, 3, 2, 5, 4, 1)
GROUPS = ((0,), (12, 2), (8, 14), (6, 4, 10), (13, 3, 9), (15, 7, 5), (11,), (1,))
V_SEM = {s: i for i, g in enumerate(GROUPS) for s in g}
INV_C = (0, 1, 2, 6, 5, 4, 3, 7)
INV_A = [2 * BACK[s // 2] + s % 2 for s in range(NA)]
INV_B = [2 * INV_C[t // 2] + t % 2 for t in range(NB)]


def rel_a(r, s):
    dy = (STEP[r // 2] - STEP[s // 2]) % 4
    return 2 * STEP.index(dy) + (r % 2 + s % 2) % 2


def nt(a, b):
    return lax.dot_general(a, b, (((1,), (1,)), ((), ())), preferred_element_type=F32)


def tn(a, b):
    return lax.dot_general(a, b, (((0,), (0,)), ((), ())), preferred_element_type=F32)


def nn(a, b):
    return jnp.dot(a, b, preferred_element_type=F32)


def forward(x, w_in, w_out, pre_s, hid_s, inv_s, unit_s):
    pre = nn(x[...], w_in[...])
    hid = jnp.maximum(pre, 0.0).astype(BF16)
    emb = nn(hid, w_out[...])
    inv = lax.rsqrt(jnp.sum(emb * emb, axis=-1, keepdims=True) + NORM_EPS)
    unit = emb * inv
    pre_s[...] = pre
    hid_s[...] = hid
    inv_s[...] = jnp.broadcast_to(inv, unit.shape)
    unit_s[...] = unit


def backward(x, w_out, pre_s, hid_s, inv_s, unit_s, d_unit):
    unit = unit_s[...]
    d_emb = inv_s[...] * (d_unit - unit * jnp.sum(unit * d_unit, axis=-1, keepdims=True))
    d_emb = d_emb.astype(BF16)
    g_out = tn(hid_s[...], d_emb)
    d_hid = nt(d_emb, w_out[...])
    d_pre = jnp.where(pre_s[...] > 0, d_hid, 0.0).astype(BF16)
    g_in = tn(x[...], d_pre)
    return g_in, g_out


def kernel(total_rows, qx_h, vx_h, lq_h, wqi_h, wqo_h, wvi_h, wvo_h,
           loss_o, gqi_o, gqo_o, gvi_o, gvo_o,
           qx, vx, lq, wqi, wqo, wvi, wvo,
           u_all, v_all, lq_all, lows, kcol, e_all, zacc, zs, rz, dut, dur, dvs, dvp, dvc, dvr, relay, v_t,
           q_pre, q_hid, q_inv, q_unit, v_pre, v_hid, v_inv, v_unit,
           gq, gv, pq, pv,
           h0, h1, h2, h3, r0, r1, r2, r3, o0, o1, o2, o3, x0, x1, x2, x3, f0, f1, f2, f3,
           ins, us, ur, vs, vr, ls, lr, lows_s, lows_r, zss, zsr, dus, durs, dvps, dvpr, dvss, dvsr, relay_r,
           ps, pr, rss, rsr):
    me = lax.axis_index("dp")
    core = me % 2
    x = (me // 2) % 4
    y = (me // 8) % 4
    z = me // 32
    lo = ((z + 1) // 2) % 2
    hi = z // 2
    scale = 1.0 / (TEMP * total_rows)
    other = (core + 1) % 2
    mate = z * 32 + y * 8 + x * 2 + other

    def a_dev(s):
        zz = z + (s % 2) * (1 - 2 * (z % 2))
        return zz * 32 + ((y + STEP[s // 2]) % 4) * 8 + x * 2 + core

    def c_dev(t, flip=0):
        dx, dh = PEER_C[t]
        return (z + dh * (3 - 2 * z)) * 32 + y * 8 + ((x + dx) % 4) * 2 + (core + flip) % 2

    def copy(src, dst, ssem, rsem, dev):
        return pltpu.make_async_remote_copy(src_ref=src, dst_ref=dst, send_sem=ssem, recv_sem=rsem,
                                            device_id=(dev,), device_id_type=pl.DeviceIdType.MESH)

    def send(src, dst, ssem, rsem, dev):
        copy(src, dst, ssem, rsem, dev).start()

    def arrived(dst, rsem):
        copy(dst, dst, rsem, rsem, me).wait_recv()

    def gone(src, ssem):
        copy(src, src, ssem, ssem, me).wait_send()

    barrier = pltpu.get_barrier_semaphore()
    partners = [a_dev(s) for s in range(1, NA)] + [c_dev(t // 2, t % 2) for t in range(1, NB)]
    for dev in partners:
        pl.semaphore_signal(barrier, inc=1, device_id=(dev,), device_id_type=pl.DeviceIdType.MESH)

    loads = [pltpu.make_async_copy(a, b, ins.at[i]) for i, (a, b) in enumerate((
        (vx_h, vx), (wvi_h, wvi), (wvo_h, wvo), (qx_h, qx), (wqi_h, wqi), (wqo_h, wqo), (lq_h, lq)))]
    for c in loads:
        c.start()
    for c in loads[:3]:
        c.wait()
    forward(vx, wvi, wvo, v_pre, v_hid, v_inv, v_unit)
    v_all[0] = v_unit[...].astype(BF16)
    for c in loads[3:]:
        c.wait()
    forward(qx, wqi, wqo, q_pre, q_hid, q_inv, q_unit)
    ub = q_unit[...].astype(BF16)
    u_all[0, 0] = ub[0:128]
    u_all[1, 0] = ub[128:256]
    pl.semaphore_wait(barrier, len(partners))
    for t in (15, 14, 13, 12, 11, 10, 5, 4, 9, 8, 7, 6, 3, 2, 1):
        send(lq, lq_all.at[INV_B[t]], ls, lr, c_dev(t // 2, t % 2))
    send(v_all.at[0], v_all.at[1], vs, vr.at[V_SEM[1]], mate)
    for s, t in zip(FAR, FAR_C):
        k = 2 * INV_C[t]
        send(u_all.at[0, 0], u_all.at[0, INV_A[s]], us.at[0], ur.at[0], a_dev(s))
        send(v_all.at[0], v_all.at[k], vs, vr.at[V_SEM[k]], c_dev(t))
    for t in FAR:
        k = INV_A[t]
        send(u_all.at[1, 0], u_all.at[1, k], us.at[1], ur.at[1], a_dev(t))
    lq_all[0] = lq[...]
    zacc[...] = jnp.zeros_like(zacc)

    low = lq[...]
    arrived(lq_all.at[1:NB], lr)
    for t in range(1, NB):
        low = jnp.minimum(low, lq_all[t])
    low = jnp.min(low, axis=1, keepdims=True)
    lows[0] = jnp.broadcast_to(low, (1, 128))

    table = jnp.concatenate([lq_all[t] for t in range(NB)], axis=0)
    table = jnp.transpose(LOG2E * ((table - low) + BOUND))
    for t in range(NB):
        kcol[t] = jnp.broadcast_to(table[:, t:t + 1], (256, 128))
    for s in FAR:
        send(lows.at[0], lows.at[INV_A[s]], lows_s, lows_r, a_dev(s))
    arrived(u_all.at[0, 1:NA], ur.at[0])

    c2 = LOG2E / TEMP

    def logits(t, h):
        vt = v_all[t]
        kc = kcol[t]
        kc = jnp.concatenate([kc, kc], axis=1)
        for m in range(4):
            um = u_all[h, 2 * m:2 * m + 2].reshape(256, 128)
            e = jnp.exp2(nt(vt, um) * c2 - kc)
            e_all[t, h, m] = e
            zacc[h, m] += jnp.sum(e.reshape(32, 8, 256), axis=0)

    def share(h):
        rows = []
        for m in range(4):
            row = jnp.sum(zacc[h, m], axis=0, keepdims=True)
            rows += [row[:, 0:128], row[:, 128:256]]
        zs[h, 0] = jnp.concatenate(rows, axis=0)

    def share_send(h):
        for s in FAR:
            send(zs.at[h, 0], zs.at[h, INV_A[s]], zss.at[h], zsr.at[h], a_dev(s))

    arrived(v_all.at[1], vr.at[V_SEM[1]])
    logits(0, 0)
    logits(1, 0)
    for i, group in enumerate(GROUPS[1:4]):
        arrived(v_all.at[0:len(group)], vr.at[i + 1])
        for t in group:
            copy(v_all.at[t], v_all.at[t + 1], vs, vr.at[V_SEM[t + 1]], mate).start()
        for t in group:
            logits(t, 0)
    for i, group in enumerate(GROUPS[4:7]):
        arrived(v_all.at[0:len(group)], vr.at[i + 4])
        for t in group:
            logits(t, 0)
    share(0)
    arrived(u_all.at[1, 1:NA], ur.at[1])
    share_send(0)

    def second(n, c):
        for i in range(8):
            logits(8 * n + i, 1)
        return c

    lax.fori_loop(0, NB // 8, second, 0)
    share(1)

    ji = lax.broadcasted_iota(jnp.int32, (256, 256), 0)
    qi = lax.broadcasted_iota(jnp.int32, (256, 256), 1)
    own = q_unit[...].astype(BF16).astype(F32) * v_unit[...].astype(BF16).astype(F32)
    pos = jnp.sum(own) / TEMP
    share_send(1)

    def combine(h):
        arrived(zs.at[h, 1:NA], zsr.at[h])
        tot = []
        for r in range(NA):
            acc = None
            for s in range(NA):
                k = rel_a(r, s)
                term = fac[s] * zs[h, s, k:k + 1, :]
                acc = term if acc is None else acc + term
            tot.append(acc)
        inv = [fac[0] / w for w in tot]
        for m in range(4):
            rz[h, m] = jnp.concatenate([inv[2 * m], inv[2 * m + 1]], axis=1)
        return jnp.log(tot[0])

    def grads(t, h, diag, even=False):
        vt = v_t[t]
        dv = None
        for m in range(4):
            p = e_all[t, h, m] * rz[h, m]
            if diag and m == 0:
                p = jnp.where((ji == qi + h * 128) & (qi < 128), p - 1.0, p)
            g = p.astype(BF16)
            d = nn(g, u_all[h, 2 * m:2 * m + 2].reshape(256, 128))
            dv = d if dv is None else dv + d
            du = nn(vt, g)
            if diag:
                dut[h, 2 * m] = du[:, 0:128]
                dut[h, 2 * m + 1] = du[:, 128:256]
            else:
                dut[h, 2 * m] += du[:, 0:128]
                dut[h, 2 * m + 1] += du[:, 128:256]
        if h == 0:
            dvs[t] = dv
        elif even:
            dvc[t // 2] = dvs[t] + dv + dvp[t // 2]
        else:
            dvs[t] += dv

    for t in range(NB):
        v_t[t] = jnp.transpose(v_all[t])
    arrived(lows.at[1:NA], lows_r)
    lowv = [lows[s] for s in range(NA)]
    least = functools.reduce(jnp.minimum, lowv)
    fac = [jnp.exp(least - w) for w in lowv]
    log0 = combine(0)
    grads(0, 0, True)

    def third(n, c):
        for i in range(1, 6):
            grads(5 * n + i, 0, False)
        return c

    lax.fori_loop(0, 3, third, 0)
    log1 = combine(1)
    for s in FAR:
        send(dut.at[0, s], dur.at[0, INV_A[s]], dus.at[0], durs.at[0], a_dev(s))

    def mate_copy(t):
        return copy(dvs.at[2 * t + 1], dvp.at[t], dvps, dvpr.at[t], mate)

    def dv_send(t):
        if t > 5:
            send(dvc.at[t], relay.at[7 - t], dvss, relay_r.at[7 - t], c_dev(1 if t == 7 else 4))
        else:
            send(dvc.at[t], dvr.at[t], dvss, dvsr, c_dev(t))

    grads(0, 1, True)

    def odd(n, c):
        t = 7 - 2 * n

        @pl.when(n > 0)
        def _():
            mate_copy(t + 1).start()

        grads(2 * t + 1, 1, False)
        grads(2 * t - 1, 1, False)
        mate_copy(t).start()
        return c

    lax.fori_loop(0, 4, odd, 0)

    mate_copy(0).start()
    for t in (7, 5, 3):
        arrived(dvp.at[t], dvpr.at[t])
        arrived(dvp.at[t - 1], dvpr.at[t - 1])
        if t < 7:
            dv_send(t + 1)
        grads(2 * t, 1, False, True)
        grads(2 * t - 2, 1, False, True)
        dv_send(t)
    arrived(dvp.at[1], dvpr.at[1])
    grads(2, 1, False, True)
    for s in FAR:
        send(dut.at[1, s], dur.at[1, INV_A[s]], dus.at[1], durs.at[1], a_dev(s))
    loss_rows = ((BOUND - least) * 2.0 + log0 + log1) + (lq[:, 0:128] + lq[:, 128:256])
    loss_loc = jnp.sum(loss_rows, axis=1, keepdims=True) - pos
    arrived(relay.at[0], relay_r.at[0])
    dvc[2] += relay[0]
    arrived(dvp.at[0], dvpr.at[0])
    dvc[0] = dvs[0] + dvp[0]
    dv_send(2)
    arrived(relay.at[1], relay_r.at[1])
    dvc[1] += relay[1]

    def sum_du(h):
        arrived(dur.at[h, 1:NA], durs.at[h])
        du = dut[h, 0]
        for s in range(1, NA):
            du = du + dur[h, s]
        return jnp.transpose(du)

    parts = [sum_du(0)]
    dv_send(1)
    parts.append(sum_du(1))
    d_unit = jnp.concatenate(parts, axis=0) * scale
    g_in, g_out = backward(qx, wqo, q_pre, q_hid, q_inv, q_unit, d_unit)

    def pack(buf, g_in, g_out):
        buf[0, 0:512, :] = g_in[:, 0:128]
        buf[0, 512:640, :] = g_in[0:128, 128:256]
        buf[1, 0:384, :] = g_in[128:512, 128:256]
        buf[1, 384:640, :] = g_out

    pack(gq, g_in, g_out)
    lt = jnp.broadcast_to(loss_loc, (8, 128))
    gq[0, 640:648, :] = lt
    gq[1, 640:648, :] = lt
    send(gq.at[other], pq, ps.at[0], pr.at[0], mate)

    a_me, b_me = y * 2 + lo, x * 2 + hi

    def a_idx(s):
        return ((y + STEP[s // 2]) % 4) * 2 + (lo + s % 2) % 2

    def c_idx(t):
        return ((x + PEER_C[t][0]) % 4) * 2 + (hi + PEER_C[t][1]) % 2

    side_a, side_c = (a_dev, a_idx, a_me, FAR, INV_A), (c_dev, c_idx, b_me, FAR_C, INV_C)
    paths = (
        (0, h0, r0, o0, x0, f0, side_c, side_a),
        (1, h1, r1, o1, x1, f1, side_a, side_c),
        (2, h2, r2, o2, x2, f2, side_a, side_c),
        (3, h3, r3, o3, x3, f3, side_c, side_a),
    )

    def pair(w, g, p):
        arrived(p, pr.at[w])
        for i, h, r, o, xx, f, (dev, idx, mine, far, inv), _ in paths[2 * w:2 * w + 2]:
            base = 320 * (i % 2)
            h[:, 0:40, :] = (g[core, base:base + 320, :] + p[base:base + 320, :]).reshape(8, 40, 128)
            if i == 0:
                extra = g[core, 640:648, :] + p[640:648, :]
                for n in range(8):
                    h[n, 40:48, :] = extra
        for i, h, r, o, xx, f, (dev, idx, mine, far, inv), _ in paths[2 * w:2 * w + 2]:
            for s in far:
                send(h.at[idx(s)], r.at[inv[s]], rss.at[0, i], rsr.at[0, i], dev(s))

    def scatter(w):
        for i, h, r, o, xx, f, (_, _, mine, _, _), (dev, _, _, far, inv) in paths[2 * w:2 * w + 2]:
            arrived(r.at[1:8], rsr.at[0, i])
            acc = h[mine]
            for s in range(1, 8):
                acc = acc + r[s]
            o[...] = acc
            for s in far:
                send(o, xx.at[inv[s]], rss.at[1, i], rsr.at[1, i], dev(s))

    def exchange(w):
        for i, h, r, o, xx, f, (dev, idx, mine, far, inv), _ in paths[2 * w:2 * w + 2]:
            arrived(xx.at[1:8], rsr.at[1, i])
            acc = o[...]
            for s in range(1, 8):
                acc = acc + xx[s]
            f[core, mine] = acc
            for s in far:
                send(f.at[core, mine], f.at[core, mine], rss.at[2, i], rsr.at[2, i], dev(s))
            if i == 0:
                loss_o[...] = acc[40:48] * (1.0 / total_rows)

    def gather(w):
        for i, h, r, o, xx, f, _, _ in paths[2 * w:2 * w + 2]:
            arrived(r.at[1:8], rsr.at[2, i])
            send(f.at[core], f.at[core], rss.at[3, i], rsr.at[3, i], mate)

    def finish(w, go_in, go_out):
        halves = [[], []]
        for i, h, r, o, xx, f, _, _ in paths[2 * w:2 * w + 2]:
            arrived(h, rsr.at[3, i])
            for c in range(2):
                halves[c].append(f[c, :, 0:40, :].reshape(320, 128))
        head, tail = [jnp.concatenate(c, axis=0) for c in halves]
        go_in[:, 0:128] = head[0:512]
        go_in[0:128, 128:256] = head[512:640]
        go_in[128:512, 128:256] = tail[0:384]
        go_out[...] = tail[384:640]

    pair(0, gq, pq)
    arrived(dvr.at[1:6], dvsr)
    dv = lax.fori_loop(1, 6, lambda t, acc: acc + dvr[t], dvc[0])
    g_in, g_out = backward(vx, wvo, v_pre, v_hid, v_inv, v_unit, dv * scale)
    pack(gv, g_in, g_out)
    send(gv.at[other], pv, ps.at[1], pr.at[1], mate)
    pair(1, gv, pv)
    scatter(0)
    scatter(1)
    exchange(0)
    exchange(1)
    gather(0)
    finish(0, gqi_o, gqo_o)
    gather(1)
    finish(1, gvi_o, gvo_o)
    gone(lq_all.at[1:NB], ls)
    gone(lows.at[1:NA], lows_s)
    gone(v_all.at[1:NB], vs)
    for h in range(2):
        gone(u_all.at[h, 1:NA], us.at[h])
        gone(zs.at[h, 1:NA], zss.at[h])
        gone(dur.at[h, 1:NA], dus.at[h])
    gone(dvp, dvps)
    gone(dvr.at[1:NC], dvss)
    gone(pq, ps.at[0])
    gone(pv, ps.at[1])
    for i, h, r, o, xx, f, _, _ in paths:
        gone(r.at[1:8], rss.at[0, i])
        gone(xx.at[1:8], rss.at[1, i])
        gone(r.at[1:8], rss.at[2, i])
        gone(h, rss.at[3, i])


def emit(loss, gqi, gqo, gvi, gvo, loss_o, gqi_o, gqo_o, gvi_o, gvo_o, value, sem):
    pairs = ((value, loss_o), (gqi, gqi_o), (gvi, gvi_o), (gqo, gqo_o), (gvo, gvo_o))
    copies = [pltpu.make_async_copy(a, b, sem.at[i]) for i, (a, b) in enumerate(pairs)]
    for c in copies[1:]:
        c.start()
    value[0] = loss[0, 0]
    copies[0].start()
    for c in copies:
        c.wait()


def solution(mesh):
    group = mesh.shape["dp"]

    def local_step(query_feat, item_feat, log_q, w_query_in, w_query_out, w_item_in, w_item_out):
        local_rows = query_feat.shape[0]
        vm = lambda *s: pltpu.VMEM(s, F32)
        vb = lambda *s: pltpu.VMEM(s, BF16)
        sem = lambda *s: pltpu.SemaphoreType.DMA(s)
        one = pltpu.SemaphoreType.DMA
        scratch = [
            vb(256, 512), vb(256, 512), vm(1, 256), vb(512, 256), vb(256, 128), vb(512, 256), vb(256, 128),
            vb(2, NA, 128, 128), vb(NB, 256, 128), vm(NB, 1, 256), vm(NA, 1, 128), vm(NB, 256, 128),
            vm(NB, 2, 4, 256, 256), vm(2, 4, 8, 256), vm(2, NA, 8, 128), vm(2, 4, 1, 256),
            vm(2, NA, 128, 128), vm(2, NA, 128, 128),
            vm(NB, 256, 128), vm(NC, 256, 128), vm(NC, 256, 128), vm(NC, 256, 128), vm(2, 256, 128), vb(NB, 128, 256),
            vm(256, 256), vb(256, 256), vm(256, 128), vm(256, 128),
            vm(256, 256), vb(256, 256), vm(256, 128), vm(256, 128),
            vm(2, 648, 128), vm(2, 640, 128), vm(648, 128), vm(640, 128),
            vm(8, 48, 128), vm(8, 40, 128), vm(8, 40, 128), vm(8, 40, 128),
            vm(8, 48, 128), vm(8, 40, 128), vm(8, 40, 128), vm(8, 40, 128),
            vm(48, 128), vm(40, 128), vm(40, 128), vm(40, 128),
            vm(8, 48, 128), vm(8, 40, 128), vm(8, 40, 128), vm(8, 40, 128),
            vm(2, 8, 48, 128), vm(2, 8, 40, 128), vm(2, 8, 40, 128), vm(2, 8, 40, 128),
            sem(7), sem(2), sem(2), one, sem(8), one, one, one, one, sem(2), sem(2),
            sem(2), sem(2), one, sem(NC), one, one, sem(2),
            sem(2), sem(2), sem(4, 4), sem(4, 4),
        ]
        vspec = pl.BlockSpec(memory_space=pltpu.VMEM)
        shapes = ((512, 256), (256, 128), (512, 256), (256, 128))
        hbm = pl.BlockSpec(memory_space=pltpu.HBM)
        staged = pl.pallas_call(
            functools.partial(kernel, local_rows * group),
            out_shape=tuple(pltpu.VMEM(s, F32) for s in ((8, 128), *shapes)),
            in_specs=[hbm] * 7,
            out_specs=(vspec,) * 5,
            scratch_shapes=scratch,
            compiler_params=pltpu.CompilerParams(collective_id=0, has_side_effects=True,
                                                 vmem_limit_bytes=56 * 1024 * 1024),
        )(query_feat, item_feat, log_q.reshape(1, local_rows), w_query_in, w_query_out, w_item_in, w_item_out)
        return pl.pallas_call(
            emit,
            out_shape=tuple(jax.ShapeDtypeStruct(s, F32) for s in ((1,), *shapes)),
            in_specs=[vspec] * 5,
            out_specs=(hbm,) * 5,
            scratch_shapes=[pltpu.SMEM((1,), F32), sem(5)],
            compiler_params=pltpu.CompilerParams(vmem_limit_bytes=1024 * 1024),
        )(*staged)

    return jax.shard_map(local_step, mesh=mesh,
                         in_specs=(P("dp", None), P("dp", None), P("dp"), P(), P(), P(), P()),
                         out_specs=(P(), P(), P(), P(), P()), check_vma=False)
```

```python
import functools

import jax
import jax.numpy as jnp
from jax import lax
from jax.experimental import pallas as pl
from jax.experimental.pallas import tpu as pltpu
from jax.sharding import PartitionSpec as P

TEMP = 0.05
NORM_EPS = 1e-6
LOG2E = 1.4426950408889634
BOUND = 20.25
F32 = jnp.float32
BF16 = jnp.bfloat16
NA, NB, NC = 8, 16, 8
STEP = (0, 1, 3, 2)
BACK = (0, 2, 1, 3)
FAR = (7, 6, 3, 5, 2, 4, 1)
PEER_C = ((0, 0), (0, 1), (2, 0), (3, 1), (1, 0), (3, 0), (1, 1), (2, 1))
FAR_C = (7, 6, 3, 2, 5, 4, 1)
GROUPS = ((0,), (12, 2), (8, 14), (6, 4, 10), (13, 3, 9), (15, 7, 5), (11,), (1,))
V_SEM = {s: i for i, g in enumerate(GROUPS) for s in g}
INV_C = (0, 1, 2, 6, 5, 4, 3, 7)
INV_A = [2 * BACK[s // 2] + s % 2 for s in range(NA)]
INV_B = [2 * INV_C[t // 2] + t % 2 for t in range(NB)]


def rel_a(r, s):
    dy = (STEP[r // 2] - STEP[s // 2]) % 4
    return 2 * STEP.index(dy) + (r % 2 + s % 2) % 2


def nt(a, b):
    return lax.dot_general(a, b, (((1,), (1,)), ((), ())), preferred_element_type=F32)


def tn(a, b):
    return lax.dot_general(a, b, (((0,), (0,)), ((), ())), preferred_element_type=F32)


def nn(a, b):
    return jnp.dot(a, b, preferred_element_type=F32)


def forward(x, w_in, w_out, pre_s, hid_s, inv_s, unit_s):
    pre = nn(x[...], w_in[...])
    hid = jnp.maximum(pre, 0.0).astype(BF16)
    emb = nn(hid, w_out[...])
    inv = lax.rsqrt(jnp.sum(emb * emb, axis=-1, keepdims=True) + NORM_EPS)
    unit = emb * inv
    pre_s[...] = pre
    hid_s[...] = hid
    inv_s[...] = jnp.broadcast_to(inv, unit.shape)
    unit_s[...] = unit


def backward(x, w_out, pre_s, hid_s, inv_s, unit_s, d_unit):
    unit = unit_s[...]
    d_emb = inv_s[...] * (d_unit - unit * jnp.sum(unit * d_unit, axis=-1, keepdims=True))
    d_emb = d_emb.astype(BF16)
    g_out = tn(hid_s[...], d_emb)
    d_hid = nt(d_emb, w_out[...])
    d_pre = jnp.where(pre_s[...] > 0, d_hid, 0.0).astype(BF16)
    g_in = tn(x[...], d_pre)
    return g_in, g_out


def kernel(total_rows, qx_h, vx_h, lq_h, wqi_h, wqo_h, wvi_h, wvo_h,
           loss_o, gqi_o, gqo_o, gvi_o, gvo_o,
           qx, vx, lq, wqi, wqo, wvi, wvo,
           u_all, v_all, lq_all, lows, kcol, e_all, zacc, zs, rz, dut, dur, dvs, dvp, dvc, dvr, relay, v_t,
           q_pre, q_hid, q_inv, q_unit, v_pre, v_hid, v_inv, v_unit,
           gq, gv, pq, pv,
           h0, h1, h2, h3, r0, r1, r2, r3, o0, o1, o2, o3, x0, x1, x2, x3, f0, f1, f2, f3,
           ins, us, ur, vs, vr, ls, lr, lows_s, lows_r, zss, zsr, dus, durs, dvps, dvpr, dvss, dvsr, relay_r,
           ps, pr, rss, rsr):
    me = lax.axis_index("dp")
    core = me % 2
    x = (me // 2) % 4
    y = (me // 8) % 4
    z = me // 32
    lo = ((z + 1) // 2) % 2
    hi = z // 2
    scale = 1.0 / (TEMP * total_rows)
    other = (core + 1) % 2
    mate = z * 32 + y * 8 + x * 2 + other

    def a_dev(s):
        zz = z + (s % 2) * (1 - 2 * (z % 2))
        return zz * 32 + ((y + STEP[s // 2]) % 4) * 8 + x * 2 + core

    def c_dev(t, flip=0):
        dx, dh = PEER_C[t]
        return (z + dh * (3 - 2 * z)) * 32 + y * 8 + ((x + dx) % 4) * 2 + (core + flip) % 2

    def copy(src, dst, ssem, rsem, dev):
        return pltpu.make_async_remote_copy(src_ref=src, dst_ref=dst, send_sem=ssem, recv_sem=rsem,
                                            device_id=(dev,), device_id_type=pl.DeviceIdType.MESH)

    def send(src, dst, ssem, rsem, dev):
        copy(src, dst, ssem, rsem, dev).start()

    def arrived(dst, rsem):
        copy(dst, dst, rsem, rsem, me).wait_recv()

    def gone(src, ssem):
        copy(src, src, ssem, ssem, me).wait_send()

    barrier = pltpu.get_barrier_semaphore()
    partners = [a_dev(s) for s in range(1, NA)] + [c_dev(t // 2, t % 2) for t in range(1, NB)]
    for dev in partners:
        pl.semaphore_signal(barrier, inc=1, device_id=(dev,), device_id_type=pl.DeviceIdType.MESH)

    loads = [pltpu.make_async_copy(a, b, ins.at[i]) for i, (a, b) in enumerate((
        (vx_h, vx), (wvi_h, wvi), (wvo_h, wvo), (qx_h, qx), (wqi_h, wqi), (wqo_h, wqo), (lq_h, lq)))]
    for c in loads:
        c.start()
    for c in loads[:3]:
        c.wait()
    forward(vx, wvi, wvo, v_pre, v_hid, v_inv, v_unit)
    v_all[0] = v_unit[...].astype(BF16)
    for c in loads[3:]:
        c.wait()
    forward(qx, wqi, wqo, q_pre, q_hid, q_inv, q_unit)
    ub = q_unit[...].astype(BF16)
    u_all[0, 0] = ub[0:128]
    u_all[1, 0] = ub[128:256]
    pl.semaphore_wait(barrier, len(partners))
    for t in (15, 14, 13, 12, 11, 10, 5, 4, 9, 8, 7, 6, 3, 2, 1):
        send(lq, lq_all.at[INV_B[t]], ls, lr, c_dev(t // 2, t % 2))
    send(v_all.at[0], v_all.at[1], vs, vr.at[V_SEM[1]], mate)
    for s, t in zip(FAR, FAR_C):
        k = 2 * INV_C[t]
        send(u_all.at[0, 0], u_all.at[0, INV_A[s]], us.at[0], ur.at[0], a_dev(s))
        send(v_all.at[0], v_all.at[k], vs, vr.at[V_SEM[k]], c_dev(t))
    for t in FAR:
        k = INV_A[t]
        send(u_all.at[1, 0], u_all.at[1, k], us.at[1], ur.at[1], a_dev(t))
    lq_all[0] = lq[...]
    zacc[...] = jnp.zeros_like(zacc)

    low = lq[...]
    arrived(lq_all.at[1:NB], lr)
    for t in range(1, NB):
        low = jnp.minimum(low, lq_all[t])
    low = jnp.min(low, axis=1, keepdims=True)
    lows[0] = jnp.broadcast_to(low, (1, 128))

    table = jnp.concatenate([lq_all[t] for t in range(NB)], axis=0)
    table = jnp.transpose(LOG2E * ((table - low) + BOUND))
    for t in range(NB):
        kcol[t] = jnp.broadcast_to(table[:, t:t + 1], (256, 128))
    for s in FAR:
        send(lows.at[0], lows.at[INV_A[s]], lows_s, lows_r, a_dev(s))
    arrived(u_all.at[0, 1:NA], ur.at[0])

    c2 = LOG2E / TEMP

    def logits(t, h):
        vt = v_all[t]
        kc = kcol[t]
        kc = jnp.concatenate([kc, kc], axis=1)
        for m in range(4):
            um = u_all[h, 2 * m:2 * m + 2].reshape(256, 128)
            e = jnp.exp2(nt(vt, um) * c2 - kc)
            e_all[t, h, m] = e
            zacc[h, m] += jnp.sum(e.reshape(32, 8, 256), axis=0)

    def share(h):
        rows = []
        for m in range(4):
            row = jnp.sum(zacc[h, m], axis=0, keepdims=True)
            rows += [row[:, 0:128], row[:, 128:256]]
        zs[h, 0] = jnp.concatenate(rows, axis=0)

    def share_send(h):
        for s in FAR:
            send(zs.at[h, 0], zs.at[h, INV_A[s]], zss.at[h], zsr.at[h], a_dev(s))

    arrived(v_all.at[1], vr.at[V_SEM[1]])
    logits(0, 0)
    logits(1, 0)
    for i, group in enumerate(GROUPS[1:4]):
        arrived(v_all.at[0:len(group)], vr.at[i + 1])
        for t in group:
            copy(v_all.at[t], v_all.at[t + 1], vs, vr.at[V_SEM[t + 1]], mate).start()
        for t in group:
            logits(t, 0)
    for i, group in enumerate(GROUPS[4:7]):
        arrived(v_all.at[0:len(group)], vr.at[i + 4])
        for t in group:
            logits(t, 0)
    share(0)
    arrived(u_all.at[1, 1:NA], ur.at[1])
    share_send(0)

    def second(n, c):
        for i in range(8):
            logits(8 * n + i, 1)
        return c

    lax.fori_loop(0, NB // 8, second, 0)
    share(1)

    ji = lax.broadcasted_iota(jnp.int32, (256, 256), 0)
    qi = lax.broadcasted_iota(jnp.int32, (256, 256), 1)
    own = q_unit[...].astype(BF16).astype(F32) * v_unit[...].astype(BF16).astype(F32)
    pos = jnp.sum(own) / TEMP
    share_send(1)

    def combine(h):
        arrived(zs.at[h, 1:NA], zsr.at[h])
        tot = []
        for r in range(NA):
            acc = None
            for s in range(NA):
                k = rel_a(r, s)
                term = fac[s] * zs[h, s, k:k + 1, :]
                acc = term if acc is None else acc + term
            tot.append(acc)
        inv = [fac[0] / w for w in tot]
        for m in range(4):
            rz[h, m] = jnp.concatenate([inv[2 * m], inv[2 * m + 1]], axis=1)
        return jnp.log(tot[0])

    def grads(t, h, diag, even=False):
        vt = v_t[t]
        dv = None
        for m in range(4):
            p = e_all[t, h, m] * rz[h, m]
            if diag and m == 0:
                p = jnp.where((ji == qi + h * 128) & (qi < 128), p - 1.0, p)
            g = p.astype(BF16)
            d = nn(g, u_all[h, 2 * m:2 * m + 2].reshape(256, 128))
            dv = d if dv is None else dv + d
            du = nn(vt, g)
            if diag:
                dut[h, 2 * m] = du[:, 0:128]
                dut[h, 2 * m + 1] = du[:, 128:256]
            else:
                dut[h, 2 * m] += du[:, 0:128]
                dut[h, 2 * m + 1] += du[:, 128:256]
        if h == 0:
            dvs[t] = dv
        elif even:
            dvc[t // 2] = dvs[t] + dv + dvp[t // 2]
        else:
            dvs[t] += dv

    for t in range(NB):
        v_t[t] = jnp.transpose(v_all[t])
    arrived(lows.at[1:NA], lows_r)
    lowv = [lows[s] for s in range(NA)]
    least = functools.reduce(jnp.minimum, lowv)
    fac = [jnp.exp(least - w) for w in lowv]
    log0 = combine(0)
    grads(0, 0, True)

    def third(n, c):
        for i in range(1, 6):
            grads(5 * n + i, 0, False)
        return c

    lax.fori_loop(0, 3, third, 0)
    log1 = combine(1)
    for s in FAR:
        send(dut.at[0, s], dur.at[0, INV_A[s]], dus.at[0], durs.at[0], a_dev(s))

    def mate_copy(t):
        return copy(dvs.at[2 * t + 1], dvp.at[t], dvps, dvpr.at[t], mate)

    def dv_send(t):
        if t > 5:
            send(dvc.at[t], relay.at[7 - t], dvss, relay_r.at[7 - t], c_dev(1 if t == 7 else 4))
        else:
            send(dvc.at[t], dvr.at[t], dvss, dvsr, c_dev(t))

    grads(0, 1, True)

    def odd(n, c):
        t = 7 - 2 * n

        @pl.when(n > 0)
        def _():
            mate_copy(t + 1).start()

        grads(2 * t + 1, 1, False)
        grads(2 * t - 1, 1, False)
        mate_copy(t).start()
        return c

    lax.fori_loop(0, 4, odd, 0)

    mate_copy(0).start()
    for t in (7, 5, 3):
        arrived(dvp.at[t], dvpr.at[t])
        arrived(dvp.at[t - 1], dvpr.at[t - 1])
        if t < 7:
            dv_send(t + 1)
        grads(2 * t, 1, False, True)
        grads(2 * t - 2, 1, False, True)
        dv_send(t)
    arrived(dvp.at[1], dvpr.at[1])
    grads(2, 1, False, True)
    for s in FAR:
        send(dut.at[1, s], dur.at[1, INV_A[s]], dus.at[1], durs.at[1], a_dev(s))
    loss_rows = ((lq[:, 0:128] - least) + BOUND + log0) + ((lq[:, 128:256] - least) + BOUND + log1)
    loss_loc = jnp.sum(loss_rows, axis=1, keepdims=True) - pos
    arrived(relay.at[0], relay_r.at[0])
    dvc[2] += relay[0]
    arrived(dvp.at[0], dvpr.at[0])
    dvc[0] = dvs[0] + dvp[0]
    dv_send(2)
    arrived(relay.at[1], relay_r.at[1])
    dvc[1] += relay[1]

    def sum_du(h):
        arrived(dur.at[h, 1:NA], durs.at[h])
        du = dut[h, 0]
        for s in range(1, NA):
            du = du + dur[h, s]
        return jnp.transpose(du)

    parts = [sum_du(0)]
    dv_send(1)
    parts.append(sum_du(1))
    d_unit = jnp.concatenate(parts, axis=0) * scale
    g_in, g_out = backward(qx, wqo, q_pre, q_hid, q_inv, q_unit, d_unit)

    def pack(buf, g_in, g_out):
        buf[0, 0:512, :] = g_in[:, 0:128]
        buf[0, 512:640, :] = g_in[0:128, 128:256]
        buf[1, 0:384, :] = g_in[128:512, 128:256]
        buf[1, 384:640, :] = g_out

    pack(gq, g_in, g_out)
    lt = jnp.broadcast_to(loss_loc, (8, 128))
    gq[0, 640:648, :] = lt
    gq[1, 640:648, :] = lt
    send(gq.at[other], pq, ps.at[0], pr.at[0], mate)

    a_me, b_me = y * 2 + lo, x * 2 + hi

    def a_idx(s):
        return ((y + STEP[s // 2]) % 4) * 2 + (lo + s % 2) % 2

    def c_idx(t):
        return ((x + PEER_C[t][0]) % 4) * 2 + (hi + PEER_C[t][1]) % 2

    side_a, side_c = (a_dev, a_idx, a_me, FAR, INV_A), (c_dev, c_idx, b_me, FAR_C, INV_C)
    paths = (
        (0, h0, r0, o0, x0, f0, side_c, side_a),
        (1, h1, r1, o1, x1, f1, side_a, side_c),
        (2, h2, r2, o2, x2, f2, side_a, side_c),
        (3, h3, r3, o3, x3, f3, side_c, side_a),
    )

    def pair(w, g, p):
        arrived(p, pr.at[w])
        for i, h, r, o, xx, f, (dev, idx, mine, far, inv), _ in paths[2 * w:2 * w + 2]:
            base = 320 * (i % 2)
            h[:, 0:40, :] = (g[core, base:base + 320, :] + p[base:base + 320, :]).reshape(8, 40, 128)
            if i == 0:
                extra = g[core, 640:648, :] + p[640:648, :]
                for n in range(8):
                    h[n, 40:48, :] = extra
        for i, h, r, o, xx, f, (dev, idx, mine, far, inv), _ in paths[2 * w:2 * w + 2]:
            for s in far:
                send(h.at[idx(s)], r.at[inv[s]], rss.at[0, i], rsr.at[0, i], dev(s))

    def scatter(w):
        for i, h, r, o, xx, f, (_, _, mine, _, _), (dev, _, _, far, inv) in paths[2 * w:2 * w + 2]:
            arrived(r.at[1:8], rsr.at[0, i])
            acc = h[mine]
            for s in range(1, 8):
                acc = acc + r[s]
            o[...] = acc
            for s in far:
                send(o, xx.at[inv[s]], rss.at[1, i], rsr.at[1, i], dev(s))

    def exchange(w):
        for i, h, r, o, xx, f, (dev, idx, mine, far, inv), _ in paths[2 * w:2 * w + 2]:
            arrived(xx.at[1:8], rsr.at[1, i])
            acc = o[...]
            for s in range(1, 8):
                acc = acc + xx[s]
            f[core, mine] = acc
            for s in far:
                send(f.at[core, mine], f.at[core, mine], rss.at[2, i], rsr.at[2, i], dev(s))
            if i == 0:
                loss_o[...] = acc[40:48] * (1.0 / total_rows)

    def gather(w):
        for i, h, r, o, xx, f, _, _ in paths[2 * w:2 * w + 2]:
            arrived(r.at[1:8], rsr.at[2, i])
            send(f.at[core], f.at[core], rss.at[3, i], rsr.at[3, i], mate)

    def finish(w, go_in, go_out):
        halves = [[], []]
        for i, h, r, o, xx, f, _, _ in paths[2 * w:2 * w + 2]:
            arrived(h, rsr.at[3, i])
            for c in range(2):
                halves[c].append(f[c, :, 0:40, :].reshape(320, 128))
        head, tail = [jnp.concatenate(c, axis=0) for c in halves]
        go_in[:, 0:128] = head[0:512]
        go_in[0:128, 128:256] = head[512:640]
        go_in[128:512, 128:256] = tail[0:384]
        go_out[...] = tail[384:640]

    pair(0, gq, pq)
    arrived(dvr.at[1:6], dvsr)
    dv = lax.fori_loop(1, 6, lambda t, acc: acc + dvr[t], dvc[0])
    g_in, g_out = backward(vx, wvo, v_pre, v_hid, v_inv, v_unit, dv * scale)
    pack(gv, g_in, g_out)
    send(gv.at[other], pv, ps.at[1], pr.at[1], mate)
    pair(1, gv, pv)
    scatter(0)
    scatter(1)
    exchange(0)
    exchange(1)
    gather(0)
    gather(1)
    finish(0, gqi_o, gqo_o)
    finish(1, gvi_o, gvo_o)
    gone(lq_all.at[1:NB], ls)
    gone(lows.at[1:NA], lows_s)
    gone(v_all.at[1:NB], vs)
    for h in range(2):
        gone(u_all.at[h, 1:NA], us.at[h])
        gone(zs.at[h, 1:NA], zss.at[h])
        gone(dur.at[h, 1:NA], dus.at[h])
    gone(dvp, dvps)
    gone(dvr.at[1:NC], dvss)
    gone(pq, ps.at[0])
    gone(pv, ps.at[1])
    for i, h, r, o, xx, f, _, _ in paths:
        gone(r.at[1:8], rss.at[0, i])
        gone(xx.at[1:8], rss.at[1, i])
        gone(r.at[1:8], rss.at[2, i])
        gone(h, rss.at[3, i])


def emit(loss, gqi, gqo, gvi, gvo, loss_o, gqi_o, gqo_o, gvi_o, gvo_o, value, sem):
    pairs = ((value, loss_o), (gqi, gqi_o), (gvi, gvi_o), (gqo, gqo_o), (gvo, gvo_o))
    copies = [pltpu.make_async_copy(a, b, sem.at[i]) for i, (a, b) in enumerate(pairs)]
    for c in copies[1:]:
        c.start()
    value[0] = loss[0, 0]
    copies[0].start()
    for c in copies:
        c.wait()


def solution(mesh):
    group = mesh.shape["dp"]

    def local_step(query_feat, item_feat, log_q, w_query_in, w_query_out, w_item_in, w_item_out):
        local_rows = query_feat.shape[0]
        vm = lambda *s: pltpu.VMEM(s, F32)
        vb = lambda *s: pltpu.VMEM(s, BF16)
        sem = lambda *s: pltpu.SemaphoreType.DMA(s)
        one = pltpu.SemaphoreType.DMA
        scratch = [
            vb(256, 512), vb(256, 512), vm(1, 256), vb(512, 256), vb(256, 128), vb(512, 256), vb(256, 128),
            vb(2, NA, 128, 128), vb(NB, 256, 128), vm(NB, 1, 256), vm(NA, 1, 128), vm(NB, 256, 128),
            vm(NB, 2, 4, 256, 256), vm(2, 4, 8, 256), vm(2, NA, 8, 128), vm(2, 4, 1, 256),
            vm(2, NA, 128, 128), vm(2, NA, 128, 128),
            vm(NB, 256, 128), vm(NC, 256, 128), vm(NC, 256, 128), vm(NC, 256, 128), vm(2, 256, 128), vb(NB, 128, 256),
            vm(256, 256), vb(256, 256), vm(256, 128), vm(256, 128),
            vm(256, 256), vb(256, 256), vm(256, 128), vm(256, 128),
            vm(2, 648, 128), vm(2, 640, 128), vm(648, 128), vm(640, 128),
            vm(8, 48, 128), vm(8, 40, 128), vm(8, 40, 128), vm(8, 40, 128),
            vm(8, 48, 128), vm(8, 40, 128), vm(8, 40, 128), vm(8, 40, 128),
            vm(48, 128), vm(40, 128), vm(40, 128), vm(40, 128),
            vm(8, 48, 128), vm(8, 40, 128), vm(8, 40, 128), vm(8, 40, 128),
            vm(2, 8, 48, 128), vm(2, 8, 40, 128), vm(2, 8, 40, 128), vm(2, 8, 40, 128),
            sem(7), sem(2), sem(2), one, sem(8), one, one, one, one, sem(2), sem(2),
            sem(2), sem(2), one, sem(NC), one, one, sem(2),
            sem(2), sem(2), sem(4, 4), sem(4, 4),
        ]
        vspec = pl.BlockSpec(memory_space=pltpu.VMEM)
        shapes = ((512, 256), (256, 128), (512, 256), (256, 128))
        hbm = pl.BlockSpec(memory_space=pltpu.HBM)
        staged = pl.pallas_call(
            functools.partial(kernel, local_rows * group),
            out_shape=tuple(pltpu.VMEM(s, F32) for s in ((8, 128), *shapes)),
            in_specs=[hbm] * 7,
            out_specs=(vspec,) * 5,
            scratch_shapes=scratch,
            compiler_params=pltpu.CompilerParams(collective_id=0, has_side_effects=True,
                                                 vmem_limit_bytes=56 * 1024 * 1024),
        )(query_feat, item_feat, log_q.reshape(1, local_rows), w_query_in, w_query_out, w_item_in, w_item_out)
        return pl.pallas_call(
            emit,
            out_shape=tuple(jax.ShapeDtypeStruct(s, F32) for s in ((1,), *shapes)),
            in_specs=[vspec] * 5,
            out_specs=(hbm,) * 5,
            scratch_shapes=[pltpu.SMEM((1,), F32), sem(5)],
            compiler_params=pltpu.CompilerParams(vmem_limit_bytes=1024 * 1024),
        )(*staged)

    return jax.shard_map(local_step, mesh=mesh,
                         in_specs=(P("dp", None), P("dp", None), P("dp"), P(), P(), P(), P()),
                         out_specs=(P(), P(), P(), P(), P()), check_vma=False)
```

```python
import functools

import jax
import jax.numpy as jnp
from jax import lax
from jax.experimental import pallas as pl
from jax.experimental.pallas import tpu as pltpu
from jax.sharding import PartitionSpec as P

TEMP = 0.05
NORM_EPS = 1e-6
LOG2E = 1.4426950408889634
BOUND = 20.25
F32 = jnp.float32
BF16 = jnp.bfloat16
NA, NB, NC = 8, 16, 8
STEP = (0, 1, 3, 2)
BACK = (0, 2, 1, 3)
FAR = (7, 6, 3, 5, 2, 4, 1)
PEER_C = ((0, 0), (0, 1), (2, 0), (3, 1), (1, 0), (3, 0), (1, 1), (2, 1))
FAR_C = (7, 6, 3, 2, 5, 4, 1)
GROUPS = ((0,), (12, 2), (8, 14), (6, 4, 10), (13, 3, 9), (15, 7, 5), (11,), (1,))
V_SEM = {s: i for i, g in enumerate(GROUPS) for s in g}
INV_C = (0, 1, 2, 6, 5, 4, 3, 7)
INV_A = [2 * BACK[s // 2] + s % 2 for s in range(NA)]
INV_B = [2 * INV_C[t // 2] + t % 2 for t in range(NB)]


def rel_a(r, s):
    dy = (STEP[r // 2] - STEP[s // 2]) % 4
    return 2 * STEP.index(dy) + (r % 2 + s % 2) % 2


def nt(a, b):
    return lax.dot_general(a, b, (((1,), (1,)), ((), ())), preferred_element_type=F32)


def tn(a, b):
    return lax.dot_general(a, b, (((0,), (0,)), ((), ())), preferred_element_type=F32)


def nn(a, b):
    return jnp.dot(a, b, preferred_element_type=F32)


def forward(x, w_in, w_out, pre_s, hid_s, inv_s, unit_s):
    pre = nn(x[...], w_in[...])
    hid = jnp.maximum(pre, 0.0).astype(BF16)
    emb = nn(hid, w_out[...])
    inv = lax.rsqrt(jnp.sum(emb * emb, axis=-1, keepdims=True) + NORM_EPS)
    unit = emb * inv
    pre_s[...] = pre
    hid_s[...] = hid
    inv_s[...] = jnp.broadcast_to(inv, unit.shape)
    unit_s[...] = unit


def backward(x, w_out, pre_s, hid_s, inv_s, unit_s, d_unit):
    unit = unit_s[...]
    d_emb = inv_s[...] * (d_unit - unit * jnp.sum(unit * d_unit, axis=-1, keepdims=True))
    d_emb = d_emb.astype(BF16)
    g_out = tn(hid_s[...], d_emb)
    d_hid = nt(d_emb, w_out[...])
    d_pre = jnp.where(pre_s[...] > 0, d_hid, 0.0).astype(BF16)
    g_in = tn(x[...], d_pre)
    return g_in, g_out


def kernel(total_rows, qx_h, vx_h, lq_h, wqi_h, wqo_h, wvi_h, wvo_h,
           loss_o, gqi_o, gqo_o, gvi_o, gvo_o,
           qx, vx, lq, wqi, wqo, wvi, wvo,
           u_all, v_all, lq_all, lows, kcol, e_all, zacc, zs, rz, dut, dur, dvs, dvp, dvc, dvr, relay, v_t,
           q_pre, q_hid, q_inv, q_unit, v_pre, v_hid, v_inv, v_unit,
           gq, gv, pq, pv,
           h0, h1, h2, h3, r0, r1, r2, r3, o0, o1, o2, o3, x0, x1, x2, x3, f0, f1, f2, f3,
           ins, us, ur, vs, vr, ls, lr, lows_s, lows_r, zss, zsr, dus, durs, dvps, dvpr, dvss, dvsr, relay_r,
           ps, pr, rss, rsr):
    me = lax.axis_index("dp")
    core = me % 2
    x = (me // 2) % 4
    y = (me // 8) % 4
    z = me // 32
    lo = ((z + 1) // 2) % 2
    hi = z // 2
    scale = 1.0 / (TEMP * total_rows)
    other = (core + 1) % 2
    mate = z * 32 + y * 8 + x * 2 + other

    def a_dev(s):
        zz = z + (s % 2) * (1 - 2 * (z % 2))
        return zz * 32 + ((y + STEP[s // 2]) % 4) * 8 + x * 2 + core

    def c_dev(t, flip=0):
        dx, dh = PEER_C[t]
        return (z + dh * (3 - 2 * z)) * 32 + y * 8 + ((x + dx) % 4) * 2 + (core + flip) % 2

    def copy(src, dst, ssem, rsem, dev):
        return pltpu.make_async_remote_copy(src_ref=src, dst_ref=dst, send_sem=ssem, recv_sem=rsem,
                                            device_id=(dev,), device_id_type=pl.DeviceIdType.MESH)

    def send(src, dst, ssem, rsem, dev):
        copy(src, dst, ssem, rsem, dev).start()

    def arrived(dst, rsem):
        copy(dst, dst, rsem, rsem, me).wait_recv()

    def gone(src, ssem):
        copy(src, src, ssem, ssem, me).wait_send()

    barrier = pltpu.get_barrier_semaphore()
    partners = [a_dev(s) for s in range(1, NA)] + [c_dev(t // 2, t % 2) for t in range(1, NB)]
    for dev in partners:
        pl.semaphore_signal(barrier, inc=1, device_id=(dev,), device_id_type=pl.DeviceIdType.MESH)

    loads = [pltpu.make_async_copy(a, b, ins.at[i]) for i, (a, b) in enumerate((
        (vx_h, vx), (wvi_h, wvi), (wvo_h, wvo), (qx_h, qx), (wqi_h, wqi), (wqo_h, wqo), (lq_h, lq)))]
    for c in loads:
        c.start()
    for c in loads[:3]:
        c.wait()
    forward(vx, wvi, wvo, v_pre, v_hid, v_inv, v_unit)
    v_all[0] = v_unit[...].astype(BF16)
    for c in loads[3:]:
        c.wait()
    forward(qx, wqi, wqo, q_pre, q_hid, q_inv, q_unit)
    ub = q_unit[...].astype(BF16)
    u_all[0, 0] = ub[0:128]
    u_all[1, 0] = ub[128:256]
    pl.semaphore_wait(barrier, len(partners))
    for t in (15, 14, 13, 12, 11, 10, 5, 4, 9, 8, 7, 6, 3, 2, 1):
        send(lq, lq_all.at[INV_B[t]], ls, lr, c_dev(t // 2, t % 2))
    for s in FAR:
        send(u_all.at[0, 0], u_all.at[0, INV_A[s]], us.at[0], ur.at[0], a_dev(s))
    send(v_all.at[0], v_all.at[1], vs, vr.at[V_SEM[1]], mate)
    for t in FAR_C:
        k = 2 * INV_C[t]
        send(v_all.at[0], v_all.at[k], vs, vr.at[V_SEM[k]], c_dev(t))
    for t in FAR:
        k = INV_A[t]
        send(u_all.at[1, 0], u_all.at[1, k], us.at[1], ur.at[1], a_dev(t))
    lq_all[0] = lq[...]
    zacc[...] = jnp.zeros_like(zacc)

    low = lq[...]
    arrived(lq_all.at[1:NB], lr)
    for t in range(1, NB):
        low = jnp.minimum(low, lq_all[t])
    low = jnp.min(low, axis=1, keepdims=True)
    lows[0] = jnp.broadcast_to(low, (1, 128))

    table = jnp.concatenate([lq_all[t] for t in range(NB)], axis=0)
    table = jnp.transpose(LOG2E * ((table - low) + BOUND))
    for t in range(NB):
        kcol[t] = jnp.broadcast_to(table[:, t:t + 1], (256, 128))
    for s in FAR:
        send(lows.at[0], lows.at[INV_A[s]], lows_s, lows_r, a_dev(s))
    arrived(u_all.at[0, 1:NA], ur.at[0])

    c2 = LOG2E / TEMP

    def logits(t, h):
        vt = v_all[t]
        kc = kcol[t]
        kc = jnp.concatenate([kc, kc], axis=1)
        for m in range(4):
            um = u_all[h, 2 * m:2 * m + 2].reshape(256, 128)
            e = jnp.exp2(nt(vt, um) * c2 - kc)
            e_all[t, h, m] = e
            zacc[h, m] += jnp.sum(e.reshape(32, 8, 256), axis=0)

    def share(h):
        rows = []
        for m in range(4):
            row = jnp.sum(zacc[h, m], axis=0, keepdims=True)
            rows += [row[:, 0:128], row[:, 128:256]]
        zs[h, 0] = jnp.concatenate(rows, axis=0)

    def share_send(h):
        for s in FAR:
            send(zs.at[h, 0], zs.at[h, INV_A[s]], zss.at[h], zsr.at[h], a_dev(s))

    arrived(v_all.at[1], vr.at[V_SEM[1]])
    logits(0, 0)
    logits(1, 0)
    for i, group in enumerate(GROUPS[1:4]):
        arrived(v_all.at[0:len(group)], vr.at[i + 1])
        for t in group:
            copy(v_all.at[t], v_all.at[t + 1], vs, vr.at[V_SEM[t + 1]], mate).start()
        for t in group:
            logits(t, 0)
    for i, group in enumerate(GROUPS[4:7]):
        arrived(v_all.at[0:len(group)], vr.at[i + 4])
        for t in group:
            logits(t, 0)
    share(0)
    arrived(u_all.at[1, 1:NA], ur.at[1])
    share_send(0)

    def second(n, c):
        for i in range(8):
            logits(8 * n + i, 1)
        return c

    lax.fori_loop(0, NB // 8, second, 0)
    share(1)

    ji = lax.broadcasted_iota(jnp.int32, (256, 256), 0)
    qi = lax.broadcasted_iota(jnp.int32, (256, 256), 1)
    own = q_unit[...].astype(BF16).astype(F32) * v_unit[...].astype(BF16).astype(F32)
    pos = jnp.sum(own) / TEMP
    share_send(1)

    def combine(h):
        arrived(zs.at[h, 1:NA], zsr.at[h])
        tot = []
        for r in range(NA):
            acc = None
            for s in range(NA):
                k = rel_a(r, s)
                term = fac[s] * zs[h, s, k:k + 1, :]
                acc = term if acc is None else acc + term
            tot.append(acc)
        inv = [fac[0] / w for w in tot]
        for m in range(4):
            rz[h, m] = jnp.concatenate([inv[2 * m], inv[2 * m + 1]], axis=1)
        return jnp.log(tot[0])

    def grads(t, h, diag, even=False):
        vt = v_t[t]
        dv = None
        for m in range(4):
            p = e_all[t, h, m] * rz[h, m]
            if diag and m == 0:
                p = jnp.where((ji == qi + h * 128) & (qi < 128), p - 1.0, p)
            g = p.astype(BF16)
            d = nn(g, u_all[h, 2 * m:2 * m + 2].reshape(256, 128))
            dv = d if dv is None else dv + d
            du = nn(vt, g)
            if diag:
                dut[h, 2 * m] = du[:, 0:128]
                dut[h, 2 * m + 1] = du[:, 128:256]
            else:
                dut[h, 2 * m] += du[:, 0:128]
                dut[h, 2 * m + 1] += du[:, 128:256]
        if h == 0:
            dvs[t] = dv
        elif even:
            dvc[t // 2] = dvs[t] + dv + dvp[t // 2]
        else:
            dvs[t] += dv

    for t in range(NB):
        v_t[t] = jnp.transpose(v_all[t])
    arrived(lows.at[1:NA], lows_r)
    lowv = [lows[s] for s in range(NA)]
    least = functools.reduce(jnp.minimum, lowv)
    fac = [jnp.exp(least - w) for w in lowv]
    log0 = combine(0)
    grads(0, 0, True)

    def third(n, c):
        for i in range(1, 6):
            grads(5 * n + i, 0, False)
        return c

    lax.fori_loop(0, 3, third, 0)
    log1 = combine(1)
    for s in FAR:
        send(dut.at[0, s], dur.at[0, INV_A[s]], dus.at[0], durs.at[0], a_dev(s))

    def mate_copy(t):
        return copy(dvs.at[2 * t + 1], dvp.at[t], dvps, dvpr.at[t], mate)

    def dv_send(t):
        if t > 5:
            send(dvc.at[t], relay.at[7 - t], dvss, relay_r.at[7 - t], c_dev(1 if t == 7 else 4))
        else:
            send(dvc.at[t], dvr.at[t], dvss, dvsr, c_dev(t))

    grads(0, 1, True)

    def odd(n, c):
        t = 7 - 2 * n

        @pl.when(n > 0)
        def _():
            mate_copy(t + 1).start()

        grads(2 * t + 1, 1, False)
        grads(2 * t - 1, 1, False)
        mate_copy(t).start()
        return c

    lax.fori_loop(0, 4, odd, 0)

    mate_copy(0).start()
    for t in (7, 5, 3):
        arrived(dvp.at[t], dvpr.at[t])
        arrived(dvp.at[t - 1], dvpr.at[t - 1])
        if t < 7:
            dv_send(t + 1)
        grads(2 * t, 1, False, True)
        grads(2 * t - 2, 1, False, True)
        dv_send(t)
    arrived(dvp.at[1], dvpr.at[1])
    grads(2, 1, False, True)
    for s in FAR:
        send(dut.at[1, s], dur.at[1, INV_A[s]], dus.at[1], durs.at[1], a_dev(s))
    loss_rows = ((lq[:, 0:128] - least) + BOUND + log0) + ((lq[:, 128:256] - least) + BOUND + log1)
    loss_loc = jnp.sum(loss_rows, axis=1, keepdims=True) - pos
    arrived(relay.at[0], relay_r.at[0])
    dvc[2] += relay[0]
    arrived(dvp.at[0], dvpr.at[0])
    dvc[0] = dvs[0] + dvp[0]
    dv_send(2)
    arrived(relay.at[1], relay_r.at[1])
    dvc[1] += relay[1]

    def sum_du(h):
        arrived(dur.at[h, 1:NA], durs.at[h])
        du = dut[h, 0]
        for s in range(1, NA):
            du = du + dur[h, s]
        return jnp.transpose(du)

    parts = [sum_du(0)]
    dv_send(1)
    parts.append(sum_du(1))
    d_unit = jnp.concatenate(parts, axis=0) * scale
    g_in, g_out = backward(qx, wqo, q_pre, q_hid, q_inv, q_unit, d_unit)

    def pack(buf, g_in, g_out):
        buf[0, 0:512, :] = g_in[:, 0:128]
        buf[0, 512:640, :] = g_in[0:128, 128:256]
        buf[1, 0:384, :] = g_in[128:512, 128:256]
        buf[1, 384:640, :] = g_out

    pack(gq, g_in, g_out)
    lt = jnp.broadcast_to(loss_loc, (8, 128))
    gq[0, 640:648, :] = lt
    gq[1, 640:648, :] = lt
    send(gq.at[other], pq, ps.at[0], pr.at[0], mate)

    a_me, b_me = y * 2 + lo, x * 2 + hi

    def a_idx(s):
        return ((y + STEP[s // 2]) % 4) * 2 + (lo + s % 2) % 2

    def c_idx(t):
        return ((x + PEER_C[t][0]) % 4) * 2 + (hi + PEER_C[t][1]) % 2

    side_a, side_c = (a_dev, a_idx, a_me, FAR, INV_A), (c_dev, c_idx, b_me, FAR_C, INV_C)
    paths = (
        (0, h0, r0, o0, x0, f0, side_c, side_a),
        (1, h1, r1, o1, x1, f1, side_a, side_c),
        (2, h2, r2, o2, x2, f2, side_a, side_c),
        (3, h3, r3, o3, x3, f3, side_c, side_a),
    )

    def pair(w, g, p):
        arrived(p, pr.at[w])
        for i, h, r, o, xx, f, (dev, idx, mine, far, inv), _ in paths[2 * w:2 * w + 2]:
            base = 320 * (i % 2)
            h[:, 0:40, :] = (g[core, base:base + 320, :] + p[base:base + 320, :]).reshape(8, 40, 128)
            if i == 0:
                extra = g[core, 640:648, :] + p[640:648, :]
                for n in range(8):
                    h[n, 40:48, :] = extra
        for i, h, r, o, xx, f, (dev, idx, mine, far, inv), _ in paths[2 * w:2 * w + 2]:
            for s in far:
                send(h.at[idx(s)], r.at[inv[s]], rss.at[0, i], rsr.at[0, i], dev(s))

    def scatter(w):
        for i, h, r, o, xx, f, (_, _, mine, _, _), (dev, _, _, far, inv) in paths[2 * w:2 * w + 2]:
            arrived(r.at[1:8], rsr.at[0, i])
            acc = h[mine]
            for s in range(1, 8):
                acc = acc + r[s]
            o[...] = acc
            for s in far:
                send(o, xx.at[inv[s]], rss.at[1, i], rsr.at[1, i], dev(s))

    def exchange(w):
        for i, h, r, o, xx, f, (dev, idx, mine, far, inv), _ in paths[2 * w:2 * w + 2]:
            arrived(xx.at[1:8], rsr.at[1, i])
            acc = o[...]
            for s in range(1, 8):
                acc = acc + xx[s]
            f[core, mine] = acc
            for s in far:
                send(f.at[core, mine], f.at[core, mine], rss.at[2, i], rsr.at[2, i], dev(s))
            if i == 0:
                loss_o[...] = acc[40:48] * (1.0 / total_rows)

    def gather(w):
        for i, h, r, o, xx, f, _, _ in paths[2 * w:2 * w + 2]:
            arrived(r.at[1:8], rsr.at[2, i])
            send(f.at[core], f.at[core], rss.at[3, i], rsr.at[3, i], mate)

    def finish(w, go_in, go_out):
        halves = [[], []]
        for i, h, r, o, xx, f, _, _ in paths[2 * w:2 * w + 2]:
            arrived(h, rsr.at[3, i])
            for c in range(2):
                halves[c].append(f[c, :, 0:40, :].reshape(320, 128))
        head, tail = [jnp.concatenate(c, axis=0) for c in halves]
        go_in[:, 0:128] = head[0:512]
        go_in[0:128, 128:256] = head[512:640]
        go_in[128:512, 128:256] = tail[0:384]
        go_out[...] = tail[384:640]

    pair(0, gq, pq)
    arrived(dvr.at[1:6], dvsr)
    dv = lax.fori_loop(1, 6, lambda t, acc: acc + dvr[t], dvc[0])
    g_in, g_out = backward(vx, wvo, v_pre, v_hid, v_inv, v_unit, dv * scale)
    pack(gv, g_in, g_out)
    send(gv.at[other], pv, ps.at[1], pr.at[1], mate)
    pair(1, gv, pv)
    scatter(0)
    scatter(1)
    exchange(0)
    exchange(1)
    gather(0)
    gather(1)
    finish(0, gqi_o, gqo_o)
    finish(1, gvi_o, gvo_o)
    gone(lq_all.at[1:NB], ls)
    gone(lows.at[1:NA], lows_s)
    gone(v_all.at[1:NB], vs)
    for h in range(2):
        gone(u_all.at[h, 1:NA], us.at[h])
        gone(zs.at[h, 1:NA], zss.at[h])
        gone(dur.at[h, 1:NA], dus.at[h])
    gone(dvp, dvps)
    gone(dvr.at[1:NC], dvss)
    gone(pq, ps.at[0])
    gone(pv, ps.at[1])
    for i, h, r, o, xx, f, _, _ in paths:
        gone(r.at[1:8], rss.at[0, i])
        gone(xx.at[1:8], rss.at[1, i])
        gone(r.at[1:8], rss.at[2, i])
        gone(h, rss.at[3, i])


def emit(loss, gqi, gqo, gvi, gvo, loss_o, gqi_o, gqo_o, gvi_o, gvo_o, value, sem):
    pairs = ((value, loss_o), (gqi, gqi_o), (gvi, gvi_o), (gqo, gqo_o), (gvo, gvo_o))
    copies = [pltpu.make_async_copy(a, b, sem.at[i]) for i, (a, b) in enumerate(pairs)]
    for c in copies[1:]:
        c.start()
    value[0] = loss[0, 0]
    copies[0].start()
    for c in copies:
        c.wait()


def solution(mesh):
    group = mesh.shape["dp"]

    def local_step(query_feat, item_feat, log_q, w_query_in, w_query_out, w_item_in, w_item_out):
        local_rows = query_feat.shape[0]
        vm = lambda *s: pltpu.VMEM(s, F32)
        vb = lambda *s: pltpu.VMEM(s, BF16)
        sem = lambda *s: pltpu.SemaphoreType.DMA(s)
        one = pltpu.SemaphoreType.DMA
        scratch = [
            vb(256, 512), vb(256, 512), vm(1, 256), vb(512, 256), vb(256, 128), vb(512, 256), vb(256, 128),
            vb(2, NA, 128, 128), vb(NB, 256, 128), vm(NB, 1, 256), vm(NA, 1, 128), vm(NB, 256, 128),
            vm(NB, 2, 4, 256, 256), vm(2, 4, 8, 256), vm(2, NA, 8, 128), vm(2, 4, 1, 256),
            vm(2, NA, 128, 128), vm(2, NA, 128, 128),
            vm(NB, 256, 128), vm(NC, 256, 128), vm(NC, 256, 128), vm(NC, 256, 128), vm(2, 256, 128), vb(NB, 128, 256),
            vm(256, 256), vb(256, 256), vm(256, 128), vm(256, 128),
            vm(256, 256), vb(256, 256), vm(256, 128), vm(256, 128),
            vm(2, 648, 128), vm(2, 640, 128), vm(648, 128), vm(640, 128),
            vm(8, 48, 128), vm(8, 40, 128), vm(8, 40, 128), vm(8, 40, 128),
            vm(8, 48, 128), vm(8, 40, 128), vm(8, 40, 128), vm(8, 40, 128),
            vm(48, 128), vm(40, 128), vm(40, 128), vm(40, 128),
            vm(8, 48, 128), vm(8, 40, 128), vm(8, 40, 128), vm(8, 40, 128),
            vm(2, 8, 48, 128), vm(2, 8, 40, 128), vm(2, 8, 40, 128), vm(2, 8, 40, 128),
            sem(7), sem(2), sem(2), one, sem(8), one, one, one, one, sem(2), sem(2),
            sem(2), sem(2), one, sem(NC), one, one, sem(2),
            sem(2), sem(2), sem(4, 4), sem(4, 4),
        ]
        vspec = pl.BlockSpec(memory_space=pltpu.VMEM)
        shapes = ((512, 256), (256, 128), (512, 256), (256, 128))
        hbm = pl.BlockSpec(memory_space=pltpu.HBM)
        staged = pl.pallas_call(
            functools.partial(kernel, local_rows * group),
            out_shape=tuple(pltpu.VMEM(s, F32) for s in ((8, 128), *shapes)),
            in_specs=[hbm] * 7,
            out_specs=(vspec,) * 5,
            scratch_shapes=scratch,
            compiler_params=pltpu.CompilerParams(collective_id=0, has_side_effects=True,
                                                 vmem_limit_bytes=56 * 1024 * 1024),
        )(query_feat, item_feat, log_q.reshape(1, local_rows), w_query_in, w_query_out, w_item_in, w_item_out)
        return pl.pallas_call(
            emit,
            out_shape=tuple(jax.ShapeDtypeStruct(s, F32) for s in ((1,), *shapes)),
            in_specs=[vspec] * 5,
            out_specs=(hbm,) * 5,
            scratch_shapes=[pltpu.SMEM((1,), F32), sem(5)],
            compiler_params=pltpu.CompilerParams(vmem_limit_bytes=1024 * 1024),
        )(*staged)

    return jax.shard_map(local_step, mesh=mesh,
                         in_specs=(P("dp", None), P("dp", None), P("dp"), P(), P(), P(), P()),
                         out_specs=(P(), P(), P(), P(), P()), check_vma=False)
```

```python
import functools

import jax
import jax.numpy as jnp
from jax import lax
from jax.experimental import pallas as pl
from jax.experimental.pallas import tpu as pltpu
from jax.sharding import PartitionSpec as P

TEMP = 0.05
NORM_EPS = 1e-6
LOG2E = 1.4426950408889634
BOUND = 20.25
F32 = jnp.float32
BF16 = jnp.bfloat16
NA, NB, NC = 8, 16, 8
STEP = (0, 1, 3, 2)
BACK = (0, 2, 1, 3)
FAR = (7, 6, 3, 5, 2, 4, 1)
PEER_C = ((0, 0), (0, 1), (2, 0), (3, 1), (1, 0), (3, 0), (1, 1), (2, 1))
FAR_C = (7, 6, 3, 2, 5, 4, 1)
GROUPS = ((0,), (12, 2), (8, 14), (6, 4, 10), (13, 3, 9), (15, 7, 5), (11,), (1,))
V_SEM = {s: i for i, g in enumerate(GROUPS) for s in g}
INV_C = (0, 1, 2, 6, 5, 4, 3, 7)
INV_A = [2 * BACK[s // 2] + s % 2 for s in range(NA)]
INV_B = [2 * INV_C[t // 2] + t % 2 for t in range(NB)]


def rel_a(r, s):
    dy = (STEP[r // 2] - STEP[s // 2]) % 4
    return 2 * STEP.index(dy) + (r % 2 + s % 2) % 2


def nt(a, b):
    return lax.dot_general(a, b, (((1,), (1,)), ((), ())), preferred_element_type=F32)


def tn(a, b):
    return lax.dot_general(a, b, (((0,), (0,)), ((), ())), preferred_element_type=F32)


def nn(a, b):
    return jnp.dot(a, b, preferred_element_type=F32)


def forward(x, w_in, w_out, pre_s, hid_s, inv_s, unit_s):
    pre = nn(x[...], w_in[...])
    hid = jnp.maximum(pre, 0.0).astype(BF16)
    emb = nn(hid, w_out[...])
    inv = lax.rsqrt(jnp.sum(emb * emb, axis=-1, keepdims=True) + NORM_EPS)
    unit = emb * inv
    pre_s[...] = pre
    hid_s[...] = hid
    inv_s[...] = jnp.broadcast_to(inv, unit.shape)
    unit_s[...] = unit


def backward(x, w_out, pre_s, hid_s, inv_s, unit_s, d_unit):
    unit = unit_s[...]
    d_emb = inv_s[...] * (d_unit - unit * jnp.sum(unit * d_unit, axis=-1, keepdims=True))
    d_emb = d_emb.astype(BF16)
    g_out = tn(hid_s[...], d_emb)
    d_hid = nt(d_emb, w_out[...])
    d_pre = jnp.where(pre_s[...] > 0, d_hid, 0.0).astype(BF16)
    g_in = tn(x[...], d_pre)
    return g_in, g_out


def kernel(total_rows, qx_h, vx_h, lq_h, wqi_h, wqo_h, wvi_h, wvo_h,
           loss_o, gqi_o, gqo_o, gvi_o, gvo_o,
           qx, vx, lq, wqi, wqo, wvi, wvo,
           u_all, v_all, lq_all, lows, kcol, e_all, zacc, zs, rz, dut, dur, dvs, dvp, dvc, dvr, relay, v_t,
           q_pre, q_hid, q_inv, q_unit, v_pre, v_hid, v_inv, v_unit,
           gq, gv, pq, pv,
           h0, h1, h2, h3, r0, r1, r2, r3, o0, o1, o2, o3, x0, x1, x2, x3, f0, f1, f2, f3,
           ins, us, ur, vs, vr, ls, lr, lows_s, lows_r, zss, zsr, dus, durs, dvps, dvpr, dvss, dvsr, relay_r,
           ps, pr, rss, rsr):
    me = lax.axis_index("dp")
    core = me % 2
    x = (me // 2) % 4
    y = (me // 8) % 4
    z = me // 32
    lo = ((z + 1) // 2) % 2
    hi = z // 2
    scale = 1.0 / (TEMP * total_rows)
    other = (core + 1) % 2
    mate = z * 32 + y * 8 + x * 2 + other

    def a_dev(s):
        zz = z + (s % 2) * (1 - 2 * (z % 2))
        return zz * 32 + ((y + STEP[s // 2]) % 4) * 8 + x * 2 + core

    def c_dev(t, flip=0):
        dx, dh = PEER_C[t]
        return (z + dh * (3 - 2 * z)) * 32 + y * 8 + ((x + dx) % 4) * 2 + (core + flip) % 2

    def copy(src, dst, ssem, rsem, dev):
        return pltpu.make_async_remote_copy(src_ref=src, dst_ref=dst, send_sem=ssem, recv_sem=rsem,
                                            device_id=(dev,), device_id_type=pl.DeviceIdType.MESH)

    def send(src, dst, ssem, rsem, dev):
        copy(src, dst, ssem, rsem, dev).start()

    def arrived(dst, rsem):
        copy(dst, dst, rsem, rsem, me).wait_recv()

    def gone(src, ssem):
        copy(src, src, ssem, ssem, me).wait_send()

    barrier = pltpu.get_barrier_semaphore()
    partners = [a_dev(s) for s in range(1, NA)] + [c_dev(t // 2, t % 2) for t in range(1, NB)]
    for dev in partners:
        pl.semaphore_signal(barrier, inc=1, device_id=(dev,), device_id_type=pl.DeviceIdType.MESH)

    loads = [pltpu.make_async_copy(a, b, ins.at[i]) for i, (a, b) in enumerate((
        (vx_h, vx), (wvi_h, wvi), (wvo_h, wvo), (qx_h, qx), (wqi_h, wqi), (wqo_h, wqo), (lq_h, lq)))]
    for c in loads:
        c.start()
    for c in loads[:3]:
        c.wait()
    forward(vx, wvi, wvo, v_pre, v_hid, v_inv, v_unit)
    v_all[0] = v_unit[...].astype(BF16)
    for c in loads[3:]:
        c.wait()
    forward(qx, wqi, wqo, q_pre, q_hid, q_inv, q_unit)
    ub = q_unit[...].astype(BF16)
    u_all[0, 0] = ub[0:128]
    u_all[1, 0] = ub[128:256]
    pl.semaphore_wait(barrier, len(partners))
    for t in (15, 14, 13, 12, 11, 10, 5, 4, 9, 8, 7, 6, 3, 2, 1):
        send(lq, lq_all.at[INV_B[t]], ls, lr, c_dev(t // 2, t % 2))
    for s in FAR:
        send(u_all.at[0, 0], u_all.at[0, INV_A[s]], us.at[0], ur.at[0], a_dev(s))
    send(v_all.at[0], v_all.at[1], vs, vr.at[V_SEM[1]], mate)
    for t in FAR_C:
        k = 2 * INV_C[t]
        send(v_all.at[0], v_all.at[k], vs, vr.at[V_SEM[k]], c_dev(t))
    for t in FAR:
        k = INV_A[t]
        send(u_all.at[1, 0], u_all.at[1, k], us.at[1], ur.at[1], a_dev(t))
    lq_all[0] = lq[...]
    zacc[...] = jnp.zeros_like(zacc)

    low = lq[...]
    arrived(lq_all.at[1:NB], lr)
    for t in range(1, NB):
        low = jnp.minimum(low, lq_all[t])
    low = jnp.min(low, axis=1, keepdims=True)
    lows[0] = jnp.broadcast_to(low, (1, 128))

    table = jnp.concatenate([lq_all[t] for t in range(NB)], axis=0)
    table = jnp.transpose(LOG2E * ((table - low) + BOUND))
    for t in range(NB):
        kcol[t] = jnp.broadcast_to(table[:, t:t + 1], (256, 128))
    for s in FAR:
        send(lows.at[0], lows.at[INV_A[s]], lows_s, lows_r, a_dev(s))
    arrived(u_all.at[0, 1:NA], ur.at[0])

    c2 = LOG2E / TEMP

    def logits(t, h):
        vt = v_all[t]
        kc = kcol[t]
        kc = jnp.concatenate([kc, kc], axis=1)
        for m in range(4):
            um = u_all[h, 2 * m:2 * m + 2].reshape(256, 128)
            e = jnp.exp2(nt(vt, um) * c2 - kc)
            e_all[t, h, m] = e
            zacc[h, m] += jnp.sum(e.reshape(32, 8, 256), axis=0)

    def share(h):
        rows = []
        for m in range(4):
            row = jnp.sum(zacc[h, m], axis=0, keepdims=True)
            rows += [row[:, 0:128], row[:, 128:256]]
        zs[h, 0] = jnp.concatenate(rows, axis=0)

    def share_send(h):
        for s in FAR:
            send(zs.at[h, 0], zs.at[h, INV_A[s]], zss.at[h], zsr.at[h], a_dev(s))

    arrived(v_all.at[1], vr.at[V_SEM[1]])
    logits(0, 0)
    logits(1, 0)
    for i, group in enumerate(GROUPS[1:4]):
        arrived(v_all.at[0:len(group)], vr.at[i + 1])
        for t in group:
            copy(v_all.at[t], v_all.at[t + 1], vs, vr.at[V_SEM[t + 1]], mate).start()
        for t in group:
            logits(t, 0)
    for i, group in enumerate(GROUPS[4:7]):
        arrived(v_all.at[0:len(group)], vr.at[i + 4])
        for t in group:
            logits(t, 0)
    share(0)
    arrived(u_all.at[1, 1:NA], ur.at[1])
    share_send(0)

    def second(n, c):
        for i in range(8):
            logits(8 * n + i, 1)
        return c

    lax.fori_loop(0, NB // 8, second, 0)
    share(1)

    ji = lax.broadcasted_iota(jnp.int32, (256, 256), 0)
    qi = lax.broadcasted_iota(jnp.int32, (256, 256), 1)
    own = q_unit[...].astype(BF16).astype(F32) * v_unit[...].astype(BF16).astype(F32)
    pos = jnp.sum(own) / TEMP
    share_send(1)

    def combine(h):
        arrived(zs.at[h, 1:NA], zsr.at[h])
        tot = []
        for r in range(NA):
            acc = None
            for s in range(NA):
                k = rel_a(r, s)
                term = fac[s] * zs[h, s, k:k + 1, :]
                acc = term if acc is None else acc + term
            tot.append(acc)
        inv = [fac[0] / w for w in tot]
        for m in range(4):
            rz[h, m] = jnp.concatenate([inv[2 * m], inv[2 * m + 1]], axis=1)
        return jnp.log(tot[0])

    def grads(t, h, diag, even=False):
        vt = v_t[t]
        dv = None
        for m in range(4):
            p = e_all[t, h, m] * rz[h, m]
            if diag and m == 0:
                p = jnp.where((ji == qi + h * 128) & (qi < 128), p - 1.0, p)
            g = p.astype(BF16)
            d = nn(g, u_all[h, 2 * m:2 * m + 2].reshape(256, 128))
            dv = d if dv is None else dv + d
            du = nn(vt, g)
            if diag:
                dut[h, 2 * m] = du[:, 0:128]
                dut[h, 2 * m + 1] = du[:, 128:256]
            else:
                dut[h, 2 * m] += du[:, 0:128]
                dut[h, 2 * m + 1] += du[:, 128:256]
        if h == 0:
            dvs[t] = dv
        elif even:
            dvc[t // 2] = dvs[t] + dv + dvp[t // 2]
        else:
            dvs[t] += dv

    for t in range(NB):
        v_t[t] = jnp.transpose(v_all[t])
    arrived(lows.at[1:NA], lows_r)
    lowv = [lows[s] for s in range(NA)]
    least = functools.reduce(jnp.minimum, lowv)
    fac = [jnp.exp(least - w) for w in lowv]
    log0 = combine(0)
    grads(0, 0, True)

    def third(n, c):
        for i in range(1, 6):
            grads(5 * n + i, 0, False)
        return c

    lax.fori_loop(0, 3, third, 0)
    log1 = combine(1)
    for s in FAR:
        send(dut.at[0, s], dur.at[0, INV_A[s]], dus.at[0], durs.at[0], a_dev(s))

    def mate_copy(t):
        return copy(dvs.at[2 * t + 1], dvp.at[t], dvps, dvpr.at[t // 2], mate)

    def dv_send(t):
        if t > 5:
            send(dvc.at[t], relay.at[7 - t], dvss, relay_r.at[7 - t], c_dev(1 if t == 7 else 4))
        else:
            send(dvc.at[t], dvr.at[t], dvss, dvsr, c_dev(t))

    grads(0, 1, True)

    def odd(n, c):
        t = 7 - 2 * n

        @pl.when(n > 0)
        def _():
            mate_copy(t + 1).start()

        grads(2 * t + 1, 1, False)
        grads(2 * t - 1, 1, False)
        mate_copy(t).start()
        return c

    lax.fori_loop(0, 4, odd, 0)

    mate_copy(0).start()
    for t in (7, 5, 3):
        arrived(dvp.at[t - 1:t + 1], dvpr.at[t // 2])
        if t < 7:
            dv_send(t + 1)
        grads(2 * t, 1, False, True)
        grads(2 * t - 2, 1, False, True)
        dv_send(t)
    arrived(dvp.at[0:2], dvpr.at[0])
    grads(2, 1, False, True)
    for s in FAR:
        send(dut.at[1, s], dur.at[1, INV_A[s]], dus.at[1], durs.at[1], a_dev(s))
    loss_rows = ((lq[:, 0:128] - least) + BOUND + log0) + ((lq[:, 128:256] - least) + BOUND + log1)
    loss_loc = jnp.sum(loss_rows, axis=1, keepdims=True) - pos
    arrived(relay.at[0], relay_r.at[0])
    dvc[2] += relay[0]
    dvc[0] = dvs[0] + dvp[0]
    dv_send(2)
    arrived(relay.at[1], relay_r.at[1])
    dvc[1] += relay[1]

    def sum_du(h):
        arrived(dur.at[h, 1:NA], durs.at[h])
        du = dut[h, 0]
        for s in range(1, NA):
            du = du + dur[h, s]
        return jnp.transpose(du)

    parts = [sum_du(0)]
    dv_send(1)
    parts.append(sum_du(1))
    d_unit = jnp.concatenate(parts, axis=0) * scale
    g_in, g_out = backward(qx, wqo, q_pre, q_hid, q_inv, q_unit, d_unit)

    def pack(buf, g_in, g_out):
        buf[0, 0:512, :] = g_in[:, 0:128]
        buf[0, 512:640, :] = g_in[0:128, 128:256]
        buf[1, 0:384, :] = g_in[128:512, 128:256]
        buf[1, 384:640, :] = g_out

    pack(gq, g_in, g_out)
    lt = jnp.broadcast_to(loss_loc, (8, 128))
    gq[0, 640:648, :] = lt
    gq[1, 640:648, :] = lt
    send(gq.at[other], pq, ps.at[0], pr.at[0], mate)

    a_me, b_me = y * 2 + lo, x * 2 + hi

    def a_idx(s):
        return ((y + STEP[s // 2]) % 4) * 2 + (lo + s % 2) % 2

    def c_idx(t):
        return ((x + PEER_C[t][0]) % 4) * 2 + (hi + PEER_C[t][1]) % 2

    side_a, side_c = (a_dev, a_idx, a_me, FAR, INV_A), (c_dev, c_idx, b_me, FAR_C, INV_C)
    paths = (
        (0, h0, r0, o0, x0, f0, side_c, side_a),
        (1, h1, r1, o1, x1, f1, side_a, side_c),
        (2, h2, r2, o2, x2, f2, side_a, side_c),
        (3, h3, r3, o3, x3, f3, side_c, side_a),
    )

    def pair(w, g, p):
        arrived(p, pr.at[w])
        for i, h, r, o, xx, f, (dev, idx, mine, far, inv), _ in paths[2 * w:2 * w + 2]:
            base = 320 * (i % 2)
            h[:, 0:40, :] = (g[core, base:base + 320, :] + p[base:base + 320, :]).reshape(8, 40, 128)
            if i == 0:
                extra = g[core, 640:648, :] + p[640:648, :]
                for n in range(8):
                    h[n, 40:48, :] = extra
        for i, h, r, o, xx, f, (dev, idx, mine, far, inv), _ in paths[2 * w:2 * w + 2]:
            for s in far:
                send(h.at[idx(s)], r.at[inv[s]], rss.at[0, i], rsr.at[0, i], dev(s))

    def scatter(w):
        for i, h, r, o, xx, f, (_, _, mine, _, _), (dev, _, _, far, inv) in paths[2 * w:2 * w + 2]:
            arrived(r.at[1:8], rsr.at[0, i])
            acc = h[mine]
            for s in range(1, 8):
                acc = acc + r[s]
            o[...] = acc
            for s in far:
                send(o, xx.at[inv[s]], rss.at[1, i], rsr.at[1, i], dev(s))

    def exchange(w):
        for i, h, r, o, xx, f, (dev, idx, mine, far, inv), _ in paths[2 * w:2 * w + 2]:
            arrived(xx.at[1:8], rsr.at[1, i])
            acc = o[...]
            for s in range(1, 8):
                acc = acc + xx[s]
            f[core, mine] = acc
            for s in far:
                send(f.at[core, mine], f.at[core, mine], rss.at[2, i], rsr.at[2, i], dev(s))
            if i == 0:
                loss_o[...] = acc[40:48] * (1.0 / total_rows)

    def gather(w):
        for i, h, r, o, xx, f, _, _ in paths[2 * w:2 * w + 2]:
            arrived(r.at[1:8], rsr.at[2, i])
            send(f.at[core], f.at[core], rss.at[3, i], rsr.at[3, i], mate)

    def finish(w, go_in, go_out):
        halves = [[], []]
        for i, h, r, o, xx, f, _, _ in paths[2 * w:2 * w + 2]:
            arrived(h, rsr.at[3, i])
            for c in range(2):
                halves[c].append(f[c, :, 0:40, :].reshape(320, 128))
        head, tail = [jnp.concatenate(c, axis=0) for c in halves]
        go_in[:, 0:128] = head[0:512]
        go_in[0:128, 128:256] = head[512:640]
        go_in[128:512, 128:256] = tail[0:384]
        go_out[...] = tail[384:640]

    pair(0, gq, pq)
    arrived(dvr.at[1:6], dvsr)
    dv = lax.fori_loop(1, 6, lambda t, acc: acc + dvr[t], dvc[0])
    g_in, g_out = backward(vx, wvo, v_pre, v_hid, v_inv, v_unit, dv * scale)
    pack(gv, g_in, g_out)
    send(gv.at[other], pv, ps.at[1], pr.at[1], mate)
    pair(1, gv, pv)
    scatter(0)
    scatter(1)
    exchange(0)
    exchange(1)
    gather(0)
    gather(1)
    finish(0, gqi_o, gqo_o)
    finish(1, gvi_o, gvo_o)
    gone(lq_all.at[1:NB], ls)
    gone(lows.at[1:NA], lows_s)
    gone(v_all.at[1:NB], vs)
    for h in range(2):
        gone(u_all.at[h, 1:NA], us.at[h])
        gone(zs.at[h, 1:NA], zss.at[h])
        gone(dur.at[h, 1:NA], dus.at[h])
    gone(dvp, dvps)
    gone(dvr.at[1:NC], dvss)
    gone(pq, ps.at[0])
    gone(pv, ps.at[1])
    for i, h, r, o, xx, f, _, _ in paths:
        gone(r.at[1:8], rss.at[0, i])
        gone(xx.at[1:8], rss.at[1, i])
        gone(r.at[1:8], rss.at[2, i])
        gone(h, rss.at[3, i])


def emit(loss, gqi, gqo, gvi, gvo, loss_o, gqi_o, gqo_o, gvi_o, gvo_o, value, sem):
    pairs = ((value, loss_o), (gqi, gqi_o), (gvi, gvi_o), (gqo, gqo_o), (gvo, gvo_o))
    copies = [pltpu.make_async_copy(a, b, sem.at[i]) for i, (a, b) in enumerate(pairs)]
    for c in copies[1:]:
        c.start()
    value[0] = loss[0, 0]
    copies[0].start()
    for c in copies:
        c.wait()


def solution(mesh):
    group = mesh.shape["dp"]

    def local_step(query_feat, item_feat, log_q, w_query_in, w_query_out, w_item_in, w_item_out):
        local_rows = query_feat.shape[0]
        vm = lambda *s: pltpu.VMEM(s, F32)
        vb = lambda *s: pltpu.VMEM(s, BF16)
        sem = lambda *s: pltpu.SemaphoreType.DMA(s)
        one = pltpu.SemaphoreType.DMA
        scratch = [
            vb(256, 512), vb(256, 512), vm(1, 256), vb(512, 256), vb(256, 128), vb(512, 256), vb(256, 128),
            vb(2, NA, 128, 128), vb(NB, 256, 128), vm(NB, 1, 256), vm(NA, 1, 128), vm(NB, 256, 128),
            vm(NB, 2, 4, 256, 256), vm(2, 4, 8, 256), vm(2, NA, 8, 128), vm(2, 4, 1, 256),
            vm(2, NA, 128, 128), vm(2, NA, 128, 128),
            vm(NB, 256, 128), vm(NC, 256, 128), vm(NC, 256, 128), vm(NC, 256, 128), vm(2, 256, 128), vb(NB, 128, 256),
            vm(256, 256), vb(256, 256), vm(256, 128), vm(256, 128),
            vm(256, 256), vb(256, 256), vm(256, 128), vm(256, 128),
            vm(2, 648, 128), vm(2, 640, 128), vm(648, 128), vm(640, 128),
            vm(8, 48, 128), vm(8, 40, 128), vm(8, 40, 128), vm(8, 40, 128),
            vm(8, 48, 128), vm(8, 40, 128), vm(8, 40, 128), vm(8, 40, 128),
            vm(48, 128), vm(40, 128), vm(40, 128), vm(40, 128),
            vm(8, 48, 128), vm(8, 40, 128), vm(8, 40, 128), vm(8, 40, 128),
            vm(2, 8, 48, 128), vm(2, 8, 40, 128), vm(2, 8, 40, 128), vm(2, 8, 40, 128),
            sem(7), sem(2), sem(2), one, sem(8), one, one, one, one, sem(2), sem(2),
            sem(2), sem(2), one, sem(4), one, one, sem(2),
            sem(2), sem(2), sem(4, 4), sem(4, 4),
        ]
        vspec = pl.BlockSpec(memory_space=pltpu.VMEM)
        shapes = ((512, 256), (256, 128), (512, 256), (256, 128))
        hbm = pl.BlockSpec(memory_space=pltpu.HBM)
        staged = pl.pallas_call(
            functools.partial(kernel, local_rows * group),
            out_shape=tuple(pltpu.VMEM(s, F32) for s in ((8, 128), *shapes)),
            in_specs=[hbm] * 7,
            out_specs=(vspec,) * 5,
            scratch_shapes=scratch,
            compiler_params=pltpu.CompilerParams(collective_id=0, has_side_effects=True,
                                                 vmem_limit_bytes=56 * 1024 * 1024),
        )(query_feat, item_feat, log_q.reshape(1, local_rows), w_query_in, w_query_out, w_item_in, w_item_out)
        return pl.pallas_call(
            emit,
            out_shape=tuple(jax.ShapeDtypeStruct(s, F32) for s in ((1,), *shapes)),
            in_specs=[vspec] * 5,
            out_specs=(hbm,) * 5,
            scratch_shapes=[pltpu.SMEM((1,), F32), sem(5)],
            compiler_params=pltpu.CompilerParams(vmem_limit_bytes=1024 * 1024),
        )(*staged)

    return jax.shard_map(local_step, mesh=mesh,
                         in_specs=(P("dp", None), P("dp", None), P("dp"), P(), P(), P(), P()),
                         out_specs=(P(), P(), P(), P(), P()), check_vma=False)
```
